256 devices in a mesh: set: 16 (over z, core), col: 16 (over y, x).
Axes of the slice: x: 4, y: 4, z: 8, core: 2. Of those that a mesh axis runs over, the one named last changes fastest.
Arguments:
- factor: float32 [32, 2, 131072], P('col'), may hold values from -8 to 8
- velocity: float32 [32, 2, 131072], P(None, None, ('set', 'col')), may hold values from -4 to 4
- labels: int32 [16, 17], P('set'), may hold values from 0 to 2
- counts: int32 [16, 131072], P('set'), may hold values from 1 to 28, as said below
Outputs:
- new_factor: float32 [32, 2, 131072], P(None, None, ('set', 'col'))
- new_velocity: float32 [32, 2, 131072], P(None, None, ('set', 'col'))
The draws below stay inside these ranges and needn't reach their ends.
Inputs may be any that keep to these rules, and one draw needn't show every extreme that they name: `labels`: 0 selects the X basis, 1 the Y basis, 2 the Z basis. The counts of setting s lie between 1 and 4 + (24 s) // 15.
All inputs are finite; a program needn't handle non-finite values.
Results may differ from the reference program's by a relative error of at most 0.0003.
Values sent between devices are 32-bit elements; how exact they have to be, the bound alone decides.
No kernel may reach another device: no remote copies, remote signals or barrier semaphores. Data moves between devices by JAX's collectives and lax.ppermute only.
A program may use at most 64 MiB of HBM per device.

```python
import jax
import jax.numpy as jnp
from jax import lax

QA = 8
QB = 9
QUBITS = 17
ORDER = 131072
RANK = 32
SETTINGS = 16


def draw_factor(key, part):
    base = jax.random.fold_in(key, 11)
    key_own, key_common = jax.random.split(base, 2)
    own = jax.random.normal(key_own, (RANK, 2, ORDER), jnp.float32)
    common = jax.random.normal(key_common, (1, 2, ORDER), jnp.float32)
    values = own + 0.5 * common
    return jnp.clip(values, -8.0, 8.0)


def draw_counts(key, part):
    base = jax.random.fold_in(key, 23)
    setting_index = jnp.arange(SETTINGS, dtype=jnp.int32)
    upper = 4 + 24 * setting_index // (SETTINGS - 1)
    return jax.random.randint(base, (SETTINGS, ORDER), 1, upper[:, None] + 1, jnp.int32)


def plant(drawn, key, low, largest):
    place = [jax.random.randint(jax.random.fold_in(key, axis), (), 0, length) for axis, length in enumerate(drawn.shape)]
    widest = drawn.shape.index(max(drawn.shape))
    neighbour = place[:widest] + [(place[widest] + 1) % drawn.shape[widest]] + place[widest + 1:]
    return drawn.at[tuple(place)].set(low).at[tuple(neighbour)].set(largest)


def level_of(stream_key, extent, cuts, low, top_value):
    def one(axis_at, shards_of):
        draws = jax.random.uniform(jax.random.fold_in(jax.random.fold_in(stream_key, 6), axis_at), (shards_of,), jnp.float32, low / len(cuts), top_value / len(cuts))
        return jnp.repeat(jnp.exp(draws), extent[axis_at] // shards_of).reshape((-1,) + (1,) * (len(extent) - axis_at - 1))

    loudness = one(*cuts[0])
    for cut in cuts[1:]:
        loudness = loudness * one(*cut)
    return loudness


def noise(stream_key, extent, spread, bound, shards=(), kind=jnp.bfloat16):
    values = spread * jax.random.normal(stream_key, extent, jnp.float32)
    if shards:
        values = values * level_of(stream_key, extent, shards, -0.22, 0.18)
    return jnp.clip(values, -bound, bound).astype(kind)


def setup_inputs(seed: int = 0) -> dict:
    arg_keys = jax.random.split(jax.random.key(seed), 5)
    return {
        "factor": draw_factor(jax.random.fold_in(arg_keys[4], 71), 0),
        "velocity": noise(arg_keys[1], (RANK, 2, ORDER), 0.5, 4.0, ((2, 256),), jnp.float32),
        "labels": plant(jax.random.randint(arg_keys[2], (SETTINGS, QUBITS), 0, 3), jax.random.fold_in(arg_keys[2], 1), 0, 2).astype(jnp.int32),
        "counts": draw_counts(jax.random.fold_in(arg_keys[4], 71), 0),
    }


mixing = 0.1
penalty = 8.0
momentum = 0.9
step_size = 0.5
half_root = 0.7071067811865476
count_norm = 8.0


def kron_factor(labels_part):
    width = labels_part.shape[0]
    size = 2 ** width
    row_index = lax.broadcasted_iota(jnp.int32, (size, size), 0)
    col_index = lax.broadcasted_iota(jnp.int32, (size, size), 1)
    phase = jnp.zeros((size, size), jnp.int32)
    allowed = jnp.ones((size, size), jnp.bool_)
    nonz_count = jnp.zeros((), jnp.float32)
    for position in range(width):
        shift_amount = width - 1 - position
        row_bit = (row_index >> shift_amount) & 1
        col_bit = (col_index >> shift_amount) & 1
        label_value = labels_part[position]
        phase = phase + jnp.where(label_value == 0, 2 * row_bit * col_bit, jnp.where(label_value == 1, col_bit * (3 + 2 * row_bit), 0))
        allowed = jnp.logical_and(allowed, jnp.logical_or(label_value != 2, row_bit == col_bit))
        nonz_count = nonz_count + jnp.where(label_value == 2, 0.0, 1.0).astype(jnp.float32)
    phase = phase % 4
    magnitude = jnp.power(jnp.float32(half_root), nonz_count)
    scale = jnp.where(allowed, magnitude, jnp.float32(0.0))
    mat_real = jnp.where(phase == 0, 1.0, jnp.where(phase == 2, -1.0, 0.0)).astype(jnp.float32) * scale
    mat_imag = jnp.where(phase == 1, 1.0, jnp.where(phase == 3, -1.0, 0.0)).astype(jnp.float32) * scale
    return mat_real, mat_imag


def setting_forms(labels_row):
    left_real, left_imag = kron_factor(labels_row[:QA])
    right_real, right_imag = kron_factor(labels_row[QA:])
    return left_real, left_imag, right_real, right_imag


def rotate_forward(columns, forms):
    left_real, left_imag, right_real, right_imag = forms
    high = lax.Precision.HIGHEST
    first_real = jnp.einsum('ae,rceb->rcab', left_real, columns, precision=high)
    first_imag = jnp.einsum('ae,rceb->rcab', left_imag, columns, precision=high)
    section_one = jnp.stack([first_real[:, 0] - first_imag[:, 1], first_real[:, 1] + first_imag[:, 0]], axis=1)
    second_real = jnp.einsum('rcab,db->rcad', section_one, right_real, precision=high)
    second_imag = jnp.einsum('rcab,db->rcad', section_one, right_imag, precision=high)
    return jnp.stack([second_real[:, 0] - second_imag[:, 1], second_real[:, 1] + second_imag[:, 0]], axis=1)


def rotate_back(columns, forms):
    left_real, left_imag, right_real, right_imag = forms
    high = lax.Precision.HIGHEST
    first_real = jnp.einsum('rcad,db->rcab', columns, right_real, precision=high)
    first_imag = jnp.einsum('rcad,db->rcab', columns, right_imag, precision=high)
    section_one = jnp.stack([first_real[:, 0] + first_imag[:, 1], first_real[:, 1] - first_imag[:, 0]], axis=1)
    second_real = jnp.einsum('ae,rcab->rceb', left_real, section_one, precision=high)
    second_imag = jnp.einsum('ae,rcab->rceb', left_imag, section_one, precision=high)
    return jnp.stack([second_real[:, 0] + second_imag[:, 1], second_real[:, 1] - second_imag[:, 0]], axis=1)


def reference(factor, velocity, labels, counts):
    left_size = 2 ** QA
    right_size = 2 ** QB
    columns = factor.reshape(RANK, 2, left_size, right_size)
    trace_value = jnp.sum(factor * factor)

    def per_setting(carry, inputs):
        adjoint_sum, ratio_sum = carry
        labels_row, counts_row = inputs
        forms = setting_forms(labels_row)
        rotated = rotate_forward(columns, forms)
        probability = jnp.sum(rotated * rotated, axis=(0, 1)).reshape(ORDER)
        quasi = (1.0 - mixing) * probability / trace_value + mixing / ORDER
        weights = counts_row.astype(jnp.float32) / ((count_norm * ORDER) * quasi)
        ratio_sum = ratio_sum + jnp.sum(weights * probability) / trace_value
        weighted = rotated * weights.reshape(1, 1, left_size, right_size)
        adjoint_sum = adjoint_sum + rotate_back(weighted, forms)
        return (adjoint_sum, ratio_sum), None

    start = (jnp.zeros((RANK, 2, left_size, right_size), jnp.float32), jnp.zeros((), jnp.float32))
    (adjoint_sum, ratio_total), unused = lax.scan(per_setting, start, (labels, counts))
    adjoint_sum = adjoint_sum.reshape(RANK, 2, ORDER)
    block_real = factor[:, 0]
    block_imag = factor[:, 1]
    high = lax.Precision.HIGHEST
    gram_real = jnp.dot(block_real, block_real.T, precision=high) + jnp.dot(block_imag, block_imag.T, precision=high)
    gram_imag = jnp.dot(block_real, block_imag.T, precision=high) - jnp.dot(block_imag, block_real.T, precision=high)
    purity = (jnp.sum(jnp.square(gram_real)) + jnp.sum(jnp.square(gram_imag))) / jnp.square(trace_value)
    mixed_real = jnp.dot(gram_real.T, block_real, precision=high) - jnp.dot(gram_imag.T, block_imag, precision=high)
    mixed_imag = jnp.dot(gram_real.T, block_imag, precision=high) + jnp.dot(gram_imag.T, block_real, precision=high)
    mixed = jnp.stack([mixed_real, mixed_imag], axis=1)
    gradient = -((1.0 - mixing) / SETTINGS) * (adjoint_sum - ratio_total * factor) + penalty * (2.0 * mixed / trace_value - 2.0 * purity * factor)
    new_velocity = momentum * velocity + gradient
    new_factor = factor - step_size * new_velocity
    return new_factor, new_velocity
```

```python
import functools

import jax
import jax.numpy as jnp
from jax import lax
from jax.experimental import pallas as pl
from jax.experimental.pallas import tpu as pltpu
from jax.sharding import Mesh
from jax.sharding import PartitionSpec as P

QA, QB, QUBITS = 8, 9, 17
ORDER = 2**QUBITS
LEFT, RIGHT = 2**QA, 2**QB
LANES = 128
HIGHS = RIGHT // LANES
ROWS = ORDER // LANES
COLS = 16
SETS = 16
ZS = 8

COL = ("y", "x")
SET = ("z", "core")

mixing = 0.1
penalty = 8.0
momentum = 0.9
step_size = 0.5
count_norm = 8.0

F32 = jnp.float32
BF16 = jnp.bfloat16
HIGH = lax.Precision.HIGHEST
PCHUNK = ROWS // COLS
VMEM = pl.BlockSpec(memory_space=pltpu.VMEM)
SMEM = pl.BlockSpec(memory_space=pltpu.SMEM)


def halves(x):
    high = x.astype(BF16)
    return high, (x - high.astype(F32)).astype(BF16)


def masks_of(labels_ref):
    rotated_bits = jnp.int32(0)
    y_bits = jnp.int32(0)
    scale = jnp.float32(1.0)
    for q in range(QUBITS):
        label = labels_ref[0, q]
        bit = jnp.int32(1 << (QUBITS - 1 - q))
        rotated_bits = rotated_bits + jnp.where(label == 2, 0, bit)
        y_bits = y_bits + jnp.where(label == 1, bit, 0)
        scale = scale * jnp.where(label == 2, jnp.float32(1.0), jnp.float32(0.5))
    return rotated_bits, y_bits, scale


def hadamard(row, size, bits):
    col = lax.broadcasted_iota(jnp.int32, row.shape, 1)
    odd = lax.population_count(row & col & bits) & 1
    same = ((row ^ col) & (size - 1 - bits)) == 0
    return jnp.where(same, (1 - 2 * odd).astype(F32), 0.0).astype(BF16)


def quarter_turns(row, high, y_bits):
    lane = lax.broadcasted_iota(jnp.int32, row.shape, 1)
    index = row * RIGHT + high * LANES + lane
    return lax.population_count(index & y_bits) & 3


def forward_kernel(labels_ref, factor_ref, rotated_ref, send_ref, xh, xl, th, tl, prob, hb):
    set_index = lax.axis_index("z") * 2 + lax.axis_index("core")
    bits, y_bits, scale = masks_of(labels_ref)
    a_bits, b_bits = bits >> QB, bits & (RIGHT - 1)
    hb[...] = hadamard(lax.broadcasted_iota(jnp.int32, (RIGHT, RIGHT), 0), RIGHT, b_bits)
    ha = hadamard(lax.broadcasted_iota(jnp.int32, (LEFT, LEFT), 0), LEFT, a_bits)
    row = lax.broadcasted_iota(jnp.int32, (LEFT, LANES), 0)
    for high in range(HIGHS):
        turns = quarter_turns(row, high, y_bits)
        swap = (turns & 1) == 1
        sign_real = jnp.where(turns >= 2, -1.0, 1.0)
        sign_imag = jnp.where((turns == 1) | (turns == 2), -1.0, 1.0)
        block = pl.ds(high * LANES, LANES)
        for r in range(2):
            real = factor_ref[r, pl.ds(2 * high, LEFT, stride=2 * HIGHS), :]
            imag = factor_ref[r, pl.ds(2 * high + 1, LEFT, stride=2 * HIGHS), :]
            for c, turned in (
                (0, sign_real * jnp.where(swap, imag, real)),
                (1, sign_imag * jnp.where(swap, real, imag)),
            ):
                xh[2 * r + c, :, block], xl[2 * r + c, :, block] = halves(turned)
    prob[...] = jnp.zeros_like(prob)

    def one(i, carry):
        for n in range(2):
            part = pl.ds(n * 256, 256)
            first = jnp.dot(ha, xh[i, :, part], preferred_element_type=F32) + jnp.dot(
                ha, xl[i, :, part], preferred_element_type=F32
            )
            th[:, part], tl[:, part] = halves(first)
        for n in range(2):
            part = pl.ds(n * 256, 256)
            second = jnp.dot(th[...], hb[:, part], preferred_element_type=F32) + jnp.dot(
                tl[...], hb[:, part], preferred_element_type=F32
            )
            rotated_ref[i, :, part] = second
            prob[:, part] += second * second
        return carry

    lax.fori_loop(0, 4, one, 0)
    for c in range(COLS):
        for high in range(HIGHS):
            send_ref[c, pl.ds(16 * high, 16), :] = (
                prob[pl.ds(16 * c, 16), pl.ds(high * LANES, LANES)] * scale
            )
        start = pl.multiple_of(set_index * (ROWS * 2 // SETS) + 8 * c, 8)
        for r in range(2):
            send_ref[c, pl.ds(PCHUNK + 8 * r, 8), :] = factor_ref[r, pl.ds(start, 8), :]


def summed_kernel(got_ref, send_ref, rows):
    total = got_ref[0, pl.ds(0, PCHUNK), :]
    for c in range(1, COLS):
        total = total + got_ref[c, pl.ds(0, PCHUNK), :]
    for c in range(COLS):
        rows[pl.ds(16 * c, 16), :] = got_ref[c, pl.ds(PCHUNK, 16), :]
    parts = both_parts(rows)
    gram = lax.dot_general(
        parts, parts, (((1,), (1,)), ((), ())), precision=HIGH, preferred_element_type=F32
    )
    rows[pl.ds(0, 64), :] = jnp.zeros((64, LANES), F32)
    rows[pl.ds(0, 64), pl.ds(0, 64)] = gram
    for c in range(COLS):
        send_ref[c, pl.ds(0, PCHUNK), :] = total
        send_ref[c, pl.ds(PCHUNK, 8), :] = jnp.zeros((8, LANES), F32)
        send_ref[c, pl.ds(PCHUNK, 4), :] = rows[pl.ds(4 * c, 4), :]


def both_parts(rows):
    real, imag = (
        jnp.concatenate(
            [rows[pl.ds(2 * high + c, 32, stride=2 * HIGHS), :] for high in range(HIGHS)], axis=1
        )
        for c in range(2)
    )
    return jnp.concatenate([real, imag], axis=0)


def back_kernel(labels_ref, got_ref, rotated_ref, counts_ref, keep_ref, send_ref, weight, wh, wl, th, tl, hb):
    core = lax.axis_index("core")
    bits, y_bits, scale = masks_of(labels_ref)
    a_bits, b_bits = bits >> QB, bits & (RIGHT - 1)
    hb[...] = hadamard(lax.broadcasted_iota(jnp.int32, (RIGHT, RIGHT), 0), RIGHT, b_bits)

    def owners(shape):
        i = lax.broadcasted_iota(jnp.int32, shape, 0)
        half, z, own = i >> 7, (i >> 4) & 7, i & 15
        return z * 32 + (half ^ core) * 16 + own

    ha = hadamard(owners((LEFT, LEFT)), LEFT, a_bits)
    total = jnp.zeros((PCHUNK, LANES), F32)
    gram = jnp.zeros((8, LANES), F32)
    for c in range(COLS):
        total = total + got_ref[c, pl.ds(0, PCHUNK), :]
        gram = gram + got_ref[c, pl.ds(PCHUNK, 8), :]
    trace = jnp.sum(total)
    slope = (1.0 - mixing) / trace
    ratio_sum = jnp.zeros((16, LANES), F32)
    for high in range(HIGHS):
        count = counts_ref[pl.ds(high, LEFT, stride=HIGHS), :].astype(F32)
        for c in range(COLS):
            p = got_ref[c, pl.ds(16 * high, 16), :]
            w = count[16 * c : 16 * c + 16] / ((count_norm * ORDER) * (slope * p + mixing / ORDER))
            weight[pl.ds(16 * c, 16), pl.ds(high * LANES, LANES)] = w
            ratio_sum = ratio_sum + w * p
    ratio = jnp.sum(ratio_sum) / trace

    def one(i, carry):
        for n in range(2):
            part = pl.ds(n * 256, 256)
            wh[:, part], wl[:, part] = halves(
                (weight[:, part] - ratio) * scale * rotated_ref[i, :, part]
            )
        for n in range(2):
            part = pl.ds(n * 256, 256)
            first = jnp.dot(wh[...], hb[:, part], preferred_element_type=F32) + jnp.dot(
                wl[...], hb[:, part], preferred_element_type=F32
            )
            th[i, :, part], tl[i, :, part] = halves(first)
        return carry

    lax.fori_loop(0, 4, one, 0)
    row = owners((LEFT, LANES))
    for high in range(HIGHS):
        turns = quarter_turns(row, high, y_bits)
        swap = (turns & 1) == 1
        sign_real = jnp.where((turns == 1) | (turns == 2), -1.0, 1.0)
        sign_imag = jnp.where(turns >= 2, -1.0, 1.0)
        block = pl.ds(high * LANES, LANES)
        for r in range(2):
            real, imag = (
                jnp.dot(ha, th[2 * r + c, :, block], preferred_element_type=F32)
                + jnp.dot(ha, tl[2 * r + c, :, block], preferred_element_type=F32)
                for c in range(2)
            )
            for c, turned in (
                (0, sign_real * jnp.where(swap, imag, real)),
                (1, sign_imag * jnp.where(swap, real, imag)),
            ):
                for half, out in ((0, keep_ref), (1, send_ref)):
                    for z in range(ZS):
                        at = 128 * half + 16 * z
                        out[z, pl.ds(128 * r + 2 * high + c, 16, stride=2 * HIGHS), :] = turned[
                            at : at + 16
                        ]
    for z in range(ZS):
        keep_ref[z, pl.ds(256, 8), :] = gram
        send_ref[z, pl.ds(256, 8), :] = gram


def packed_kernel(got_ref, send_ref):
    total = got_ref[0]
    for z in range(1, ZS):
        total = total + got_ref[z]
    for c in range(COLS):
        for r in range(2):
            send_ref[c, pl.ds(8 * r, 8), :] = total[128 * r + 8 * c : 128 * r + 8 * c + 8]
        send_ref[c, pl.ds(16, 8), :] = total[256:264]


def update_kernel(got_ref, first_ref, velocity_ref, factor_ref_out, velocity_ref_out, rows, gram_ref, mixed_ref):
    for c in range(COLS):
        rows[pl.ds(16 * c, 16), :] = first_ref[c, pl.ds(PCHUNK, 16), :]
        gram_ref[pl.ds(4 * c, 4), :] = got_ref[c, pl.ds(16, 4), :]
    gram = gram_ref[:, pl.ds(0, 64)]
    i = lax.broadcasted_iota(jnp.int32, (64, 64), 0)
    j = lax.broadcasted_iota(jnp.int32, (64, 64), 1)
    turn = jnp.where(j == i + 32, -1.0, jnp.where(j == i - 32, 1.0, 0.0)).astype(F32)
    turned = jnp.dot(turn, gram, precision=HIGH, preferred_element_type=F32)
    turned = lax.dot_general(
        turned, turn, (((1,), (1,)), ((), ())), precision=HIGH, preferred_element_type=F32
    )
    whole = gram + turned
    trace = jnp.sum(jnp.where(i == j, gram, 0.0))
    purity = 0.5 * jnp.sum(whole * whole) / (trace * trace)
    mixed = jnp.dot(whole, both_parts(rows), precision=HIGH, preferred_element_type=F32)
    for high in range(HIGHS):
        for c in range(2):
            mixed_ref[pl.ds(2 * high + c, 32, stride=2 * HIGHS), :] = mixed[
                32 * c : 32 * c + 32, high * LANES : (high + 1) * LANES
            ]
    for c in range(COLS):
        at = pl.ds(16 * c, 16)
        own = rows[at, :]
        gradient = -((1.0 - mixing) / SETS) * got_ref[c, pl.ds(0, 16), :] + penalty * (
            2.0 * mixed_ref[at, :] / trace - 2.0 * purity * own
        )
        velocity = momentum * velocity_ref[at, :] + gradient
        velocity_ref_out[at, :] = velocity
        factor_ref_out[at, :] = own - step_size * velocity


def shape(*dims):
    return jax.ShapeDtypeStruct(dims, F32)


def call(kernel, name, out, n_in, scratch=(), scalars=0):
    return pl.pallas_call(
        kernel,
        name=name,
        out_shape=out,
        in_specs=[SMEM] * scalars + [VMEM] * (n_in - scalars),
        out_specs=jax.tree.map(lambda _: VMEM, out),
        scratch_shapes=list(scratch),
        compiler_params=pltpu.CompilerParams(vmem_limit_bytes=48 * 2**20),
    )


def exchange(array, axis):
    return lax.all_to_all(array, axis, split_axis=0, concat_axis=0, tiled=True)


def shards(factor, velocity, labels, counts):
    own = factor.reshape(2, 2, ROWS, LANES).transpose(0, 2, 1, 3).reshape(2, 2 * ROWS, LANES)
    counted = counts.reshape(ROWS, LANES)
    moved = velocity.reshape(32, 2, HIGHS, LANES).transpose(0, 2, 1, 3).reshape(256, LANES)
    matrix = (LEFT, RIGHT)
    rotated, sent = call(
        forward_kernel,
        "forward",
        (shape(4, *matrix), shape(COLS, PCHUNK + 16, LANES)),
        2,
        [
            pltpu.VMEM((4, *matrix), BF16),
            pltpu.VMEM((4, *matrix), BF16),
            pltpu.VMEM(matrix, BF16),
            pltpu.VMEM(matrix, BF16),
            pltpu.VMEM(matrix, F32),
            pltpu.VMEM((RIGHT, RIGHT), BF16),
        ],
        scalars=1,
    )(labels, own)
    first = exchange(sent, COL)
    sent = call(
        summed_kernel, "summed", shape(COLS, PCHUNK + 8, LANES), 1, [pltpu.VMEM((256, LANES), F32)]
    )(first)
    second = exchange(sent, COL)
    kept, sent = call(
        back_kernel,
        "back",
        (shape(ZS, 264, LANES), shape(ZS, 264, LANES)),
        4,
        [
            pltpu.VMEM(matrix, F32),
            pltpu.VMEM(matrix, BF16),
            pltpu.VMEM(matrix, BF16),
            pltpu.VMEM((4, *matrix), BF16),
            pltpu.VMEM((4, *matrix), BF16),
            pltpu.VMEM((RIGHT, RIGHT), BF16),
        ],
        scalars=1,
    )(labels, second, rotated, counted)
    pair = kept + lax.ppermute(sent, "core", [(0, 1), (1, 0)])
    third = exchange(pair, "z")
    sent = call(packed_kernel, "packed", shape(COLS, 24, LANES), 1)(third)
    fourth = exchange(sent, COL)
    new_factor, new_velocity = call(
        update_kernel,
        "update",
        (shape(256, LANES), shape(256, LANES)),
        3,
        [pltpu.VMEM((256, LANES), F32), pltpu.VMEM((64, LANES), F32), pltpu.VMEM((256, LANES), F32)],
    )(fourth, first, moved)

    def back_to_rows(array):
        return array.reshape(32, HIGHS, 2, LANES).transpose(0, 2, 1, 3).reshape(32, 2, RIGHT)

    return back_to_rows(new_factor), back_to_rows(new_velocity)


def solution(mesh):
    split = Mesh(mesh.devices.reshape(8, 2, 4, 4), ("z", "core", "y", "x"))
    every = ("z", "core", "y", "x")
    return jax.shard_map(
        shards,
        mesh=split,
        in_specs=(P(COL, None, None), P(None, None, every), P(SET, None), P(SET, None)),
        out_specs=(P(None, None, every), P(None, None, every)),
        check_vma=False,
    )
```

```python
import functools

import jax
import jax.numpy as jnp
from jax import lax
from jax.experimental import pallas as pl
from jax.experimental.pallas import tpu as pltpu
from jax.sharding import Mesh
from jax.sharding import PartitionSpec as P

QA, QB, QUBITS = 8, 9, 17
ORDER = 2**QUBITS
LEFT, RIGHT = 2**QA, 2**QB
LANES = 128
HIGHS = RIGHT // LANES
ROWS = ORDER // LANES
COLS = 16
SETS = 16
ZS = 8

COL = ("y", "x")
SET = ("z", "core")

mixing = 0.1
penalty = 8.0
momentum = 0.9
step_size = 0.5
count_norm = 8.0

F32 = jnp.float32
BF16 = jnp.bfloat16
HIGH = lax.Precision.HIGHEST
PCHUNK = ROWS // COLS
P1 = PCHUNK + 1
MESSAGE = 17
PEERS = 128
VMEM = pl.BlockSpec(memory_space=pltpu.VMEM)
SMEM = pl.BlockSpec(memory_space=pltpu.SMEM)


def halves(x):
    high = x.astype(BF16)
    return high, (x - high.astype(F32)).astype(BF16)


def masks_of(labels_ref):
    rotated_bits = jnp.int32(0)
    y_bits = jnp.int32(0)
    scale = jnp.float32(1.0)
    for q in range(QUBITS):
        label = labels_ref[0, q]
        bit = jnp.int32(1 << (QUBITS - 1 - q))
        rotated_bits = rotated_bits + jnp.where(label == 2, 0, bit)
        y_bits = y_bits + jnp.where(label == 1, bit, 0)
        scale = scale * jnp.where(label == 2, jnp.float32(1.0), jnp.float32(0.5))
    return rotated_bits, y_bits, scale


def hadamard(row, size, bits):
    col = lax.broadcasted_iota(jnp.int32, row.shape, 1)
    odd = lax.population_count(row & col & bits) & 1
    same = ((row ^ col) & (size - 1 - bits)) == 0
    return jnp.where(same, (1 - 2 * odd).astype(F32), 0.0).astype(BF16)


def quarter_turns(row, high, y_bits):
    lane = lax.broadcasted_iota(jnp.int32, row.shape, 1)
    index = row * RIGHT + high * LANES + lane
    return lax.population_count(index & y_bits) & 3


def forward_kernel(labels_ref, factor_ref, rotated_ref, send_ref, xh, xl, th, tl, prob, hb):
    set_index = lax.axis_index("z") * 2 + lax.axis_index("core")
    bits, y_bits, scale = masks_of(labels_ref)
    a_bits, b_bits = bits >> QB, bits & (RIGHT - 1)
    hb[...] = hadamard(lax.broadcasted_iota(jnp.int32, (RIGHT, RIGHT), 0), RIGHT, b_bits)
    ha = hadamard(lax.broadcasted_iota(jnp.int32, (LEFT, LEFT), 0), LEFT, a_bits)
    row = lax.broadcasted_iota(jnp.int32, (LEFT, LANES), 0)
    for high in range(HIGHS):
        turns = quarter_turns(row, high, y_bits)
        swap = (turns & 1) == 1
        sign_real = jnp.where(turns >= 2, -1.0, 1.0)
        sign_imag = jnp.where((turns == 1) | (turns == 2), -1.0, 1.0)
        block = pl.ds(high * LANES, LANES)
        for r in range(2):
            real = factor_ref[r, pl.ds(2 * high, LEFT, stride=2 * HIGHS), :]
            imag = factor_ref[r, pl.ds(2 * high + 1, LEFT, stride=2 * HIGHS), :]
            for c, turned in (
                (0, sign_real * jnp.where(swap, imag, real)),
                (1, sign_imag * jnp.where(swap, real, imag)),
            ):
                xh[2 * r + c, :, block], xl[2 * r + c, :, block] = halves(turned)
    prob[...] = jnp.zeros_like(prob)

    def one(i, carry):
        for n in range(2):
            part = pl.ds(n * 256, 256)
            first = jnp.dot(ha, xh[i, :, part], preferred_element_type=F32) + jnp.dot(
                ha, xl[i, :, part], preferred_element_type=F32
            )
            th[:, part], tl[:, part] = halves(first)
        for n in range(2):
            part = pl.ds(n * 256, 256)
            second = jnp.dot(th[...], hb[:, part], preferred_element_type=F32) + jnp.dot(
                tl[...], hb[:, part], preferred_element_type=F32
            )
            rotated_ref[i, :, part] = second
            prob[:, part] += second * second
        return carry

    lax.fori_loop(0, 4, one, 0)
    for c in range(COLS):
        for high in range(HIGHS):
            send_ref[c, pl.ds(16 * high, 16), :] = (
                prob[pl.ds(16 * c, 16), pl.ds(high * LANES, LANES)] * scale
            )
        start = pl.multiple_of(set_index * (ROWS * 2 // SETS) + 8 * c, 8)
        for r in range(2):
            send_ref[c, pl.ds(PCHUNK + 8 * r, 8), :] = factor_ref[r, pl.ds(start, 8), :]


def summed_kernel(got_ref, send_ref, rows):
    total = got_ref[0, pl.ds(0, PCHUNK), :]
    for c in range(1, COLS):
        total = total + got_ref[c, pl.ds(0, PCHUNK), :]
    for c in range(COLS):
        rows[pl.ds(16 * c, 16), :] = got_ref[c, pl.ds(PCHUNK, 16), :]
    parts = jnp.concatenate(parts_of(rows), axis=0)
    gram = lax.dot_general(
        parts, parts, (((1,), (1,)), ((), ())), precision=HIGH, preferred_element_type=F32
    )
    turn = quarter_turn()
    turned = jnp.dot(turn, gram, precision=HIGH, preferred_element_type=F32)
    turned = lax.dot_general(
        turned, turn, (((1,), (1,)), ((), ())), precision=HIGH, preferred_element_type=F32
    )
    rows[pl.ds(0, 32), :] = jnp.zeros((32, LANES), F32)
    rows[pl.ds(0, 32), pl.ds(0, 64)] = (gram + turned)[:32]
    pairs = rows[pl.ds(0, 16, stride=2), :] + pltpu.roll(rows[pl.ds(1, 16, stride=2), :], 64, 1)
    for c in range(COLS):
        send_ref[pl.ds(P1 * c, PCHUNK), :] = total
    send_ref[pl.ds(PCHUNK, 16, stride=P1), :] = pairs


def quarter_turn():
    i = lax.broadcasted_iota(jnp.int32, (64, 64), 0)
    j = lax.broadcasted_iota(jnp.int32, (64, 64), 1)
    return jnp.where(j == i + 32, -1.0, jnp.where(j == i - 32, 1.0, 0.0)).astype(F32)


def parts_of(rows):
    return tuple(
        jnp.concatenate(
            [rows[pl.ds(2 * high + c, 32, stride=2 * HIGHS), :] for high in range(HIGHS)], axis=1
        )
        for c in range(2)
    )


def back_kernel(labels_ref, got_ref, rotated_ref, counts_ref, keep_ref, send_ref, weight, wh, wl, th, tl, hb):
    core = lax.axis_index("core")
    bits, y_bits, scale = masks_of(labels_ref)
    a_bits, b_bits = bits >> QB, bits & (RIGHT - 1)
    hb[...] = hadamard(lax.broadcasted_iota(jnp.int32, (RIGHT, RIGHT), 0), RIGHT, b_bits)

    def owners(shape):
        i = lax.broadcasted_iota(jnp.int32, shape, 0)
        half, z, own = i >> 7, (i >> 4) & 7, i & 15
        return z * 32 + (half ^ core) * 16 + own

    ha = hadamard(owners((LEFT, LEFT)), LEFT, a_bits)
    total = jnp.zeros((PCHUNK, LANES), F32)
    gram = jnp.zeros((1, LANES), F32)
    for c in range(COLS):
        total = total + got_ref[pl.ds(P1 * c, PCHUNK), :]
        gram = gram + got_ref[pl.ds(P1 * c + PCHUNK, 1), :]
    trace = jnp.sum(total)
    slope = (1.0 - mixing) / trace
    ratio_sum = jnp.zeros((16, LANES), F32)
    for high in range(HIGHS):
        count = counts_ref[pl.ds(high, LEFT, stride=HIGHS), :].astype(F32)
        for c in range(COLS):
            p = got_ref[pl.ds(P1 * c + 16 * high, 16), :]
            w = count[16 * c : 16 * c + 16] / ((count_norm * ORDER) * (slope * p + mixing / ORDER))
            weight[pl.ds(16 * c, 16), pl.ds(high * LANES, LANES)] = w
            ratio_sum = ratio_sum + w * p
    ratio = jnp.sum(ratio_sum) / trace

    def one(i, carry):
        for n in range(2):
            part = pl.ds(n * 256, 256)
            wh[:, part], wl[:, part] = halves(
                (weight[:, part] - ratio) * scale * rotated_ref[i, :, part]
            )
        for n in range(2):
            part = pl.ds(n * 256, 256)
            first = jnp.dot(wh[...], hb[:, part], preferred_element_type=F32) + jnp.dot(
                wl[...], hb[:, part], preferred_element_type=F32
            )
            th[i, :, part], tl[i, :, part] = halves(first)
        return carry

    lax.fori_loop(0, 4, one, 0)
    row = owners((LEFT, LANES))
    for high in range(HIGHS):
        turns = quarter_turns(row, high, y_bits)
        swap = (turns & 1) == 1
        sign_real = jnp.where((turns == 1) | (turns == 2), -1.0, 1.0)
        sign_imag = jnp.where(turns >= 2, -1.0, 1.0)
        block = pl.ds(high * LANES, LANES)
        for r in range(2):
            real, imag = (
                jnp.dot(ha, th[2 * r + c, :, block], preferred_element_type=F32)
                + jnp.dot(ha, tl[2 * r + c, :, block], preferred_element_type=F32)
                for c in range(2)
            )
            for c, turned in (
                (0, sign_real * jnp.where(swap, imag, real)),
                (1, sign_imag * jnp.where(swap, real, imag)),
            ):
                for half, out in ((0, keep_ref), (1, send_ref)):
                    out[pl.ds(8 * r + 2 * high + c, PEERS, stride=MESSAGE), :] = turned[
                        PEERS * half : PEERS * (half + 1)
                    ]
    for out in (keep_ref, send_ref):
        out[pl.ds(16, PEERS, stride=MESSAGE), :] = jnp.broadcast_to(gram, (PEERS, LANES))


def update_kernel(got_ref, first_ref, velocity_ref, new_factor_ref, new_velocity_ref, rows, sums, gram_ref, mixed_ref):
    block = COLS * MESSAGE
    total = got_ref[pl.ds(0, block), :]
    for z in range(1, ZS):
        total = total + got_ref[pl.ds(block * z, block), :]
    sums[...] = total
    for c in range(COLS):
        rows[pl.ds(16 * c, 16), :] = first_ref[c, pl.ds(PCHUNK, 16), :]
    pairs = sums[pl.ds(16, 16, stride=MESSAGE), :]
    gram_ref[pl.ds(0, 16, stride=2), :] = pairs
    gram_ref[pl.ds(1, 16, stride=2), :] = pltpu.roll(pairs, 64, 1)
    gram = gram_ref[:, pl.ds(0, 64)]
    i = lax.broadcasted_iota(jnp.int32, (32, 64), 0)
    j = lax.broadcasted_iota(jnp.int32, (32, 64), 1)
    trace = jnp.sum(jnp.where(i == j, gram, 0.0))
    purity = jnp.sum(gram * gram) / (trace * trace)
    real, imag = parts_of(rows)
    for c, parts in ((0, (real, imag)), (1, (imag, -real))):
        mixed = jnp.dot(
            gram, jnp.concatenate(parts, axis=0), precision=HIGH, preferred_element_type=F32
        )
        for high in range(HIGHS):
            mixed_ref[pl.ds(2 * high + c, 32, stride=2 * HIGHS), :] = mixed[
                :, high * LANES : (high + 1) * LANES
            ]
    for c in range(COLS):
        at = pl.ds(16 * c, 16)
        own = rows[at, :]
        gradient = -((1.0 - mixing) / SETS) * sums[pl.ds(MESSAGE * c, 16), :] + penalty * (
            2.0 * mixed_ref[at, :] / trace - 2.0 * purity * own
        )
        velocity = momentum * velocity_ref[at, :] + gradient
        new_velocity_ref[at, :] = velocity
        new_factor_ref[at, :] = own - step_size * velocity


def shape(*dims):
    return jax.ShapeDtypeStruct(dims, F32)


def call(kernel, name, out, n_in, scratch=(), scalars=0):
    return pl.pallas_call(
        kernel,
        name=name,
        out_shape=out,
        in_specs=[SMEM] * scalars + [VMEM] * (n_in - scalars),
        out_specs=jax.tree.map(lambda _: VMEM, out),
        scratch_shapes=list(scratch),
        compiler_params=pltpu.CompilerParams(vmem_limit_bytes=48 * 2**20),
    )


def exchange(array, axis):
    return lax.all_to_all(array, axis, split_axis=0, concat_axis=0, tiled=True)


def exchange_flat(array, axis, peers):
    return exchange(array.reshape(peers, 1, -1), axis).reshape(array.shape)


def shards(factor, velocity, labels, counts):
    own = factor.reshape(2, 2, ROWS, LANES).transpose(0, 2, 1, 3).reshape(2, 2 * ROWS, LANES)
    counted = counts.reshape(ROWS, LANES)
    moved = velocity.reshape(32, 2, HIGHS, LANES).transpose(0, 2, 1, 3).reshape(256, LANES)
    matrix = (LEFT, RIGHT)
    rotated, sent = call(
        forward_kernel,
        "forward",
        (shape(4, *matrix), shape(COLS, PCHUNK + 16, LANES)),
        2,
        [
            pltpu.VMEM((4, *matrix), BF16),
            pltpu.VMEM((4, *matrix), BF16),
            pltpu.VMEM(matrix, BF16),
            pltpu.VMEM(matrix, BF16),
            pltpu.VMEM(matrix, F32),
            pltpu.VMEM((RIGHT, RIGHT), BF16),
        ],
        scalars=1,
    )(labels, own)
    first = exchange(sent, COL)
    sent = call(
        summed_kernel, "summed", shape(COLS * P1, LANES), 1, [pltpu.VMEM((256, LANES), F32)]
    )(first)
    second = exchange_flat(sent, COL, COLS)
    kept, sent = call(
        back_kernel,
        "back",
        (shape(PEERS * MESSAGE, LANES), shape(PEERS * MESSAGE, LANES)),
        4,
        [
            pltpu.VMEM(matrix, F32),
            pltpu.VMEM(matrix, BF16),
            pltpu.VMEM(matrix, BF16),
            pltpu.VMEM((4, *matrix), BF16),
            pltpu.VMEM((4, *matrix), BF16),
            pltpu.VMEM((RIGHT, RIGHT), BF16),
        ],
        scalars=1,
    )(labels, second, rotated, counted)
    pair = kept + lax.ppermute(sent, "core", [(0, 1), (1, 0)])
    third = exchange_flat(pair, ("z", *COL), PEERS)
    new_factor, new_velocity = call(
        update_kernel,
        "update",
        (shape(256, LANES), shape(256, LANES)),
        3,
        [
            pltpu.VMEM((256, LANES), F32),
            pltpu.VMEM((COLS * MESSAGE, LANES), F32),
            pltpu.VMEM((32, LANES), F32),
            pltpu.VMEM((256, LANES), F32),
        ],
    )(third, first, moved)

    def back_to_rows(array):
        return array.reshape(32, HIGHS, 2, LANES).transpose(0, 2, 1, 3).reshape(32, 2, RIGHT)

    return back_to_rows(new_factor), back_to_rows(new_velocity)


def solution(mesh):
    split = Mesh(mesh.devices.reshape(8, 2, 4, 4), ("z", "core", "y", "x"))
    every = ("z", "core", "y", "x")
    return jax.shard_map(
        shards,
        mesh=split,
        in_specs=(P(COL, None, None), P(None, None, every), P(SET, None), P(SET, None)),
        out_specs=(P(None, None, every), P(None, None, every)),
        check_vma=False,
    )
```

```python
import functools

import jax
import jax.numpy as jnp
from jax import lax
from jax.experimental import pallas as pl
from jax.experimental.pallas import tpu as pltpu
from jax.sharding import Mesh
from jax.sharding import PartitionSpec as P

QA, QB, QUBITS = 8, 9, 17
ORDER = 2**QUBITS
LEFT, RIGHT = 2**QA, 2**QB
LANES = 128
HIGHS = RIGHT // LANES
ROWS = ORDER // LANES
COLS = 16
SETS = 16
PAIRS = 4

COL = ("y", "x")
SET = ("zh", "zl", "core")

mixing = 0.1
penalty = 8.0
momentum = 0.9
step_size = 0.5
count_norm = 8.0

F32 = jnp.float32
BF16 = jnp.bfloat16
HIGH = lax.Precision.HIGHEST
PCHUNK = ROWS // COLS
P1 = PCHUNK + 1
MESSAGE = 17
PEERS = 64
VMEM = pl.BlockSpec(memory_space=pltpu.VMEM)
SMEM = pl.BlockSpec(memory_space=pltpu.SMEM)
HBM = pl.BlockSpec(memory_space=pltpu.HBM)


def halves(x):
    high = x.astype(BF16)
    return high, (x - high.astype(F32)).astype(BF16)


def two_pass(high, low, matrix):
    return jnp.dot(high, matrix, preferred_element_type=F32) + jnp.dot(
        low, matrix, preferred_element_type=F32
    )


def masks_of(labels_ref):
    rotated_bits = jnp.int32(0)
    y_bits = jnp.int32(0)
    scale = jnp.float32(1.0)
    for q in range(QUBITS):
        label = labels_ref[0, q]
        bit = jnp.int32(1 << (QUBITS - 1 - q))
        rotated_bits = rotated_bits + jnp.where(label == 2, 0, bit)
        y_bits = y_bits + jnp.where(label == 1, bit, 0)
        scale = scale * jnp.where(label == 2, jnp.float32(1.0), jnp.float32(0.5))
    return rotated_bits, y_bits, scale


def tall(tile, rows):
    return jnp.concatenate([tile] * (rows // 8), axis=0)


def store_hadamard(ref, size, bits):
    row = lax.broadcasted_iota(jnp.int32, (LANES, LANES), 0)
    col = lax.broadcasted_iota(jnp.int32, (LANES, LANES), 1)
    lower = tall(bits & (LANES - 1), LANES)
    odd = lax.population_count(row & col & lower) & 1
    same = ((row ^ col) & (LANES - 1 - lower)) == 0
    block = jnp.where(same, (1 - 2 * odd).astype(F32), 0.0)
    count = size // LANES
    signs = {}
    for t in range(2):
        here = ((bits >> (7 + t)) & 1).astype(F32)
        signs[t] = {(0, 0): 1.0, (0, 1): here, (1, 0): here, (1, 1): 1.0 - 2.0 * here}
    for i in range(count):
        for j in range(count):
            sign = signs[0][i & 1, j & 1] * signs[1][i >> 1, j >> 1] * jnp.ones((8, LANES), F32)
            ref[pl.ds(LANES * i, LANES), pl.ds(LANES * j, LANES)] = (
                block * tall(sign, LANES)
            ).astype(BF16)


STEP = 64


def forward_kernel(labels_hbm, factor_hbm, rotated_ref, send_ref, masks_ref, scale_ref, labels_ref, factor_ref, xh, xl, th, tl, prob, ha, hb, sems):
    copies = [
        pltpu.make_async_copy(labels_hbm, labels_ref, sems.at[0]),
        pltpu.make_async_copy(factor_hbm, factor_ref, sems.at[1]),
    ]
    for copy in copies:
        copy.start()
    set_index = (lax.axis_index("zh") * 2 + lax.axis_index("zl")) * 2 + lax.axis_index("core")
    copies[0].wait()
    bits, y_bits, scale = masks_of(labels_ref)
    masks_ref[0] = jnp.full((8, LANES), bits, jnp.int32)
    masks_ref[1] = jnp.full((8, LANES), y_bits, jnp.int32)
    scale_ref[...] = jnp.full((8, LANES), scale, F32)
    store_hadamard(hb, RIGHT, masks_ref[0] & (RIGHT - 1))
    store_hadamard(ha, LEFT, masks_ref[0] >> QB)
    prob[...] = jnp.zeros_like(prob)
    copies[1].wait()
    lane = lax.broadcasted_iota(jnp.int32, (8, LANES), 1)

    def turned(step, carry):
        row = lax.broadcasted_iota(jnp.int32, (STEP, LANES), 0) + step * STEP
        left_turns = lax.population_count((row * RIGHT) & y_bits)
        to = pl.ds(pl.multiple_of(step * STEP, STEP), STEP)
        for high in range(HIGHS):
            right_turns = lax.population_count((lane + high * LANES) & y_bits)
            turns = (left_turns + jnp.concatenate([right_turns] * (STEP // 8), axis=0)) & 3
            swap = (turns & 1) == 1
            sign_real = jnp.where(turns >= 2, -1.0, 1.0)
            sign_imag = jnp.where(((turns + 1) & 2) == 2, -1.0, 1.0)
            block = pl.ds(high * LANES, LANES)
            for r in range(2):
                real, imag = (
                    factor_ref[r, pl.ds(step * (STEP * 8) + 2 * high + c, STEP, stride=8), :]
                    for c in range(2)
                )
                for c, value in (
                    (0, sign_real * jnp.where(swap, imag, real)),
                    (1, sign_imag * jnp.where(swap, real, imag)),
                ):
                    xh[2 * r + c, to, block], xl[2 * r + c, to, block] = halves(value)
        return carry

    lax.fori_loop(0, LEFT // STEP, turned, 0)

    def one(i, carry):
        for n in range(2):
            part = pl.ds(n * 256, 256)
            first = jnp.dot(ha[...], xh[i, :, part], preferred_element_type=F32) + jnp.dot(
                ha[...], xl[i, :, part], preferred_element_type=F32
            )
            th[:, part], tl[:, part] = halves(first)
        for n in range(2):
            part = pl.ds(n * 256, 256)
            second = two_pass(th[...], tl[...], hb[:, part])
            rotated_ref[i, :, part] = second
            prob[:, part] += second * second
        return carry

    lax.fori_loop(0, 4, one, 0)
    for c in range(COLS):
        for high in range(HIGHS):
            send_ref[c, pl.ds(16 * high, 16), :] = (
                prob[pl.ds(16 * c, 16), pl.ds(high * LANES, LANES)] * scale
            )
        start = pl.multiple_of(set_index * (ROWS * 2 // SETS) + 8 * c, 8)
        for r in range(2):
            send_ref[c, pl.ds(PCHUNK + 8 * r, 8), :] = factor_ref[r, pl.ds(start, 8), :]


def prepare(masks_ref, scale_ref, ha_ref, hb_ref, cosine_ref, sine_ref, ha):
    core, parity = lax.axis_index("core"), lax.axis_index("zl")
    bits, y_bits = masks_ref[0], masks_ref[1]
    store_hadamard(hb_ref, RIGHT, bits & (RIGHT - 1))
    store_hadamard(ha, LEFT, bits >> QB)
    lane = lax.broadcasted_iota(jnp.int32, (8, LANES), 1)
    row = lax.broadcasted_iota(jnp.int32, (16, LANES), 0)
    right_turns = [
        tall(lax.population_count((lane + high * LANES) & y_bits), 16) for high in range(HIGHS)
    ]
    y_tall, scale = tall(y_bits, 16), tall(scale_ref[...], 16)
    for half in range(2):
        for kept in range(2):
            for pair in range(PAIRS):
                z = 2 * pair + (parity ^ kept)
                start = pl.multiple_of(z * 32 + (core ^ half) * 16, 16)
                at = 128 * half + 64 * kept + 16 * pair
                ha_ref[pl.ds(at, 16), :] = ha[pl.ds(start, 16), :]
                left_turns = lax.population_count(((row + start) * RIGHT) & y_tall)
                for high in range(HIGHS):
                    turns = (left_turns + right_turns[high]) & 3
                    to = pl.ds(high * LANES, LANES)
                    signed = jnp.where(turns >= 2, -scale, scale)
                    odd = (turns & 1) == 1
                    cosine_ref[pl.ds(at, 16), to] = jnp.where(odd, 0.0, signed)
                    sine_ref[pl.ds(at, 16), to] = jnp.where(odd, signed, 0.0)


def parts_of(rows):
    return tuple(
        jnp.concatenate(
            [rows[pl.ds(2 * high + c, 32, stride=2 * HIGHS), :] for high in range(HIGHS)], axis=1
        )
        for c in range(2)
    )


def summed_kernel(got_ref, send_ref, rows):
    total = got_ref[0, pl.ds(0, PCHUNK), :]
    for c in range(1, COLS):
        total = total + got_ref[c, pl.ds(0, PCHUNK), :]
    for c in range(COLS):
        rows[pl.ds(16 * c, 16), :] = got_ref[c, pl.ds(PCHUNK, 16), :]
    parts = jnp.concatenate(parts_of(rows), axis=0)
    gram = lax.dot_general(
        parts, parts, (((1,), (1,)), ((), ())), precision=HIGH, preferred_element_type=F32
    )
    turn = quarter_turn()
    turned = jnp.dot(turn, gram, precision=HIGH, preferred_element_type=F32)
    turned = lax.dot_general(
        turned, turn, (((1,), (1,)), ((), ())), precision=HIGH, preferred_element_type=F32
    )
    rows[pl.ds(0, 32), :] = jnp.zeros((32, LANES), F32)
    rows[pl.ds(0, 32), pl.ds(0, 64)] = (gram + turned)[:32]
    pairs = rows[pl.ds(0, 16, stride=2), :] + pltpu.roll(rows[pl.ds(1, 16, stride=2), :], 64, 1)
    for c in range(COLS):
        send_ref[pl.ds(P1 * c, PCHUNK), :] = total
    send_ref[pl.ds(PCHUNK, 16, stride=P1), :] = pairs


def quarter_turn():
    i = lax.broadcasted_iota(jnp.int32, (64, 64), 0)
    j = lax.broadcasted_iota(jnp.int32, (64, 64), 1)
    return jnp.where(j == i + 32, -1.0, jnp.where(j == i - 32, 1.0, 0.0)).astype(F32)


def unrotated(r, weight_ref, rotated_ref, ha_ref, hb_ref, cosine_ref, sine_ref, keep_ref, send_ref, wh, wl, th, tl):
    for c in range(2):
        for n in range(2):
            part = pl.ds(n * 256, 256)
            wh[:, part], wl[:, part] = halves(weight_ref[:, part] * rotated_ref[2 * r + c, :, part])
        for n in range(2):
            part = pl.ds(n * 256, 256)
            th[c, :, part], tl[c, :, part] = halves(two_pass(wh[...], wl[...], hb_ref[:, part]))
    for high in range(HIGHS):
        block = pl.ds(high * LANES, LANES)
        real, imag = (
            jnp.dot(ha_ref[...], th[c, :, block], preferred_element_type=F32)
            + jnp.dot(ha_ref[...], tl[c, :, block], preferred_element_type=F32)
            for c in range(2)
        )
        cosine, sine = cosine_ref[:, block], sine_ref[:, block]
        for c, value in ((0, cosine * real - sine * imag), (1, cosine * imag + sine * real)):
            for half, out in ((0, keep_ref), (1, send_ref)):
                for kept in range(2):
                    at = 128 * half + 64 * kept
                    out[kept, 2 * high + c] = value[at : at + 64]


def back_first_kernel(got_ref, counts_ref, rotated_ref, masks_ref, scale_ref, keep_ref, send_ref, weight_ref, ha_ref, hb_ref, cosine_ref, sine_ref, wh, wl, th, tl, ha):
    prepare(masks_ref, scale_ref, ha_ref, hb_ref, cosine_ref, sine_ref, ha)
    total = jnp.zeros((PCHUNK, LANES), F32)
    gram = jnp.zeros((1, LANES), F32)
    for c in range(COLS):
        total = total + got_ref[pl.ds(P1 * c, PCHUNK), :]
        gram = gram + got_ref[pl.ds(P1 * c + PCHUNK, 1), :]
    trace = jnp.sum(total)
    slope = (1.0 - mixing) / trace
    ratio_sum = jnp.zeros((16, LANES), F32)
    for c in range(COLS):
        for high in range(HIGHS):
            count = counts_ref[pl.ds(64 * c + high, 16, stride=HIGHS), :].astype(F32)
            p = got_ref[pl.ds(P1 * c + 16 * high, 16), :]
            w = count / ((slope * p + mixing / ORDER) * (count_norm * ORDER))
            weight_ref[pl.ds(16 * c, 16), pl.ds(high * LANES, LANES)] = w
            ratio_sum = ratio_sum + w * p
    weight_ref[...] = weight_ref[...] - jnp.sum(ratio_sum) / trace
    unrotated(0, weight_ref, rotated_ref, ha_ref, hb_ref, cosine_ref, sine_ref, keep_ref, send_ref, wh, wl, th, tl)
    for out in (keep_ref, send_ref):
        for kept in range(2):
            out[kept, 8] = jnp.broadcast_to(gram, (PEERS, LANES))


def back_second_kernel(weight_ref, *refs):
    unrotated(1, weight_ref, *refs)


def merged_kernel(mine_a, got_a, mine_b, got_b, send_ref):
    for j in range(8):
        send_ref[pl.ds(j, PEERS, stride=MESSAGE), :] = mine_a[j] + got_a[j]
        send_ref[pl.ds(8 + j, PEERS, stride=MESSAGE), :] = mine_b[j] + got_b[j]
    send_ref[pl.ds(16, PEERS, stride=MESSAGE), :] = mine_a[8] + got_a[8]


def update_kernel(got_ref, first_ref, velocity_ref, new_factor_ref, new_velocity_ref, rows, sums, gram_ref, mixed_ref):
    block = COLS * MESSAGE
    total = got_ref[pl.ds(0, block), :]
    for pair in range(1, PAIRS):
        total = total + got_ref[pl.ds(block * pair, block), :]
    sums[...] = total
    for c in range(COLS):
        rows[pl.ds(16 * c, 16), :] = first_ref[c, pl.ds(PCHUNK, 16), :]
    pairs = sums[pl.ds(16, 16, stride=MESSAGE), :]
    gram_ref[pl.ds(0, 16, stride=2), :] = pairs
    gram_ref[pl.ds(1, 16, stride=2), :] = pltpu.roll(pairs, 64, 1)
    gram = gram_ref[:, pl.ds(0, 64)]
    i = lax.broadcasted_iota(jnp.int32, (32, 64), 0)
    j = lax.broadcasted_iota(jnp.int32, (32, 64), 1)
    trace = jnp.sum(jnp.where(i == j, gram, 0.0))
    purity = jnp.sum(gram * gram) / (trace * trace)
    real, imag = parts_of(rows)
    for c, parts in ((0, (real, imag)), (1, (imag, -real))):
        mixed = jnp.dot(
            gram, jnp.concatenate(parts, axis=0), precision=HIGH, preferred_element_type=F32
        )
        for high in range(HIGHS):
            mixed_ref[pl.ds(2 * high + c, 32, stride=2 * HIGHS), :] = mixed[
                :, high * LANES : (high + 1) * LANES
            ]
    for c in range(COLS):
        at = pl.ds(16 * c, 16)
        own = rows[at, :]
        gradient = -((1.0 - mixing) / SETS) * sums[pl.ds(MESSAGE * c, 16), :] + penalty * (
            2.0 * mixed_ref[at, :] / trace - 2.0 * purity * own
        )
        velocity = momentum * velocity_ref[at, :] + gradient
        new_velocity_ref[at, :] = velocity
        new_factor_ref[at, :] = own - step_size * velocity


def shape(*dims, dtype=F32):
    return jax.ShapeDtypeStruct(dims, dtype)


def call(kernel, name, out, specs, scratch=(), flops=0, moved=0, vmem=16 * 2**20):
    return pl.pallas_call(
        kernel,
        name=name,
        out_shape=out,
        in_specs=specs,
        out_specs=jax.tree.map(lambda _: VMEM, out),
        scratch_shapes=list(scratch),
        compiler_params=pltpu.CompilerParams(vmem_limit_bytes=vmem),
        cost_estimate=pl.CostEstimate(flops=flops, bytes_accessed=moved, transcendentals=0),
    )


def exchange(array, axis):
    return lax.all_to_all(array, axis, split_axis=0, concat_axis=0, tiled=True)


def exchange_flat(array, axis, peers):
    return exchange(array.reshape(peers, 1, -1), axis).reshape(array.shape)


def shards(factor, velocity, labels, counts):
    own = factor.reshape(2, 2, ROWS, LANES).transpose(0, 2, 1, 3).reshape(2, 2 * ROWS, LANES)
    moved = velocity.reshape(32, 2, HIGHS, LANES).transpose(0, 2, 1, 3).reshape(256, LANES)
    matrix = (LEFT, RIGHT)
    rotated, sent, masks, scale = call(
        forward_kernel,
        "forward",
        (
            shape(4, *matrix),
            shape(COLS, PCHUNK + 16, LANES),
            shape(2, 8, LANES, dtype=jnp.int32),
            shape(8, LANES),
        ),
        [HBM, HBM],
        [
            pltpu.SMEM((1, QUBITS), jnp.int32),
            pltpu.VMEM((2, 2 * ROWS, LANES), F32),
            pltpu.VMEM((4, *matrix), BF16),
            pltpu.VMEM((4, *matrix), BF16),
            pltpu.VMEM(matrix, BF16),
            pltpu.VMEM(matrix, BF16),
            pltpu.VMEM(matrix, F32),
            pltpu.VMEM((LEFT, LEFT), BF16),
            pltpu.VMEM((RIGHT, RIGHT), BF16),
            pltpu.SemaphoreType.DMA((2,)),
        ],
        flops=2 * 10**9,
        moved=7 * 10**6,
        vmem=int(40 * 2**20),
    )(labels, own)
    first = exchange(sent, COL)
    sent = call(
        summed_kernel,
        "summed",
        shape(COLS * P1, LANES),
        [VMEM],
        [pltpu.VMEM((256, LANES), F32)],
        flops=10**7,
        moved=10**6,
    )(first)
    second = exchange_flat(sent, COL, COLS)
    back_scratch = [
        pltpu.VMEM(matrix, BF16),
        pltpu.VMEM(matrix, BF16),
        pltpu.VMEM((2, *matrix), BF16),
        pltpu.VMEM((2, *matrix), BF16),
    ]
    keep_a, send_a, weight, *forms = call(
        back_first_kernel,
        "back_first",
        (
            shape(2, 9, PEERS, LANES),
            shape(2, 9, PEERS, LANES),
            shape(*matrix),
            shape(LEFT, LEFT, dtype=BF16),
            shape(RIGHT, RIGHT, dtype=BF16),
            shape(*matrix),
            shape(*matrix),
        ),
        [VMEM] * 5,
        [*back_scratch, pltpu.VMEM((LEFT, LEFT), BF16)],
        flops=10**9,
        moved=4 * 10**6,
    )(second, counts.reshape(ROWS, LANES), rotated, masks, scale)
    swap = [(0, 1), (1, 0)]
    got_a = lax.ppermute(send_a, "core", swap)
    keep_b, send_b = call(
        back_second_kernel,
        "back_second",
        (shape(2, 8, PEERS, LANES), shape(2, 8, PEERS, LANES)),
        [VMEM] * 6,
        back_scratch,
        flops=10**9,
        moved=4 * 10**6,
    )(weight, rotated, *forms)
    got_b = lax.ppermute(send_b, "core", swap)
    pair_a = lax.ppermute(keep_a[1] + got_a[1], "zl", swap)
    pair_b = lax.ppermute(
        keep_b[1] + got_b[1], ("zh", "zl"), [(z, (z + (1 if z % 2 else -1)) % 8) for z in range(8)]
    )
    sent = call(
        merged_kernel,
        "merged",
        shape(PEERS * MESSAGE, LANES),
        [VMEM] * 4,
        flops=10**6,
        moved=2 * 10**6,
    )(keep_a[0] + got_a[0], pair_a, keep_b[0] + got_b[0], pair_b)
    third = exchange_flat(sent, ("zh", *COL), PEERS)
    new_factor, new_velocity = call(
        update_kernel,
        "update",
        (shape(256, LANES), shape(256, LANES)),
        [VMEM] * 3,
        [
            pltpu.VMEM((256, LANES), F32),
            pltpu.VMEM((COLS * MESSAGE, LANES), F32),
            pltpu.VMEM((32, LANES), F32),
            pltpu.VMEM((256, LANES), F32),
        ],
        flops=10**7,
        moved=10**6,
    )(third, first, moved)

    def back_to_rows(array):
        return array.reshape(32, HIGHS, 2, LANES).transpose(0, 2, 1, 3).reshape(32, 2, RIGHT)

    return back_to_rows(new_factor), back_to_rows(new_velocity)


def solution(mesh):
    split = Mesh(mesh.devices.reshape(4, 2, 2, 4, 4), ("zh", "zl", "core", "y", "x"))
    every = ("zh", "zl", "core", "y", "x")
    return jax.shard_map(
        shards,
        mesh=split,
        in_specs=(P(COL, None, None), P(None, None, every), P(SET, None), P(SET, None)),
        out_specs=(P(None, None, every), P(None, None, every)),
        check_vma=False,
    )
```

```python
import functools

import jax
import jax.numpy as jnp
from jax import lax
from jax.experimental import pallas as pl
from jax.experimental.pallas import tpu as pltpu
from jax.sharding import Mesh
from jax.sharding import PartitionSpec as P

QA, QB, QUBITS = 8, 9, 17
ORDER = 2**QUBITS
LEFT, RIGHT = 2**QA, 2**QB
LANES = 128
HIGHS = RIGHT // LANES
ROWS = ORDER // LANES
COLS = 16
SETS = 16
PAIRS = 4

COL = ("y", "x")
SET = ("zh", "zl", "core")

mixing = 0.1
penalty = 8.0
momentum = 0.9
step_size = 0.5
count_norm = 8.0

F32 = jnp.float32
BF16 = jnp.bfloat16
HIGH = lax.Precision.HIGHEST
PCHUNK = ROWS // COLS
P1 = PCHUNK + 1
MESSAGE = 17
PEERS = 64
VMEM = pl.BlockSpec(memory_space=pltpu.VMEM)
SMEM = pl.BlockSpec(memory_space=pltpu.SMEM)
HBM = pl.BlockSpec(memory_space=pltpu.HBM)


def halves(x):
    high = x.astype(BF16)
    return high, (x - high.astype(F32)).astype(BF16)


def two_pass(high, low, matrix):
    return jnp.dot(high, matrix, preferred_element_type=F32) + jnp.dot(
        low, matrix, preferred_element_type=F32
    )


def masks_of(labels_ref):
    rotated_bits = jnp.int32(0)
    y_bits = jnp.int32(0)
    scale = jnp.float32(1.0)
    for q in range(QUBITS):
        label = labels_ref[0, q]
        bit = jnp.int32(1 << (QUBITS - 1 - q))
        rotated_bits = rotated_bits + jnp.where(label == 2, 0, bit)
        y_bits = y_bits + jnp.where(label == 1, bit, 0)
        scale = scale * jnp.where(label == 2, jnp.float32(1.0), jnp.float32(0.5))
    return rotated_bits, y_bits, scale


def tall(tile, rows):
    return jnp.concatenate([tile] * (rows // 8), axis=0)


def store_hadamard(ref, size, bits):
    row = lax.broadcasted_iota(jnp.int32, (LANES, LANES), 0)
    col = lax.broadcasted_iota(jnp.int32, (LANES, LANES), 1)
    lower = tall(bits & (LANES - 1), LANES)
    odd = lax.population_count(row & col & lower) & 1
    same = ((row ^ col) & (LANES - 1 - lower)) == 0
    block = jnp.where(same, (1 - 2 * odd).astype(F32), 0.0)
    count = size // LANES
    signs = {}
    for t in range(2):
        here = ((bits >> (7 + t)) & 1).astype(F32)
        signs[t] = {(0, 0): 1.0, (0, 1): here, (1, 0): here, (1, 1): 1.0 - 2.0 * here}
    for i in range(count):
        for j in range(count):
            sign = signs[0][i & 1, j & 1] * signs[1][i >> 1, j >> 1] * jnp.ones((8, LANES), F32)
            ref[pl.ds(LANES * i, LANES), pl.ds(LANES * j, LANES)] = (
                block * tall(sign, LANES)
            ).astype(BF16)


STEP = 64


def forward_kernel(labels_hbm, factor_hbm, rotated_ref, send_ref, masks_ref, scale_ref, labels_ref, factor_ref, xh, xl, th, tl, prob, ha, hb, sems):
    copies = [
        pltpu.make_async_copy(labels_hbm, labels_ref, sems.at[0]),
        pltpu.make_async_copy(factor_hbm, factor_ref, sems.at[1]),
    ]
    for copy in copies:
        copy.start()
    set_index = (lax.axis_index("zh") * 2 + lax.axis_index("zl")) * 2 + lax.axis_index("core")
    copies[0].wait()
    bits, y_bits, scale = masks_of(labels_ref)
    masks_ref[0] = jnp.full((8, LANES), bits, jnp.int32)
    masks_ref[1] = jnp.full((8, LANES), y_bits, jnp.int32)
    scale_ref[...] = jnp.full((8, LANES), scale, F32)
    store_hadamard(hb, RIGHT, masks_ref[0] & (RIGHT - 1))
    store_hadamard(ha, LEFT, masks_ref[0] >> QB)
    prob[...] = jnp.zeros_like(prob)
    copies[1].wait()
    lane = lax.broadcasted_iota(jnp.int32, (8, LANES), 1)

    def turned(step, carry):
        row = lax.broadcasted_iota(jnp.int32, (STEP, LANES), 0) + step * STEP
        left_turns = lax.population_count((row * RIGHT) & y_bits)
        to = pl.ds(pl.multiple_of(step * STEP, STEP), STEP)
        for high in range(HIGHS):
            right_turns = lax.population_count((lane + high * LANES) & y_bits)
            turns = (left_turns + jnp.concatenate([right_turns] * (STEP // 8), axis=0)) & 3
            swap = (turns & 1) == 1
            sign_real = jnp.where(turns >= 2, -1.0, 1.0)
            sign_imag = jnp.where(((turns + 1) & 2) == 2, -1.0, 1.0)
            block = pl.ds(high * LANES, LANES)
            for r in range(2):
                real, imag = (
                    factor_ref[r, pl.ds(step * (STEP * 8) + 2 * high + c, STEP, stride=8), :]
                    for c in range(2)
                )
                for c, value in (
                    (0, sign_real * jnp.where(swap, imag, real)),
                    (1, sign_imag * jnp.where(swap, real, imag)),
                ):
                    xh[2 * r + c, to, block], xl[2 * r + c, to, block] = halves(value)
        return carry

    lax.fori_loop(0, LEFT // STEP, turned, 0)

    def one(i, carry):
        for n in range(2):
            part = pl.ds(n * 256, 256)
            first = jnp.dot(ha[...], xh[i, :, part], preferred_element_type=F32) + jnp.dot(
                ha[...], xl[i, :, part], preferred_element_type=F32
            )
            th[:, part], tl[:, part] = halves(first)
        for n in range(2):
            part = pl.ds(n * 256, 256)
            second = two_pass(th[...], tl[...], hb[:, part])
            rotated_ref[i, :, part] = second
            prob[:, part] += second * second
        return carry

    lax.fori_loop(0, 4, one, 0, unroll=2)
    for c in range(COLS):
        for high in range(HIGHS):
            send_ref[c, pl.ds(16 * high, 16), :] = (
                prob[pl.ds(16 * c, 16), pl.ds(high * LANES, LANES)] * scale
            )
        start = pl.multiple_of(set_index * (ROWS * 2 // SETS) + 8 * c, 8)
        for r in range(2):
            send_ref[c, pl.ds(PCHUNK + 8 * r, 8), :] = factor_ref[r, pl.ds(start, 8), :]


def prepare(masks_ref, scale_ref, ha_ref, hb_ref, cosine_ref, sine_ref, ha):
    core, parity = lax.axis_index("core"), lax.axis_index("zl")
    bits, y_bits = masks_ref[0], masks_ref[1]
    store_hadamard(hb_ref, RIGHT, bits & (RIGHT - 1))
    store_hadamard(ha, LEFT, bits >> QB)
    lane = lax.broadcasted_iota(jnp.int32, (8, LANES), 1)
    row = lax.broadcasted_iota(jnp.int32, (16, LANES), 0)
    right_turns = [
        tall(lax.population_count((lane + high * LANES) & y_bits), 16) for high in range(HIGHS)
    ]
    y_tall, scale = tall(y_bits, 16), tall(scale_ref[...], 16)
    for half in range(2):
        for kept in range(2):
            for pair in range(PAIRS):
                z = 2 * pair + (parity ^ kept)
                start = pl.multiple_of(z * 32 + (core ^ half) * 16, 16)
                at = 128 * half + 64 * kept + 16 * pair
                ha_ref[pl.ds(at, 16), :] = ha[pl.ds(start, 16), :]
                left_turns = lax.population_count(((row + start) * RIGHT) & y_tall)
                for high in range(HIGHS):
                    turns = (left_turns + right_turns[high]) & 3
                    to = pl.ds(high * LANES, LANES)
                    signed = jnp.where(turns >= 2, -scale, scale)
                    odd = (turns & 1) == 1
                    cosine_ref[pl.ds(at, 16), to] = jnp.where(odd, 0.0, signed)
                    sine_ref[pl.ds(at, 16), to] = jnp.where(odd, signed, 0.0)


def parts_of(rows):
    return tuple(
        jnp.concatenate(
            [rows[pl.ds(2 * high + c, 32, stride=2 * HIGHS), :] for high in range(HIGHS)], axis=1
        )
        for c in range(2)
    )


def summed_kernel(got_ref, send_ref, rows):
    total = got_ref[0, pl.ds(0, PCHUNK), :]
    for c in range(1, COLS):
        total = total + got_ref[c, pl.ds(0, PCHUNK), :]
    for c in range(COLS):
        rows[pl.ds(16 * c, 16), :] = got_ref[c, pl.ds(PCHUNK, 16), :]
    real, imag = parts_of(rows)
    left_high, left_low = halves(jnp.concatenate([real, imag], axis=1))
    both = jnp.concatenate(
        [jnp.concatenate([real, imag], axis=1), jnp.concatenate([imag, -real], axis=1)], axis=0
    )
    both_high, both_low = halves(both)
    gram = sum(
        lax.dot_general(x, y, (((1,), (1,)), ((), ())), preferred_element_type=F32)
        for x, y in ((left_high, both_low), (left_low, both_high), (left_high, both_high))
    )
    rows[pl.ds(0, 32), :] = jnp.zeros((32, LANES), F32)
    rows[pl.ds(0, 32), pl.ds(0, 64)] = gram
    pairs = rows[pl.ds(0, 16, stride=2), :] + pltpu.roll(rows[pl.ds(1, 16, stride=2), :], 64, 1)
    for c in range(COLS):
        send_ref[pl.ds(P1 * c, PCHUNK), :] = total
    send_ref[pl.ds(PCHUNK, 16, stride=P1), :] = pairs


def unrotated(r, weight_ref, rotated_ref, ha_ref, hb_ref, cosine_ref, sine_ref, keep_ref, send_ref, wh, wl, th, tl):
    for c in range(2):
        for n in range(2):
            part = pl.ds(n * 256, 256)
            wh[:, part], wl[:, part] = halves(weight_ref[:, part] * rotated_ref[2 * r + c, :, part])
        for n in range(2):
            part = pl.ds(n * 256, 256)
            th[c, :, part], tl[c, :, part] = halves(two_pass(wh[...], wl[...], hb_ref[:, part]))
    for high in range(HIGHS):
        block = pl.ds(high * LANES, LANES)
        real, imag = (
            jnp.dot(ha_ref[...], th[c, :, block], preferred_element_type=F32)
            + jnp.dot(ha_ref[...], tl[c, :, block], preferred_element_type=F32)
            for c in range(2)
        )
        cosine, sine = cosine_ref[:, block], sine_ref[:, block]
        for c, value in ((0, cosine * real - sine * imag), (1, cosine * imag + sine * real)):
            for half, out in ((0, keep_ref), (1, send_ref)):
                for kept in range(2):
                    at = 128 * half + 64 * kept
                    out[kept, 2 * high + c] = value[at : at + 64]


def back_first_kernel(got_ref, counts_ref, rotated_ref, masks_ref, scale_ref, keep_ref, send_ref, weight_ref, ha_ref, hb_ref, cosine_ref, sine_ref, wh, wl, th, tl, ha):
    prepare(masks_ref, scale_ref, ha_ref, hb_ref, cosine_ref, sine_ref, ha)
    total = jnp.zeros((PCHUNK, LANES), F32)
    gram = jnp.zeros((1, LANES), F32)
    for c in range(COLS):
        total = total + got_ref[pl.ds(P1 * c, PCHUNK), :]
        gram = gram + got_ref[pl.ds(P1 * c + PCHUNK, 1), :]
    trace = jnp.sum(total)
    slope = (1.0 - mixing) / trace
    ratio_sum = jnp.zeros((16, LANES), F32)
    for c in range(COLS):
        for high in range(HIGHS):
            count = counts_ref[pl.ds(64 * c + high, 16, stride=HIGHS), :].astype(F32)
            p = got_ref[pl.ds(P1 * c + 16 * high, 16), :]
            w = count / ((slope * p + mixing / ORDER) * (count_norm * ORDER))
            weight_ref[pl.ds(16 * c, 16), pl.ds(high * LANES, LANES)] = w
            ratio_sum = ratio_sum + w * p
    weight_ref[...] = weight_ref[...] - jnp.sum(ratio_sum) / trace
    unrotated(0, weight_ref, rotated_ref, ha_ref, hb_ref, cosine_ref, sine_ref, keep_ref, send_ref, wh, wl, th, tl)
    for out in (keep_ref, send_ref):
        for kept in range(2):
            out[kept, 8] = jnp.broadcast_to(gram, (PEERS, LANES))


def back_second_kernel(weight_ref, *refs):
    unrotated(1, weight_ref, *refs)


def merged_kernel(mine_a, got_a, mine_b, got_b, send_ref):
    for j in range(8):
        send_ref[pl.ds(j, PEERS, stride=MESSAGE), :] = mine_a[j] + got_a[j]
        send_ref[pl.ds(8 + j, PEERS, stride=MESSAGE), :] = mine_b[j] + got_b[j]
    send_ref[pl.ds(16, PEERS, stride=MESSAGE), :] = mine_a[8] + got_a[8]


def update_kernel(got_ref, first_ref, velocity_ref, new_factor_ref, new_velocity_ref, rows, sums, gram_ref, mixed_ref):
    block = COLS * MESSAGE
    total = got_ref[pl.ds(0, block), :]
    for pair in range(1, PAIRS):
        total = total + got_ref[pl.ds(block * pair, block), :]
    sums[...] = total
    for c in range(COLS):
        rows[pl.ds(16 * c, 16), :] = first_ref[c, pl.ds(PCHUNK, 16), :]
    pairs = sums[pl.ds(16, 16, stride=MESSAGE), :]
    gram_ref[pl.ds(0, 16, stride=2), :] = pairs
    gram_ref[pl.ds(1, 16, stride=2), :] = pltpu.roll(pairs, 64, 1)
    gram = gram_ref[:, pl.ds(0, 64)]
    i = lax.broadcasted_iota(jnp.int32, (32, 64), 0)
    j = lax.broadcasted_iota(jnp.int32, (32, 64), 1)
    trace = jnp.sum(jnp.where(i == j, gram, 0.0))
    purity = jnp.sum(gram * gram) / (trace * trace)
    real, imag = parts_of(rows)
    for c, parts in ((0, (real, imag)), (1, (imag, -real))):
        mixed = jnp.dot(
            gram, jnp.concatenate(parts, axis=0), precision=HIGH, preferred_element_type=F32
        )
        for high in range(HIGHS):
            mixed_ref[pl.ds(2 * high + c, 32, stride=2 * HIGHS), :] = mixed[
                :, high * LANES : (high + 1) * LANES
            ]
    for c in range(COLS):
        at = pl.ds(16 * c, 16)
        own = rows[at, :]
        gradient = -((1.0 - mixing) / SETS) * sums[pl.ds(MESSAGE * c, 16), :] + penalty * (
            2.0 * mixed_ref[at, :] / trace - 2.0 * purity * own
        )
        velocity = momentum * velocity_ref[at, :] + gradient
        new_velocity_ref[at, :] = velocity
        new_factor_ref[at, :] = own - step_size * velocity


def shape(*dims, dtype=F32):
    return jax.ShapeDtypeStruct(dims, dtype)


def call(kernel, name, out, specs, scratch=(), flops=0, moved=0, vmem=16 * 2**20):
    return pl.pallas_call(
        kernel,
        name=name,
        out_shape=out,
        in_specs=specs,
        out_specs=jax.tree.map(lambda _: VMEM, out),
        scratch_shapes=list(scratch),
        compiler_params=pltpu.CompilerParams(vmem_limit_bytes=vmem),
        cost_estimate=pl.CostEstimate(flops=flops, bytes_accessed=moved, transcendentals=0),
    )


def exchange(array, axis):
    return lax.all_to_all(array, axis, split_axis=0, concat_axis=0, tiled=True)


def exchange_flat(array, axis, peers):
    return exchange(array.reshape(peers, 1, -1), axis).reshape(array.shape)


def shards(factor, velocity, labels, counts):
    own = factor.reshape(2, 2, ROWS, LANES).transpose(0, 2, 1, 3).reshape(2, 2 * ROWS, LANES)
    moved = velocity.reshape(32, 2, HIGHS, LANES).transpose(0, 2, 1, 3).reshape(256, LANES)
    matrix = (LEFT, RIGHT)
    rotated, sent, masks, scale = call(
        forward_kernel,
        "forward",
        (
            shape(4, *matrix),
            shape(COLS, PCHUNK + 16, LANES),
            shape(2, 8, LANES, dtype=jnp.int32),
            shape(8, LANES),
        ),
        [HBM, HBM],
        [
            pltpu.SMEM((1, QUBITS), jnp.int32),
            pltpu.VMEM((2, 2 * ROWS, LANES), F32),
            pltpu.VMEM((4, *matrix), BF16),
            pltpu.VMEM((4, *matrix), BF16),
            pltpu.VMEM(matrix, BF16),
            pltpu.VMEM(matrix, BF16),
            pltpu.VMEM(matrix, F32),
            pltpu.VMEM((LEFT, LEFT), BF16),
            pltpu.VMEM((RIGHT, RIGHT), BF16),
            pltpu.SemaphoreType.DMA((2,)),
        ],
        flops=2 * 10**9,
        moved=7 * 10**6,
        vmem=50 * 2**20,
    )(labels, own)
    first = exchange(sent, COL)
    sent = call(
        summed_kernel,
        "summed",
        shape(COLS * P1, LANES),
        [VMEM],
        [pltpu.VMEM((256, LANES), F32)],
        flops=10**7,
        moved=10**6,
    )(first)
    second = exchange_flat(sent, COL, COLS)
    back_scratch = [
        pltpu.VMEM(matrix, BF16),
        pltpu.VMEM(matrix, BF16),
        pltpu.VMEM((2, *matrix), BF16),
        pltpu.VMEM((2, *matrix), BF16),
    ]
    keep_a, send_a, weight, *forms = call(
        back_first_kernel,
        "back_first",
        (
            shape(2, 9, PEERS, LANES),
            shape(2, 9, PEERS, LANES),
            shape(*matrix),
            shape(LEFT, LEFT, dtype=BF16),
            shape(RIGHT, RIGHT, dtype=BF16),
            shape(*matrix),
            shape(*matrix),
        ),
        [VMEM] * 5,
        [*back_scratch, pltpu.VMEM((LEFT, LEFT), BF16)],
        flops=10**9,
        moved=4 * 10**6,
    )(second, counts.reshape(ROWS, LANES), rotated, masks, scale)
    swap = [(0, 1), (1, 0)]
    got_a = lax.ppermute(send_a, "core", swap)
    keep_b, send_b = call(
        back_second_kernel,
        "back_second",
        (shape(2, 8, PEERS, LANES), shape(2, 8, PEERS, LANES)),
        [VMEM] * 6,
        back_scratch,
        flops=10**9,
        moved=4 * 10**6,
    )(weight, rotated, *forms)
    got_b = lax.ppermute(send_b, "core", swap)
    pair_a = lax.ppermute(keep_a[1] + got_a[1], "zl", swap)
    pair_b = lax.ppermute(
        keep_b[1] + got_b[1], ("zh", "zl"), [(z, (z + (1 if z % 2 else -1)) % 8) for z in range(8)]
    )
    sent = call(
        merged_kernel,
        "merged",
        shape(PEERS * MESSAGE, LANES),
        [VMEM] * 4,
        flops=10**6,
        moved=2 * 10**6,
    )(keep_a[0] + got_a[0], pair_a, keep_b[0] + got_b[0], pair_b)
    third = exchange_flat(sent, ("zh", *COL), PEERS)
    new_factor, new_velocity = call(
        update_kernel,
        "update",
        (shape(256, LANES), shape(256, LANES)),
        [VMEM] * 3,
        [
            pltpu.VMEM((256, LANES), F32),
            pltpu.VMEM((COLS * MESSAGE, LANES), F32),
            pltpu.VMEM((32, LANES), F32),
            pltpu.VMEM((256, LANES), F32),
        ],
        flops=10**7,
        moved=10**6,
    )(third, first, moved)

    def back_to_rows(array):
        return array.reshape(32, HIGHS, 2, LANES).transpose(0, 2, 1, 3).reshape(32, 2, RIGHT)

    return back_to_rows(new_factor), back_to_rows(new_velocity)


def solution(mesh):
    split = Mesh(mesh.devices.reshape(4, 2, 2, 4, 4), ("zh", "zl", "core", "y", "x"))
    every = ("zh", "zl", "core", "y", "x")
    return jax.shard_map(
        shards,
        mesh=split,
        in_specs=(P(COL, None, None), P(None, None, every), P(SET, None), P(SET, None)),
        out_specs=(P(None, None, every), P(None, None, every)),
        check_vma=False,
    )
```

```python
import functools

import jax
import jax.numpy as jnp
from jax import lax
from jax.experimental import pallas as pl
from jax.experimental.pallas import tpu as pltpu
from jax.sharding import Mesh
from jax.sharding import PartitionSpec as P

QA, QB, QUBITS = 8, 9, 17
ORDER = 2**QUBITS
LEFT, RIGHT = 2**QA, 2**QB
LANES = 128
HIGHS = RIGHT // LANES
ROWS = ORDER // LANES
COLS = 16
SETS = 16
PAIRS = 4

COL = ("y", "x")
SET = ("zh", "zl", "core")

mixing = 0.1
penalty = 8.0
momentum = 0.9
step_size = 0.5
count_norm = 8.0

F32 = jnp.float32
BF16 = jnp.bfloat16
HIGH = lax.Precision.HIGHEST
PCHUNK = ROWS // COLS
P1 = PCHUNK + 1
MESSAGE = 17
PEERS = 64
VMEM = pl.BlockSpec(memory_space=pltpu.VMEM)
SMEM = pl.BlockSpec(memory_space=pltpu.SMEM)
HBM = pl.BlockSpec(memory_space=pltpu.HBM)


def halves(x):
    high = x.astype(BF16)
    return high, (x - high.astype(F32)).astype(BF16)


def two_pass(high, low, matrix):
    return jnp.dot(high, matrix, preferred_element_type=F32) + jnp.dot(
        low, matrix, preferred_element_type=F32
    )


def masks_of(labels_ref):
    rotated_bits = jnp.int32(0)
    y_bits = jnp.int32(0)
    scale = jnp.float32(1.0)
    for q in range(QUBITS):
        label = labels_ref[0, q]
        bit = jnp.int32(1 << (QUBITS - 1 - q))
        rotated_bits = rotated_bits + jnp.where(label == 2, 0, bit)
        y_bits = y_bits + jnp.where(label == 1, bit, 0)
        scale = scale * jnp.where(label == 2, jnp.float32(1.0), jnp.float32(0.5))
    return rotated_bits, y_bits, scale


def tall(tile, rows):
    return jnp.concatenate([tile] * (rows // 8), axis=0)


def store_hadamard(ref, size, bits):
    row = lax.broadcasted_iota(jnp.int32, (LANES, LANES), 0)
    col = lax.broadcasted_iota(jnp.int32, (LANES, LANES), 1)
    lower = tall(bits & (LANES - 1), LANES)
    odd = lax.population_count(row & col & lower) & 1
    same = ((row ^ col) & (LANES - 1 - lower)) == 0
    block = jnp.where(same, (1 - 2 * odd).astype(F32), 0.0)
    count = size // LANES
    signs = {}
    for t in range(2):
        here = ((bits >> (7 + t)) & 1).astype(F32)
        signs[t] = {(0, 0): 1.0, (0, 1): here, (1, 0): here, (1, 1): 1.0 - 2.0 * here}
    for i in range(count):
        for j in range(count):
            sign = signs[0][i & 1, j & 1] * signs[1][i >> 1, j >> 1] * jnp.ones((8, LANES), F32)
            ref[pl.ds(LANES * i, LANES), pl.ds(LANES * j, LANES)] = (
                block * tall(sign, LANES)
            ).astype(BF16)


def crossed(left, right, bit):
    return left + bit * right, bit * left + (1.0 - 2.0 * bit) * right


STEP = 64
HALF = RIGHT // 2


def forward_kernel(labels_hbm, factor_hbm, rotated_ref, send_ref, masks_ref, scale_ref, labels_ref, factor_ref, xh, xl, th, tl, prob, ha, hb, sems):
    def fetch(step):
        rows = pl.ds(pl.multiple_of(step * (STEP * 8), STEP * 8), STEP * 8)
        return pltpu.make_async_copy(factor_hbm.at[:, rows], factor_ref.at[:, rows], sems.at[step])

    fetched = pltpu.make_async_copy(labels_hbm, labels_ref, sems.at[LEFT // STEP])
    fetched.start()
    for step in range(LEFT // STEP):
        fetch(step).start()
    set_index = (lax.axis_index("zh") * 2 + lax.axis_index("zl")) * 2 + lax.axis_index("core")
    fetched.wait()
    bits, y_bits, scale = masks_of(labels_ref)
    masks_ref[0] = jnp.full((8, LANES), bits, jnp.int32)
    masks_ref[1] = jnp.full((8, LANES), y_bits, jnp.int32)
    scale_ref[...] = jnp.full((8, LANES), scale, F32)
    store_hadamard(hb, HALF, masks_ref[0] & (HALF - 1))
    store_hadamard(ha, LEFT, masks_ref[0] >> QB)
    top = ((bits >> (QB - 1)) & 1).astype(F32)
    prob[...] = jnp.zeros_like(prob)
    lane = lax.broadcasted_iota(jnp.int32, (8, LANES), 1)

    def turned(step, carry):
        fetch(step).wait()
        row = lax.broadcasted_iota(jnp.int32, (STEP, LANES), 0) + step * STEP
        left_turns = lax.population_count((row * RIGHT) & y_bits)
        to = pl.ds(pl.multiple_of(step * STEP, STEP), STEP)
        values = {}
        for high in (0, 2, 1, 3):
            right_turns = lax.population_count((lane + high * LANES) & y_bits)
            turns = (left_turns + tall(right_turns, STEP)) & 3
            swap = (turns & 1) == 1
            sign_real = jnp.where(turns >= 2, -1.0, 1.0)
            sign_imag = jnp.where(((turns + 1) & 2) == 2, -1.0, 1.0)
            for r in range(2):
                real, imag = (
                    factor_ref[r, pl.ds(step * (STEP * 8) + 2 * high + c, STEP, stride=8), :]
                    for c in range(2)
                )
                values[high, 2 * r] = sign_real * jnp.where(swap, imag, real)
                values[high, 2 * r + 1] = sign_imag * jnp.where(swap, real, imag)
            if high >= 2:
                for i in range(4):
                    pair = crossed(values[high - 2, i], values[high, i], top)
                    for at, value in zip((high - 2, high), pair):
                        block = pl.ds(at * LANES, LANES)
                        xh[i, to, block], xl[i, to, block] = halves(value)
        return carry

    lax.fori_loop(0, LEFT // STEP, turned, 0)

    def one(i, carry):
        for n in range(2):
            part = pl.ds(n * 256, 256)
            first = jnp.dot(ha[...], xh[i, :, part], preferred_element_type=F32) + jnp.dot(
                ha[...], xl[i, :, part], preferred_element_type=F32
            )
            th[:, part], tl[:, part] = halves(first)
        for n in range(2):
            part = pl.ds(n * 256, 256)
            second = two_pass(th[:, part], tl[:, part], hb[...])
            rotated_ref[i, :, part] = second
            prob[:, part] += second * second
        return carry

    lax.fori_loop(0, 4, one, 0, unroll=4)
    for c in range(COLS):
        for high in range(HIGHS):
            send_ref[c, pl.ds(16 * high, 16), :] = (
                prob[pl.ds(16 * c, 16), pl.ds(high * LANES, LANES)] * scale
            )
        start = pl.multiple_of(set_index * (ROWS * 2 // SETS) + 8 * c, 8)
        for r in range(2):
            send_ref[c, pl.ds(PCHUNK + 8 * r, 8), :] = factor_ref[r, pl.ds(start, 8), :]


def prepare(masks_ref, scale_ref, ha_ref, hb_ref, cosine_ref, sine_ref, ha):
    core, parity = lax.axis_index("core"), lax.axis_index("zl")
    bits, y_bits = masks_ref[0], masks_ref[1]
    store_hadamard(hb_ref, HALF, bits & (HALF - 1))
    store_hadamard(ha, LEFT, bits >> QB)
    lane = lax.broadcasted_iota(jnp.int32, (8, LANES), 1)
    row = lax.broadcasted_iota(jnp.int32, (16, LANES), 0)
    right_turns = [
        tall(lax.population_count((lane + high * LANES) & y_bits), 16) for high in range(HIGHS)
    ]
    y_tall, scale = tall(y_bits, 16), tall(scale_ref[...], 16)
    for half in range(2):
        for kept in range(2):
            for pair in range(PAIRS):
                z = 2 * pair + (parity ^ kept)
                start = pl.multiple_of(z * 32 + (core ^ half) * 16, 16)
                at = 128 * half + 64 * kept + 16 * pair
                ha_ref[pl.ds(at, 16), :] = ha[pl.ds(start, 16), :]
                left_turns = lax.population_count(((row + start) * RIGHT) & y_tall)
                for high in range(HIGHS):
                    turns = (left_turns + right_turns[high]) & 3
                    to = pl.ds(high * LANES, LANES)
                    signed = jnp.where(turns >= 2, -scale, scale)
                    odd = (turns & 1) == 1
                    cosine_ref[pl.ds(at, 16), to] = jnp.where(odd, 0.0, signed)
                    sine_ref[pl.ds(at, 16), to] = jnp.where(odd, signed, 0.0)


def parts_of(rows):
    return tuple(
        jnp.concatenate(
            [rows[pl.ds(2 * high + c, 32, stride=2 * HIGHS), :] for high in range(HIGHS)], axis=1
        )
        for c in range(2)
    )


def summed_kernel(got_ref, send_ref, rows):
    total = got_ref[0, pl.ds(0, PCHUNK), :]
    for c in range(1, COLS):
        total = total + got_ref[c, pl.ds(0, PCHUNK), :]
    for c in range(COLS):
        rows[pl.ds(16 * c, 16), :] = got_ref[c, pl.ds(PCHUNK, 16), :]
    real, imag = parts_of(rows)
    left_high, left_low = halves(jnp.concatenate([real, imag], axis=1))
    both = jnp.concatenate(
        [jnp.concatenate([real, imag], axis=1), jnp.concatenate([imag, -real], axis=1)], axis=0
    )
    both_high, both_low = halves(both)
    gram = sum(
        lax.dot_general(x, y, (((1,), (1,)), ((), ())), preferred_element_type=F32)
        for x, y in ((left_high, both_low), (left_low, both_high), (left_high, both_high))
    )
    rows[pl.ds(0, 32), :] = jnp.zeros((32, LANES), F32)
    rows[pl.ds(0, 32), pl.ds(0, 64)] = gram
    pairs = rows[pl.ds(0, 16, stride=2), :] + pltpu.roll(rows[pl.ds(1, 16, stride=2), :], 64, 1)
    for c in range(COLS):
        send_ref[pl.ds(P1 * c, PCHUNK), :] = total
    send_ref[pl.ds(PCHUNK, 16, stride=P1), :] = pairs


def unrotated(r, weight_ref, rotated_ref, masks_ref, ha_ref, hb_ref, cosine_ref, sine_ref, keep_ref, send_ref, wh, wl, th, tl):
    top = ((masks_ref[0] >> (QB - 1)) & 1).astype(F32)[:1, :1]
    for c in range(2):
        for n in range(2):
            parts = [pl.ds(n * LANES, LANES), pl.ds(HALF + n * LANES, LANES)]
            pair = crossed(
                *(weight_ref[:, part] * rotated_ref[2 * r + c, :, part] for part in parts), top
            )
            for part, value in zip(parts, pair):
                wh[:, part], wl[:, part] = halves(value)
        for n in range(2):
            part = pl.ds(n * HALF, HALF)
            th[c, :, part], tl[c, :, part] = halves(two_pass(wh[:, part], wl[:, part], hb_ref[...]))
    for high in range(HIGHS):
        block = pl.ds(high * LANES, LANES)
        real, imag = (
            jnp.dot(ha_ref[...], th[c, :, block], preferred_element_type=F32)
            + jnp.dot(ha_ref[...], tl[c, :, block], preferred_element_type=F32)
            for c in range(2)
        )
        cosine, sine = cosine_ref[:, block], sine_ref[:, block]
        for c, value in ((0, cosine * real - sine * imag), (1, cosine * imag + sine * real)):
            for half, out in ((0, keep_ref), (1, send_ref)):
                for kept in range(2):
                    at = 128 * half + 64 * kept
                    out[kept, 2 * high + c] = value[at : at + 64]


def back_first_kernel(got_ref, counts_ref, rotated_ref, masks_ref, scale_ref, keep_ref, send_ref, weight_ref, ha_ref, hb_ref, cosine_ref, sine_ref, wh, wl, th, tl, ha):
    prepare(masks_ref, scale_ref, ha_ref, hb_ref, cosine_ref, sine_ref, ha)
    total = jnp.zeros((PCHUNK, LANES), F32)
    gram = jnp.zeros((1, LANES), F32)
    for c in range(COLS):
        total = total + got_ref[pl.ds(P1 * c, PCHUNK), :]
        gram = gram + got_ref[pl.ds(P1 * c + PCHUNK, 1), :]
    trace = jnp.sum(total)
    slope = (1.0 - mixing) / trace
    ratio_sum = jnp.zeros((16, LANES), F32)
    for c in range(COLS):
        for high in range(HIGHS):
            count = counts_ref[pl.ds(64 * c + high, 16, stride=HIGHS), :].astype(F32)
            p = got_ref[pl.ds(P1 * c + 16 * high, 16), :]
            w = count / ((slope * p + mixing / ORDER) * (count_norm * ORDER))
            weight_ref[pl.ds(16 * c, 16), pl.ds(high * LANES, LANES)] = w
            ratio_sum = ratio_sum + w * p
    weight_ref[...] = weight_ref[...] - jnp.sum(ratio_sum) / trace
    unrotated(0, weight_ref, rotated_ref, masks_ref, ha_ref, hb_ref, cosine_ref, sine_ref, keep_ref, send_ref, wh, wl, th, tl)
    for out in (keep_ref, send_ref):
        for kept in range(2):
            out[kept, 8] = jnp.broadcast_to(gram, (PEERS, LANES))


def back_second_kernel(weight_ref, *refs):
    unrotated(1, weight_ref, *refs)


def merged_kernel(mine_a, got_a, mine_b, got_b, send_ref):
    for j in range(8):
        send_ref[pl.ds(j, PEERS, stride=MESSAGE), :] = mine_a[j] + got_a[j]
        send_ref[pl.ds(8 + j, PEERS, stride=MESSAGE), :] = mine_b[j] + got_b[j]
    send_ref[pl.ds(16, PEERS, stride=MESSAGE), :] = mine_a[8] + got_a[8]


def update_kernel(got_ref, first_ref, velocity_ref, new_factor_ref, new_velocity_ref, rows, sums, gram_ref, mixed_ref):
    block = COLS * MESSAGE
    total = got_ref[pl.ds(0, block), :]
    for pair in range(1, PAIRS):
        total = total + got_ref[pl.ds(block * pair, block), :]
    sums[...] = total
    for c in range(COLS):
        rows[pl.ds(16 * c, 16), :] = first_ref[c, pl.ds(PCHUNK, 16), :]
    pairs = sums[pl.ds(16, 16, stride=MESSAGE), :]
    gram_ref[pl.ds(0, 16, stride=2), :] = pairs
    gram_ref[pl.ds(1, 16, stride=2), :] = pltpu.roll(pairs, 64, 1)
    gram = gram_ref[:, pl.ds(0, 64)]
    i = lax.broadcasted_iota(jnp.int32, (32, 64), 0)
    j = lax.broadcasted_iota(jnp.int32, (32, 64), 1)
    trace = jnp.sum(jnp.where(i == j, gram, 0.0))
    purity = jnp.sum(gram * gram) / (trace * trace)
    real, imag = parts_of(rows)
    for c, parts in ((0, (real, imag)), (1, (imag, -real))):
        mixed = jnp.dot(
            gram, jnp.concatenate(parts, axis=0), precision=HIGH, preferred_element_type=F32
        )
        for high in range(HIGHS):
            mixed_ref[pl.ds(2 * high + c, 32, stride=2 * HIGHS), :] = mixed[
                :, high * LANES : (high + 1) * LANES
            ]
    for c in range(COLS):
        at = pl.ds(16 * c, 16)
        own = rows[at, :]
        gradient = -((1.0 - mixing) / SETS) * sums[pl.ds(MESSAGE * c, 16), :] + penalty * (
            2.0 * mixed_ref[at, :] / trace - 2.0 * purity * own
        )
        velocity = momentum * velocity_ref[at, :] + gradient
        new_velocity_ref[at, :] = velocity
        new_factor_ref[at, :] = own - step_size * velocity


def shape(*dims, dtype=F32):
    return jax.ShapeDtypeStruct(dims, dtype)


def call(kernel, name, out, specs, scratch=(), flops=0, moved=0, vmem=16 * 2**20):
    return pl.pallas_call(
        kernel,
        name=name,
        out_shape=out,
        in_specs=specs,
        out_specs=jax.tree.map(lambda _: VMEM, out),
        scratch_shapes=list(scratch),
        compiler_params=pltpu.CompilerParams(vmem_limit_bytes=vmem),
        cost_estimate=pl.CostEstimate(flops=flops, bytes_accessed=moved, transcendentals=0),
    )


def exchange(array, axis):
    return lax.all_to_all(array, axis, split_axis=0, concat_axis=0, tiled=True)


def exchange_flat(array, axis, peers):
    return exchange(array.reshape(peers, 1, -1), axis).reshape(array.shape)


def shards(factor, velocity, labels, counts):
    own = factor.reshape(2, 2, ROWS, LANES).transpose(0, 2, 1, 3).reshape(2, 2 * ROWS, LANES)
    moved = velocity.reshape(32, 2, HIGHS, LANES).transpose(0, 2, 1, 3).reshape(256, LANES)
    matrix = (LEFT, RIGHT)
    rotated, sent, masks, scale = call(
        forward_kernel,
        "forward",
        (
            shape(4, *matrix),
            shape(COLS, PCHUNK + 16, LANES),
            shape(2, 8, LANES, dtype=jnp.int32),
            shape(8, LANES),
        ),
        [HBM, HBM],
        [
            pltpu.SMEM((1, QUBITS), jnp.int32),
            pltpu.VMEM((2, 2 * ROWS, LANES), F32),
            pltpu.VMEM((4, *matrix), BF16),
            pltpu.VMEM((4, *matrix), BF16),
            pltpu.VMEM(matrix, BF16),
            pltpu.VMEM(matrix, BF16),
            pltpu.VMEM(matrix, F32),
            pltpu.VMEM((LEFT, LEFT), BF16),
            pltpu.VMEM((HALF, HALF), BF16),
            pltpu.SemaphoreType.DMA((LEFT // STEP + 1,)),
        ],
        flops=2 * 10**9,
        moved=7 * 10**6,
        vmem=50 * 2**20,
    )(labels, own)
    first = exchange(sent, COL)
    sent = call(
        summed_kernel,
        "summed",
        shape(COLS * P1, LANES),
        [VMEM],
        [pltpu.VMEM((256, LANES), F32)],
        flops=10**7,
        moved=10**6,
    )(first)
    second = exchange_flat(sent, COL, COLS)
    back_scratch = [
        pltpu.VMEM(matrix, BF16),
        pltpu.VMEM(matrix, BF16),
        pltpu.VMEM((2, *matrix), BF16),
        pltpu.VMEM((2, *matrix), BF16),
    ]
    keep_a, send_a, weight, *forms = call(
        back_first_kernel,
        "back_first",
        (
            shape(2, 9, PEERS, LANES),
            shape(2, 9, PEERS, LANES),
            shape(*matrix),
            shape(LEFT, LEFT, dtype=BF16),
            shape(HALF, HALF, dtype=BF16),
            shape(*matrix),
            shape(*matrix),
        ),
        [VMEM] * 5,
        [*back_scratch, pltpu.VMEM((LEFT, LEFT), BF16)],
        flops=10**9,
        moved=4 * 10**6,
    )(second, counts.reshape(ROWS, LANES), rotated, masks, scale)
    swap = [(0, 1), (1, 0)]
    got_a = lax.ppermute(send_a, "core", swap)
    keep_b, send_b = call(
        back_second_kernel,
        "back_second",
        (shape(2, 8, PEERS, LANES), shape(2, 8, PEERS, LANES)),
        [VMEM] * 7,
        back_scratch,
        flops=10**9,
        moved=4 * 10**6,
    )(weight, rotated, masks, *forms)
    got_b = lax.ppermute(send_b, "core", swap)
    pair_a = lax.ppermute(keep_a[1] + got_a[1], "zl", swap)
    pair_b = lax.ppermute(
        keep_b[1] + got_b[1], ("zh", "zl"), [(z, (z + (1 if z % 2 else -1)) % 8) for z in range(8)]
    )
    sent = call(
        merged_kernel,
        "merged",
        shape(PEERS * MESSAGE, LANES),
        [VMEM] * 4,
        flops=10**6,
        moved=2 * 10**6,
    )(keep_a[0] + got_a[0], pair_a, keep_b[0] + got_b[0], pair_b)
    third = exchange_flat(sent, ("zh", *COL), PEERS)
    new_factor, new_velocity = call(
        update_kernel,
        "update",
        (shape(256, LANES), shape(256, LANES)),
        [VMEM] * 3,
        [
            pltpu.VMEM((256, LANES), F32),
            pltpu.VMEM((COLS * MESSAGE, LANES), F32),
            pltpu.VMEM((32, LANES), F32),
            pltpu.VMEM((256, LANES), F32),
        ],
        flops=10**7,
        moved=10**6,
    )(third, first, moved)

    def back_to_rows(array):
        return array.reshape(32, HIGHS, 2, LANES).transpose(0, 2, 1, 3).reshape(32, 2, RIGHT)

    return back_to_rows(new_factor), back_to_rows(new_velocity)


def solution(mesh):
    split = Mesh(mesh.devices.reshape(4, 2, 2, 4, 4), ("zh", "zl", "core", "y", "x"))
    every = ("zh", "zl", "core", "y", "x")
    return jax.shard_map(
        shards,
        mesh=split,
        in_specs=(P(COL, None, None), P(None, None, every), P(SET, None), P(SET, None)),
        out_specs=(P(None, None, every), P(None, None, every)),
        check_vma=False,
    )
```

```python
import functools

import jax
import jax.numpy as jnp
from jax import lax
from jax.experimental import pallas as pl
from jax.experimental.pallas import tpu as pltpu
from jax.sharding import Mesh
from jax.sharding import PartitionSpec as P

QA, QB, QUBITS = 8, 9, 17
ORDER = 2**QUBITS
LEFT, RIGHT = 2**QA, 2**QB
LANES = 128
HIGHS = RIGHT // LANES
ROWS = ORDER // LANES
COLS = 16
SETS = 16
PAIRS = 4

COL = ("y", "x")
SET = ("zh", "zl", "core")

mixing = 0.1
penalty = 8.0
momentum = 0.9
step_size = 0.5
count_norm = 8.0

F32 = jnp.float32
BF16 = jnp.bfloat16
HIGH = lax.Precision.HIGHEST
PCHUNK = ROWS // COLS
P1 = PCHUNK + 1
MESSAGE = 17
PEERS = 64
VMEM = pl.BlockSpec(memory_space=pltpu.VMEM)
SMEM = pl.BlockSpec(memory_space=pltpu.SMEM)
HBM = pl.BlockSpec(memory_space=pltpu.HBM)


def halves(x):
    high = x.astype(BF16)
    return high, (x - high.astype(F32)).astype(BF16)


def two_pass(high, low, matrix):
    return jnp.dot(high, matrix, preferred_element_type=F32) + jnp.dot(
        low, matrix, preferred_element_type=F32
    )


def masks_of(labels_ref):
    rotated_bits = jnp.int32(0)
    y_bits = jnp.int32(0)
    scale = jnp.float32(1.0)
    for q in range(QUBITS):
        label = labels_ref[0, q]
        bit = jnp.int32(1 << (QUBITS - 1 - q))
        rotated_bits = rotated_bits + jnp.where(label == 2, 0, bit)
        y_bits = y_bits + jnp.where(label == 1, bit, 0)
        scale = scale * jnp.where(label == 2, jnp.float32(1.0), jnp.float32(0.5))
    return rotated_bits, y_bits, scale


def tall(tile, rows):
    return jnp.concatenate([tile] * (rows // 8), axis=0)


def store_hadamard(ref, size, bits):
    row = lax.broadcasted_iota(jnp.int32, (LANES, LANES), 0)
    col = lax.broadcasted_iota(jnp.int32, (LANES, LANES), 1)
    lower = tall(bits & (LANES - 1), LANES)
    odd = lax.population_count(row & col & lower) & 1
    same = ((row ^ col) & (LANES - 1 - lower)) == 0
    block = jnp.where(same, (1 - 2 * odd).astype(F32), 0.0)
    count = size // LANES
    signs = {}
    for t in range(2):
        here = ((bits >> (7 + t)) & 1).astype(F32)
        signs[t] = {(0, 0): 1.0, (0, 1): here, (1, 0): here, (1, 1): 1.0 - 2.0 * here}
    for i in range(count):
        for j in range(count):
            sign = signs[0][i & 1, j & 1] * signs[1][i >> 1, j >> 1] * jnp.ones((8, LANES), F32)
            ref[pl.ds(LANES * i, LANES), pl.ds(LANES * j, LANES)] = (
                block * tall(sign, LANES)
            ).astype(BF16)


def crossed(left, right, bit):
    return left + bit * right, bit * left + (1.0 - 2.0 * bit) * right


STEP = 32
HALF = RIGHT // 2


def forward_kernel(labels_hbm, factor_hbm, rotated_ref, send_ref, masks_ref, scale_ref, labels_ref, factor_ref, xh, xl, th, tl, prob, ha, hb, sems):
    def fetch(step):
        rows = pl.ds(pl.multiple_of(step * (STEP * 8), STEP * 8), STEP * 8)
        return pltpu.make_async_copy(factor_hbm.at[:, rows], factor_ref.at[:, rows], sems.at[step])

    fetched = pltpu.make_async_copy(labels_hbm, labels_ref, sems.at[LEFT // STEP])
    fetched.start()
    for step in range(LEFT // STEP):
        fetch(step).start()
    set_index = (lax.axis_index("zh") * 2 + lax.axis_index("zl")) * 2 + lax.axis_index("core")
    fetched.wait()
    bits, y_bits, scale = masks_of(labels_ref)
    masks_ref[0] = jnp.full((8, LANES), bits, jnp.int32)
    masks_ref[1] = jnp.full((8, LANES), y_bits, jnp.int32)
    scale_ref[...] = jnp.full((8, LANES), scale, F32)
    store_hadamard(hb, HALF, masks_ref[0] & (HALF - 1))
    store_hadamard(ha, LEFT, masks_ref[0] >> QB)
    top = ((bits >> (QB - 1)) & 1).astype(F32)
    prob[...] = jnp.zeros_like(prob)
    lane = lax.broadcasted_iota(jnp.int32, (8, LANES), 1)

    def turned(step, carry):
        fetch(step).wait()
        row = lax.broadcasted_iota(jnp.int32, (STEP, LANES), 0) + step * STEP
        left_turns = lax.population_count((row * RIGHT) & y_bits)
        to = pl.ds(pl.multiple_of(step * STEP, STEP), STEP)
        values = {}
        for high in (0, 2, 1, 3):
            right_turns = lax.population_count((lane + high * LANES) & y_bits)
            turns = (left_turns + tall(right_turns, STEP)) & 3
            swap = (turns & 1) == 1
            sign_real = jnp.where(turns >= 2, -1.0, 1.0)
            sign_imag = jnp.where(((turns + 1) & 2) == 2, -1.0, 1.0)
            for r in range(2):
                real, imag = (
                    factor_ref[r, pl.ds(step * (STEP * 8) + 2 * high + c, STEP, stride=8), :]
                    for c in range(2)
                )
                values[high, 2 * r] = sign_real * jnp.where(swap, imag, real)
                values[high, 2 * r + 1] = sign_imag * jnp.where(swap, real, imag)
            if high >= 2:
                for i in range(4):
                    pair = crossed(values[high - 2, i], values[high, i], top)
                    for at, value in zip((high - 2, high), pair):
                        block = pl.ds(at * LANES, LANES)
                        xh[i, to, block], xl[i, to, block] = halves(value)
        return carry

    lax.fori_loop(0, LEFT // STEP, turned, 0)

    def one(i, carry):
        for n in range(2):
            part = pl.ds(n * 256, 256)
            first = jnp.dot(ha[...], xh[i, :, part], preferred_element_type=F32) + jnp.dot(
                ha[...], xl[i, :, part], preferred_element_type=F32
            )
            th[:, part], tl[:, part] = halves(first)
        for n in range(2):
            part = pl.ds(n * 256, 256)
            second = two_pass(th[:, part], tl[:, part], hb[...])
            rotated_ref[i, :, part] = second
            prob[:, part] += second * second
        return carry

    lax.fori_loop(0, 4, one, 0, unroll=4)
    for c in range(COLS):
        for high in range(HIGHS):
            send_ref[c, pl.ds(16 * high, 16), :] = (
                prob[pl.ds(16 * c, 16), pl.ds(high * LANES, LANES)] * scale
            )
        start = pl.multiple_of(set_index * (ROWS * 2 // SETS) + 8 * c, 8)
        for r in range(2):
            send_ref[c, pl.ds(PCHUNK + 8 * r, 8), :] = factor_ref[r, pl.ds(start, 8), :]


def prepare(masks_ref, scale_ref, ha_ref, hb_ref, cosine_ref, sine_ref, ha):
    core, parity = lax.axis_index("core"), lax.axis_index("zl")
    bits, y_bits = masks_ref[0], masks_ref[1]
    store_hadamard(hb_ref, HALF, bits & (HALF - 1))
    store_hadamard(ha, LEFT, bits >> QB)
    lane = lax.broadcasted_iota(jnp.int32, (8, LANES), 1)
    row = lax.broadcasted_iota(jnp.int32, (16, LANES), 0)
    right_turns = [
        tall(lax.population_count((lane + high * LANES) & y_bits), 16) for high in range(HIGHS)
    ]
    y_tall, scale = tall(y_bits, 16), tall(scale_ref[...], 16)
    for half in range(2):
        for kept in range(2):
            for pair in range(PAIRS):
                z = 2 * pair + (parity ^ kept)
                start = pl.multiple_of(z * 32 + (core ^ half) * 16, 16)
                at = 128 * half + 64 * kept + 16 * pair
                ha_ref[pl.ds(at, 16), :] = ha[pl.ds(start, 16), :]
                left_turns = lax.population_count(((row + start) * RIGHT) & y_tall)
                for high in range(HIGHS):
                    turns = (left_turns + right_turns[high]) & 3
                    to = pl.ds(high * LANES, LANES)
                    signed = jnp.where(turns >= 2, -scale, scale)
                    odd = (turns & 1) == 1
                    cosine_ref[pl.ds(at, 16), to] = jnp.where(odd, 0.0, signed)
                    sine_ref[pl.ds(at, 16), to] = jnp.where(odd, signed, 0.0)


def parts_of(rows):
    return tuple(
        jnp.concatenate(
            [rows[pl.ds(2 * high + c, 32, stride=2 * HIGHS), :] for high in range(HIGHS)], axis=1
        )
        for c in range(2)
    )


def summed_kernel(got_ref, send_ref, rows):
    total = got_ref[0, pl.ds(0, PCHUNK), :]
    for c in range(1, COLS):
        total = total + got_ref[c, pl.ds(0, PCHUNK), :]
    for c in range(COLS):
        rows[pl.ds(16 * c, 16), :] = got_ref[c, pl.ds(PCHUNK, 16), :]
    real, imag = parts_of(rows)
    left_high, left_low = halves(jnp.concatenate([real, imag], axis=1))
    both = jnp.concatenate(
        [jnp.concatenate([real, imag], axis=1), jnp.concatenate([imag, -real], axis=1)], axis=0
    )
    both_high, both_low = halves(both)
    gram = sum(
        lax.dot_general(x, y, (((1,), (1,)), ((), ())), preferred_element_type=F32)
        for x, y in ((left_high, both_low), (left_low, both_high), (left_high, both_high))
    )
    rows[pl.ds(0, 32), :] = jnp.zeros((32, LANES), F32)
    rows[pl.ds(0, 32), pl.ds(0, 64)] = gram
    pairs = rows[pl.ds(0, 16, stride=2), :] + pltpu.roll(rows[pl.ds(1, 16, stride=2), :], 64, 1)
    for c in range(COLS):
        send_ref[pl.ds(P1 * c, PCHUNK), :] = total
    send_ref[pl.ds(PCHUNK, 16, stride=P1), :] = pairs


def unrotated(r, weight_ref, rotated_ref, masks_ref, ha_ref, hb_ref, cosine_ref, sine_ref, keep_ref, send_ref, wh, wl, th, tl):
    top = ((masks_ref[0] >> (QB - 1)) & 1).astype(F32)[:1, :1]
    for c in range(2):
        for n in range(2):
            parts = [pl.ds(n * LANES, LANES), pl.ds(HALF + n * LANES, LANES)]
            pair = crossed(
                *(weight_ref[:, part] * rotated_ref[2 * r + c, :, part] for part in parts), top
            )
            for part, value in zip(parts, pair):
                wh[:, part], wl[:, part] = halves(value)
        for n in range(2):
            part = pl.ds(n * HALF, HALF)
            th[c, :, part], tl[c, :, part] = halves(two_pass(wh[:, part], wl[:, part], hb_ref[...]))
    for n in range(2):
        part = pl.ds(n * HALF, HALF)
        real, imag = (
            jnp.dot(ha_ref[...], th[c, :, part], preferred_element_type=F32)
            + jnp.dot(ha_ref[...], tl[c, :, part], preferred_element_type=F32)
            for c in range(2)
        )
        cosine, sine = cosine_ref[:, part], sine_ref[:, part]
        for c, value in ((0, cosine * real - sine * imag), (1, cosine * imag + sine * real)):
            for half, out in ((0, keep_ref), (1, send_ref)):
                for kept in range(2):
                    at = 128 * half + 64 * kept
                    for k in range(2):
                        out[kept, 4 * n + 2 * k + c] = value[
                            at : at + 64, k * LANES : (k + 1) * LANES
                        ]


def back_first_kernel(got_ref, counts_ref, rotated_ref, masks_ref, scale_ref, keep_ref, send_ref, weight_ref, ha_ref, hb_ref, cosine_ref, sine_ref, wh, wl, th, tl, ha):
    prepare(masks_ref, scale_ref, ha_ref, hb_ref, cosine_ref, sine_ref, ha)
    total = jnp.zeros((PCHUNK, LANES), F32)
    gram = jnp.zeros((1, LANES), F32)
    for c in range(COLS):
        total = total + got_ref[pl.ds(P1 * c, PCHUNK), :]
        gram = gram + got_ref[pl.ds(P1 * c + PCHUNK, 1), :]
    trace = jnp.sum(total)
    slope = (1.0 - mixing) / trace
    ratio_sum = jnp.zeros((16, LANES), F32)
    for c in range(COLS):
        for high in range(HIGHS):
            count = counts_ref[pl.ds(64 * c + high, 16, stride=HIGHS), :].astype(F32)
            p = got_ref[pl.ds(P1 * c + 16 * high, 16), :]
            w = count / ((slope * p + mixing / ORDER) * (count_norm * ORDER))
            weight_ref[pl.ds(16 * c, 16), pl.ds(high * LANES, LANES)] = w
            ratio_sum = ratio_sum + w * p
    weight_ref[...] = weight_ref[...] - jnp.sum(ratio_sum) / trace
    unrotated(0, weight_ref, rotated_ref, masks_ref, ha_ref, hb_ref, cosine_ref, sine_ref, keep_ref, send_ref, wh, wl, th, tl)
    for out in (keep_ref, send_ref):
        for kept in range(2):
            out[kept, 8] = jnp.broadcast_to(gram, (PEERS, LANES))


def back_second_kernel(weight_ref, *refs):
    unrotated(1, weight_ref, *refs)


def merged_kernel(mine_a, got_a, mine_b, got_b, send_ref):
    for j in range(8):
        send_ref[pl.ds(j, PEERS, stride=MESSAGE), :] = mine_a[j] + got_a[j]
        send_ref[pl.ds(8 + j, PEERS, stride=MESSAGE), :] = mine_b[j] + got_b[j]
    send_ref[pl.ds(16, PEERS, stride=MESSAGE), :] = mine_a[8] + got_a[8]


def update_kernel(got_ref, first_ref, velocity_ref, new_factor_ref, new_velocity_ref, rows, sums, gram_ref, mixed_ref):
    block = COLS * MESSAGE
    total = got_ref[pl.ds(0, block), :]
    for pair in range(1, PAIRS):
        total = total + got_ref[pl.ds(block * pair, block), :]
    sums[...] = total
    for c in range(COLS):
        rows[pl.ds(16 * c, 16), :] = first_ref[c, pl.ds(PCHUNK, 16), :]
    pairs = sums[pl.ds(16, 16, stride=MESSAGE), :]
    gram_ref[pl.ds(0, 16, stride=2), :] = pairs
    gram_ref[pl.ds(1, 16, stride=2), :] = pltpu.roll(pairs, 64, 1)
    gram = gram_ref[:, pl.ds(0, 64)]
    i = lax.broadcasted_iota(jnp.int32, (32, 64), 0)
    j = lax.broadcasted_iota(jnp.int32, (32, 64), 1)
    trace = jnp.sum(jnp.where(i == j, gram, 0.0))
    purity = jnp.sum(gram * gram) / (trace * trace)
    real, imag = parts_of(rows)
    for c, parts in ((0, (real, imag)), (1, (imag, -real))):
        mixed = jnp.dot(
            gram, jnp.concatenate(parts, axis=0), precision=HIGH, preferred_element_type=F32
        )
        for high in range(HIGHS):
            mixed_ref[pl.ds(2 * high + c, 32, stride=2 * HIGHS), :] = mixed[
                :, high * LANES : (high + 1) * LANES
            ]
    for c in range(COLS):
        at = pl.ds(16 * c, 16)
        own = rows[at, :]
        gradient = -((1.0 - mixing) / SETS) * sums[pl.ds(MESSAGE * c, 16), :] + penalty * (
            2.0 * mixed_ref[at, :] / trace - 2.0 * purity * own
        )
        velocity = momentum * velocity_ref[at, :] + gradient
        new_velocity_ref[at, :] = velocity
        new_factor_ref[at, :] = own - step_size * velocity


def shape(*dims, dtype=F32):
    return jax.ShapeDtypeStruct(dims, dtype)


def call(kernel, name, out, specs, scratch=(), flops=0, moved=0, vmem=16 * 2**20):
    return pl.pallas_call(
        kernel,
        name=name,
        out_shape=out,
        in_specs=specs,
        out_specs=jax.tree.map(lambda _: VMEM, out),
        scratch_shapes=list(scratch),
        compiler_params=pltpu.CompilerParams(vmem_limit_bytes=vmem),
        cost_estimate=pl.CostEstimate(flops=flops, bytes_accessed=moved, transcendentals=0),
    )


def exchange(array, axis):
    return lax.all_to_all(array, axis, split_axis=0, concat_axis=0, tiled=True)


def exchange_flat(array, axis, peers):
    return exchange(array.reshape(peers, 1, -1), axis).reshape(array.shape)


def shards(factor, velocity, labels, counts):
    own = factor.reshape(2, 2, ROWS, LANES).transpose(0, 2, 1, 3).reshape(2, 2 * ROWS, LANES)
    moved = velocity.reshape(32, 2, HIGHS, LANES).transpose(0, 2, 1, 3).reshape(256, LANES)
    matrix = (LEFT, RIGHT)
    rotated, sent, masks, scale = call(
        forward_kernel,
        "forward",
        (
            shape(4, *matrix),
            shape(COLS, PCHUNK + 16, LANES),
            shape(2, 8, LANES, dtype=jnp.int32),
            shape(8, LANES),
        ),
        [HBM, HBM],
        [
            pltpu.SMEM((1, QUBITS), jnp.int32),
            pltpu.VMEM((2, 2 * ROWS, LANES), F32),
            pltpu.VMEM((4, *matrix), BF16),
            pltpu.VMEM((4, *matrix), BF16),
            pltpu.VMEM(matrix, BF16),
            pltpu.VMEM(matrix, BF16),
            pltpu.VMEM(matrix, F32),
            pltpu.VMEM((LEFT, LEFT), BF16),
            pltpu.VMEM((HALF, HALF), BF16),
            pltpu.SemaphoreType.DMA((LEFT // STEP + 1,)),
        ],
        flops=2 * 10**9,
        moved=7 * 10**6,
        vmem=50 * 2**20,
    )(labels, own)
    first = exchange(sent, COL)
    sent = call(
        summed_kernel,
        "summed",
        shape(COLS * P1, LANES),
        [VMEM],
        [pltpu.VMEM((256, LANES), F32)],
        flops=10**7,
        moved=10**6,
    )(first)
    second = exchange_flat(sent, COL, COLS)
    back_scratch = [
        pltpu.VMEM(matrix, BF16),
        pltpu.VMEM(matrix, BF16),
        pltpu.VMEM((2, *matrix), BF16),
        pltpu.VMEM((2, *matrix), BF16),
    ]
    keep_a, send_a, weight, *forms = call(
        back_first_kernel,
        "back_first",
        (
            shape(2, 9, PEERS, LANES),
            shape(2, 9, PEERS, LANES),
            shape(*matrix),
            shape(LEFT, LEFT, dtype=BF16),
            shape(HALF, HALF, dtype=BF16),
            shape(*matrix),
            shape(*matrix),
        ),
        [VMEM] * 5,
        [*back_scratch, pltpu.VMEM((LEFT, LEFT), BF16)],
        flops=10**9,
        moved=4 * 10**6,
    )(second, counts.reshape(ROWS, LANES), rotated, masks, scale)
    swap = [(0, 1), (1, 0)]
    got_a = lax.ppermute(send_a, "core", swap)
    keep_b, send_b = call(
        back_second_kernel,
        "back_second",
        (shape(2, 8, PEERS, LANES), shape(2, 8, PEERS, LANES)),
        [VMEM] * 7,
        back_scratch,
        flops=10**9,
        moved=4 * 10**6,
    )(weight, rotated, masks, *forms)
    got_b = lax.ppermute(send_b, "core", swap)
    pair_a = lax.ppermute(keep_a[1] + got_a[1], "zl", swap)
    pair_b = lax.ppermute(
        keep_b[1] + got_b[1], ("zh", "zl"), [(z, (z + (1 if z % 2 else -1)) % 8) for z in range(8)]
    )
    sent = call(
        merged_kernel,
        "merged",
        shape(PEERS * MESSAGE, LANES),
        [VMEM] * 4,
        flops=10**6,
        moved=2 * 10**6,
    )(keep_a[0] + got_a[0], pair_a, keep_b[0] + got_b[0], pair_b)
    third = exchange_flat(sent, ("zh", *COL), PEERS)
    new_factor, new_velocity = call(
        update_kernel,
        "update",
        (shape(256, LANES), shape(256, LANES)),
        [VMEM] * 3,
        [
            pltpu.VMEM((256, LANES), F32),
            pltpu.VMEM((COLS * MESSAGE, LANES), F32),
            pltpu.VMEM((32, LANES), F32),
            pltpu.VMEM((256, LANES), F32),
        ],
        flops=10**7,
        moved=10**6,
    )(third, first, moved)

    def back_to_rows(array):
        return array.reshape(32, HIGHS, 2, LANES).transpose(0, 2, 1, 3).reshape(32, 2, RIGHT)

    return back_to_rows(new_factor), back_to_rows(new_velocity)


def solution(mesh):
    split = Mesh(mesh.devices.reshape(4, 2, 2, 4, 4), ("zh", "zl", "core", "y", "x"))
    every = ("zh", "zl", "core", "y", "x")
    return jax.shard_map(
        shards,
        mesh=split,
        in_specs=(P(COL, None, None), P(None, None, every), P(SET, None), P(SET, None)),
        out_specs=(P(None, None, every), P(None, None, every)),
        check_vma=False,
    )
```

```python
import functools

import jax
import jax.numpy as jnp
from jax import lax
from jax.experimental import pallas as pl
from jax.experimental.pallas import tpu as pltpu
from jax.sharding import Mesh
from jax.sharding import PartitionSpec as P

QA, QB, QUBITS = 8, 9, 17
ORDER = 2**QUBITS
LEFT, RIGHT = 2**QA, 2**QB
LANES = 128
HIGHS = RIGHT // LANES
ROWS = ORDER // LANES
COLS = 16
SETS = 16
PAIRS = 4

COL = ("y", "x")
SET = ("zh", "zl", "core")

mixing = 0.1
penalty = 8.0
momentum = 0.9
step_size = 0.5
count_norm = 8.0

F32 = jnp.float32
BF16 = jnp.bfloat16
HIGH = lax.Precision.HIGHEST
PCHUNK = ROWS // COLS
P1 = PCHUNK + 1
MESSAGE = 17
PEERS = 64
VMEM = pl.BlockSpec(memory_space=pltpu.VMEM)
SMEM = pl.BlockSpec(memory_space=pltpu.SMEM)
HBM = pl.BlockSpec(memory_space=pltpu.HBM)


def halves(x):
    high = x.astype(BF16)
    return high, (x - high.astype(F32)).astype(BF16)


def two_pass(high, low, matrix):
    return jnp.dot(high, matrix, preferred_element_type=F32) + jnp.dot(
        low, matrix, preferred_element_type=F32
    )


def masks_of(labels_ref):
    rotated_bits = jnp.int32(0)
    y_bits = jnp.int32(0)
    scale = jnp.float32(1.0)
    for q in range(QUBITS):
        label = labels_ref[0, q]
        bit = jnp.int32(1 << (QUBITS - 1 - q))
        rotated_bits = rotated_bits + jnp.where(label == 2, 0, bit)
        y_bits = y_bits + jnp.where(label == 1, bit, 0)
        scale = scale * jnp.where(label == 2, jnp.float32(1.0), jnp.float32(0.5))
    return rotated_bits, y_bits, scale


def tall(tile, rows):
    return jnp.concatenate([tile] * (rows // 8), axis=0)


def store_hadamard(ref, size, bits):
    row = lax.broadcasted_iota(jnp.int32, (LANES, LANES), 0)
    col = lax.broadcasted_iota(jnp.int32, (LANES, LANES), 1)
    lower = tall(bits & (LANES - 1), LANES)
    odd = lax.population_count(row & col & lower) & 1
    same = ((row ^ col) & (LANES - 1 - lower)) == 0
    block = jnp.where(same, (1 - 2 * odd).astype(F32), 0.0)
    count = size // LANES
    signs = {}
    for t in range(2):
        here = ((bits >> (7 + t)) & 1).astype(F32)
        signs[t] = {(0, 0): 1.0, (0, 1): here, (1, 0): here, (1, 1): 1.0 - 2.0 * here}
    for i in range(count):
        for j in range(count):
            sign = signs[0][i & 1, j & 1] * signs[1][i >> 1, j >> 1] * jnp.ones((8, LANES), F32)
            ref[pl.ds(LANES * i, LANES), pl.ds(LANES * j, LANES)] = (
                block * tall(sign, LANES)
            ).astype(BF16)


def crossed(left, right, bit):
    return left + bit * right, bit * left + (1.0 - 2.0 * bit) * right


def store_tables(y_bits, scale, turned_ha_ref, cosine_ref, sine_ref, ha):
    core, parity = lax.axis_index("core"), lax.axis_index("zl")
    lane = lax.broadcasted_iota(jnp.int32, (8, LANES), 1)
    row = lax.broadcasted_iota(jnp.int32, (16, LANES), 0)
    right_turns = [
        tall(lax.population_count((lane + high * LANES) & y_bits), 16) for high in range(HIGHS)
    ]
    for half in range(2):
        for kept in range(2):
            for pair in range(PAIRS):
                z = 2 * pair + (parity ^ kept)
                start = pl.multiple_of(z * 32 + (core ^ half) * 16, 16)
                at = 128 * half + 64 * kept + 16 * pair
                turned_ha_ref[pl.ds(at, 16), :] = ha[pl.ds(start, 16), :]
                left_turns = lax.population_count(((row + start) * RIGHT) & y_bits)
                for high in range(HIGHS):
                    turns = (left_turns + right_turns[high]) & 3
                    to = pl.ds(high * LANES, LANES)
                    signed = jnp.where(turns >= 2, -scale, scale)
                    odd = (turns & 1) == 1
                    cosine_ref[pl.ds(at, 16), to] = jnp.where(odd, 0.0, signed)
                    sine_ref[pl.ds(at, 16), to] = jnp.where(odd, signed, 0.0)


STEP = 32
HALF = RIGHT // 2


def forward_kernel(labels_hbm, factor_hbm, rotated_ref, send_ref, top_ref, turned_ha_ref, hb, cosine_ref, sine_ref, labels_ref, factor_ref, xh, xl, th, tl, prob, ha, sems):
    def fetch(step):
        rows = pl.ds(pl.multiple_of(step * (STEP * 8), STEP * 8), STEP * 8)
        return pltpu.make_async_copy(factor_hbm.at[:, rows], factor_ref.at[:, rows], sems.at[step])

    fetched = pltpu.make_async_copy(labels_hbm, labels_ref, sems.at[LEFT // STEP])
    fetched.start()
    for step in range(LEFT // STEP):
        fetch(step).start()
    set_index = (lax.axis_index("zh") * 2 + lax.axis_index("zl")) * 2 + lax.axis_index("core")
    fetched.wait()
    bits, y_bits, scale = masks_of(labels_ref)
    tile = jnp.full((8, LANES), bits, jnp.int32)
    store_hadamard(hb, HALF, tile & (HALF - 1))
    store_hadamard(ha, LEFT, tile >> QB)
    top = ((bits >> (QB - 1)) & 1).astype(F32)
    top_ref[...] = jnp.full((8, LANES), top, F32)
    store_tables(y_bits, scale, turned_ha_ref, cosine_ref, sine_ref, ha)
    prob[...] = jnp.zeros_like(prob)
    lane = lax.broadcasted_iota(jnp.int32, (8, LANES), 1)

    def turned(step, carry):
        fetch(step).wait()
        row = lax.broadcasted_iota(jnp.int32, (STEP, LANES), 0) + step * STEP
        left_turns = lax.population_count((row * RIGHT) & y_bits)
        to = pl.ds(pl.multiple_of(step * STEP, STEP), STEP)
        values = {}
        for high in (0, 2, 1, 3):
            right_turns = lax.population_count((lane + high * LANES) & y_bits)
            turns = (left_turns + tall(right_turns, STEP)) & 3
            swap = (turns & 1) == 1
            sign_real = jnp.where(turns >= 2, -1.0, 1.0)
            sign_imag = jnp.where(((turns + 1) & 2) == 2, -1.0, 1.0)
            for r in range(2):
                real, imag = (
                    factor_ref[r, pl.ds(step * (STEP * 8) + 2 * high + c, STEP, stride=8), :]
                    for c in range(2)
                )
                values[high, 2 * r] = sign_real * jnp.where(swap, imag, real)
                values[high, 2 * r + 1] = sign_imag * jnp.where(swap, real, imag)
            if high >= 2:
                for i in range(4):
                    pair = crossed(values[high - 2, i], values[high, i], top)
                    for at, value in zip((high - 2, high), pair):
                        block = pl.ds(at * LANES, LANES)
                        xh[i, to, block], xl[i, to, block] = halves(value)
        return carry

    lax.fori_loop(0, LEFT // STEP, turned, 0)

    def one(i, carry):
        for n in range(2):
            part = pl.ds(n * 256, 256)
            first = jnp.dot(ha[...], xh[i, :, part], preferred_element_type=F32) + jnp.dot(
                ha[...], xl[i, :, part], preferred_element_type=F32
            )
            th[:, part], tl[:, part] = halves(first)
        for n in range(2):
            part = pl.ds(n * 256, 256)
            second = two_pass(th[:, part], tl[:, part], hb[...])
            rotated_ref[i, :, part] = second
            prob[:, part] += second * second
        return carry

    lax.fori_loop(0, 4, one, 0, unroll=4)
    for c in range(COLS):
        for high in range(HIGHS):
            send_ref[c, pl.ds(16 * high, 16), :] = (
                prob[pl.ds(16 * c, 16), pl.ds(high * LANES, LANES)] * scale
            )
        start = pl.multiple_of(set_index * (ROWS * 2 // SETS) + 8 * c, 8)
        for r in range(2):
            send_ref[c, pl.ds(PCHUNK + 8 * r, 8), :] = factor_ref[r, pl.ds(start, 8), :]


def parts_of(rows):
    return tuple(
        jnp.concatenate(
            [rows[pl.ds(2 * high + c, 32, stride=2 * HIGHS), :] for high in range(HIGHS)], axis=1
        )
        for c in range(2)
    )


def summed_kernel(got_ref, send_ref, rows):
    total = got_ref[0, pl.ds(0, PCHUNK), :]
    for c in range(1, COLS):
        total = total + got_ref[c, pl.ds(0, PCHUNK), :]
    for c in range(COLS):
        rows[pl.ds(16 * c, 16), :] = got_ref[c, pl.ds(PCHUNK, 16), :]
    real, imag = parts_of(rows)
    left_high, left_low = halves(jnp.concatenate([real, imag], axis=1))
    both = jnp.concatenate(
        [jnp.concatenate([real, imag], axis=1), jnp.concatenate([imag, -real], axis=1)], axis=0
    )
    both_high, both_low = halves(both)
    gram = sum(
        lax.dot_general(x, y, (((1,), (1,)), ((), ())), preferred_element_type=F32)
        for x, y in ((left_high, both_low), (left_low, both_high), (left_high, both_high))
    )
    rows[pl.ds(0, 32), :] = jnp.zeros((32, LANES), F32)
    rows[pl.ds(0, 32), pl.ds(0, 64)] = gram
    pairs = rows[pl.ds(0, 16, stride=2), :] + pltpu.roll(rows[pl.ds(1, 16, stride=2), :], 64, 1)
    for c in range(COLS):
        send_ref[pl.ds(P1 * c, PCHUNK), :] = total
    send_ref[pl.ds(PCHUNK, 16, stride=P1), :] = pairs


def unrotated(r, weight_ref, rotated_ref, top_ref, ha_ref, hb_ref, cosine_ref, sine_ref, keep_ref, send_ref, wh, wl, th, tl):
    top = top_ref[:1, :1]
    for c in range(2):
        for n in range(2):
            parts = [pl.ds(n * LANES, LANES), pl.ds(HALF + n * LANES, LANES)]
            pair = crossed(
                *(weight_ref[:, part] * rotated_ref[2 * r + c, :, part] for part in parts), top
            )
            for part, value in zip(parts, pair):
                wh[:, part], wl[:, part] = halves(value)
        for n in range(2):
            part = pl.ds(n * HALF, HALF)
            th[c, :, part], tl[c, :, part] = halves(two_pass(wh[:, part], wl[:, part], hb_ref[...]))
    for n in range(2):
        part = pl.ds(n * HALF, HALF)
        real, imag = (
            jnp.dot(ha_ref[...], th[c, :, part], preferred_element_type=F32)
            + jnp.dot(ha_ref[...], tl[c, :, part], preferred_element_type=F32)
            for c in range(2)
        )
        cosine, sine = cosine_ref[:, part], sine_ref[:, part]
        for c, value in ((0, cosine * real - sine * imag), (1, cosine * imag + sine * real)):
            for half, out in ((0, keep_ref), (1, send_ref)):
                for kept in range(2):
                    at = 128 * half + 64 * kept
                    for k in range(2):
                        out[kept, 4 * n + 2 * k + c] = value[
                            at : at + 64, k * LANES : (k + 1) * LANES
                        ]


def back_first_kernel(got_ref, counts_ref, rotated_ref, top_ref, ha_ref, hb_ref, cosine_ref, sine_ref, keep_ref, send_ref, weight_ref, wh, wl, th, tl):
    total = jnp.zeros((PCHUNK, LANES), F32)
    gram = jnp.zeros((1, LANES), F32)
    for c in range(COLS):
        total = total + got_ref[pl.ds(P1 * c, PCHUNK), :]
        gram = gram + got_ref[pl.ds(P1 * c + PCHUNK, 1), :]
    trace = jnp.sum(total)
    slope = (1.0 - mixing) / trace
    ratio_sum = jnp.zeros((16, LANES), F32)
    for c in range(COLS):
        for high in range(HIGHS):
            count = counts_ref[pl.ds(64 * c + high, 16, stride=HIGHS), :].astype(F32)
            p = got_ref[pl.ds(P1 * c + 16 * high, 16), :]
            w = count / ((slope * p + mixing / ORDER) * (count_norm * ORDER))
            weight_ref[pl.ds(16 * c, 16), pl.ds(high * LANES, LANES)] = w
            ratio_sum = ratio_sum + w * p
    weight_ref[...] = weight_ref[...] - jnp.sum(ratio_sum) / trace
    unrotated(0, weight_ref, rotated_ref, top_ref, ha_ref, hb_ref, cosine_ref, sine_ref, keep_ref, send_ref, wh, wl, th, tl)
    for out in (keep_ref, send_ref):
        for kept in range(2):
            out[kept, 8] = jnp.broadcast_to(gram, (PEERS, LANES))


def back_second_kernel(weight_ref, *refs):
    unrotated(1, weight_ref, *refs)


def merged_kernel(mine_a, got_a, mine_b, got_b, send_ref):
    for j in range(8):
        send_ref[pl.ds(j, PEERS, stride=MESSAGE), :] = mine_a[j] + got_a[j]
        send_ref[pl.ds(8 + j, PEERS, stride=MESSAGE), :] = mine_b[j] + got_b[j]
    send_ref[pl.ds(16, PEERS, stride=MESSAGE), :] = mine_a[8] + got_a[8]


def update_kernel(got_ref, first_ref, velocity_ref, new_factor_ref, new_velocity_ref, rows, sums, gram_ref, mixed_ref):
    block = COLS * MESSAGE
    total = got_ref[pl.ds(0, block), :]
    for pair in range(1, PAIRS):
        total = total + got_ref[pl.ds(block * pair, block), :]
    sums[...] = total
    for c in range(COLS):
        rows[pl.ds(16 * c, 16), :] = first_ref[c, pl.ds(PCHUNK, 16), :]
    pairs = sums[pl.ds(16, 16, stride=MESSAGE), :]
    gram_ref[pl.ds(0, 16, stride=2), :] = pairs
    gram_ref[pl.ds(1, 16, stride=2), :] = pltpu.roll(pairs, 64, 1)
    gram = gram_ref[:, pl.ds(0, 64)]
    i = lax.broadcasted_iota(jnp.int32, (32, 64), 0)
    j = lax.broadcasted_iota(jnp.int32, (32, 64), 1)
    trace = jnp.sum(jnp.where(i == j, gram, 0.0))
    purity = jnp.sum(gram * gram) / (trace * trace)
    real, imag = parts_of(rows)
    for c, parts in ((0, (real, imag)), (1, (imag, -real))):
        mixed = jnp.dot(
            gram, jnp.concatenate(parts, axis=0), precision=HIGH, preferred_element_type=F32
        )
        for high in range(HIGHS):
            mixed_ref[pl.ds(2 * high + c, 32, stride=2 * HIGHS), :] = mixed[
                :, high * LANES : (high + 1) * LANES
            ]
    for c in range(COLS):
        at = pl.ds(16 * c, 16)
        own = rows[at, :]
        gradient = -((1.0 - mixing) / SETS) * sums[pl.ds(MESSAGE * c, 16), :] + penalty * (
            2.0 * mixed_ref[at, :] / trace - 2.0 * purity * own
        )
        velocity = momentum * velocity_ref[at, :] + gradient
        new_velocity_ref[at, :] = velocity
        new_factor_ref[at, :] = own - step_size * velocity


def shape(*dims, dtype=F32):
    return jax.ShapeDtypeStruct(dims, dtype)


def call(kernel, name, out, specs, scratch=(), flops=0, moved=0, vmem=16 * 2**20):
    return pl.pallas_call(
        kernel,
        name=name,
        out_shape=out,
        in_specs=specs,
        out_specs=jax.tree.map(lambda _: VMEM, out),
        scratch_shapes=list(scratch),
        compiler_params=pltpu.CompilerParams(vmem_limit_bytes=vmem),
        cost_estimate=pl.CostEstimate(flops=flops, bytes_accessed=moved, transcendentals=0),
    )


def exchange(array, axis):
    return lax.all_to_all(array, axis, split_axis=0, concat_axis=0, tiled=True)


def exchange_flat(array, axis, peers):
    return exchange(array.reshape(peers, 1, -1), axis).reshape(array.shape)


def shards(factor, velocity, labels, counts):
    own = factor.reshape(2, 2, ROWS, LANES).transpose(0, 2, 1, 3).reshape(2, 2 * ROWS, LANES)
    moved = velocity.reshape(32, 2, HIGHS, LANES).transpose(0, 2, 1, 3).reshape(256, LANES)
    matrix = (LEFT, RIGHT)
    rotated, sent, *forms = call(
        forward_kernel,
        "forward",
        (
            shape(4, *matrix),
            shape(COLS, PCHUNK + 16, LANES),
            shape(8, LANES),
            shape(LEFT, LEFT, dtype=BF16),
            shape(HALF, HALF, dtype=BF16),
            shape(*matrix),
            shape(*matrix),
        ),
        [HBM, HBM],
        [
            pltpu.SMEM((1, QUBITS), jnp.int32),
            pltpu.VMEM((2, 2 * ROWS, LANES), F32),
            pltpu.VMEM((4, *matrix), BF16),
            pltpu.VMEM((4, *matrix), BF16),
            pltpu.VMEM(matrix, BF16),
            pltpu.VMEM(matrix, BF16),
            pltpu.VMEM(matrix, F32),
            pltpu.VMEM((LEFT, LEFT), BF16),
            pltpu.SemaphoreType.DMA((LEFT // STEP + 1,)),
        ],
        flops=2 * 10**9,
        moved=7 * 10**6,
    )(*(pltpu.with_memory_space_constraint(x, pltpu.HBM) for x in (labels, own)))
    first = exchange(sent, COL)
    sent = call(
        summed_kernel,
        "summed",
        shape(COLS * P1, LANES),
        [VMEM],
        [pltpu.VMEM((256, LANES), F32)],
        flops=10**7,
        moved=10**6,
    )(first)
    second = exchange_flat(sent, COL, COLS)
    back_scratch = [
        pltpu.VMEM(matrix, BF16),
        pltpu.VMEM(matrix, BF16),
        pltpu.VMEM((2, *matrix), BF16),
        pltpu.VMEM((2, *matrix), BF16),
    ]
    keep_a, send_a, weight = call(
        back_first_kernel,
        "back_first",
        (shape(2, 9, PEERS, LANES), shape(2, 9, PEERS, LANES), shape(*matrix)),
        [VMEM] * 8,
        back_scratch,
        flops=10**9,
        moved=4 * 10**6,
    )(second, counts.reshape(ROWS, LANES), rotated, *forms)
    swap = [(0, 1), (1, 0)]
    got_a = lax.ppermute(send_a, "core", swap)
    keep_b, send_b = call(
        back_second_kernel,
        "back_second",
        (shape(2, 8, PEERS, LANES), shape(2, 8, PEERS, LANES)),
        [VMEM] * 7,
        back_scratch,
        flops=10**9,
        moved=4 * 10**6,
    )(weight, rotated, *forms)
    got_b = lax.ppermute(send_b, "core", swap)
    pair_a = lax.ppermute(keep_a[1] + got_a[1], "zl", swap)
    pair_b = lax.ppermute(
        keep_b[1] + got_b[1], ("zh", "zl"), [(z, (z + (1 if z % 2 else -1)) % 8) for z in range(8)]
    )
    sent = call(
        merged_kernel,
        "merged",
        shape(PEERS * MESSAGE, LANES),
        [VMEM] * 4,
        flops=10**6,
        moved=2 * 10**6,
    )(keep_a[0] + got_a[0], pair_a, keep_b[0] + got_b[0], pair_b)
    third = exchange_flat(sent, ("zh", *COL), PEERS)
    new_factor, new_velocity = call(
        update_kernel,
        "update",
        (shape(256, LANES), shape(256, LANES)),
        [VMEM] * 3,
        [
            pltpu.VMEM((256, LANES), F32),
            pltpu.VMEM((COLS * MESSAGE, LANES), F32),
            pltpu.VMEM((32, LANES), F32),
            pltpu.VMEM((256, LANES), F32),
        ],
        flops=10**7,
        moved=10**6,
    )(third, first, moved)

    def back_to_rows(array):
        return array.reshape(32, HIGHS, 2, LANES).transpose(0, 2, 1, 3).reshape(32, 2, RIGHT)

    return back_to_rows(new_factor), back_to_rows(new_velocity)


def solution(mesh):
    split = Mesh(mesh.devices.reshape(4, 2, 2, 4, 4), ("zh", "zl", "core", "y", "x"))
    every = ("zh", "zl", "core", "y", "x")
    return jax.shard_map(
        shards,
        mesh=split,
        in_specs=(P(COL, None, None), P(None, None, every), P(SET, None), P(SET, None)),
        out_specs=(P(None, None, every), P(None, None, every)),
        check_vma=False,
    )
```

```python
import functools

import jax
import jax.numpy as jnp
from jax import lax
from jax.experimental import pallas as pl
from jax.experimental.pallas import tpu as pltpu
from jax.sharding import Mesh
from jax.sharding import PartitionSpec as P

QA, QB, QUBITS = 8, 9, 17
ORDER = 2**QUBITS
LEFT, RIGHT = 2**QA, 2**QB
LANES = 128
HIGHS = RIGHT // LANES
ROWS = ORDER // LANES
COLS = 16
SETS = 16
TOPS = 2

COL = ("y", "x")
SET = ("zt", "zm", "zl", "core")

mixing = 0.1
penalty = 8.0
momentum = 0.9
step_size = 0.5
count_norm = 8.0

F32 = jnp.float32
BF16 = jnp.bfloat16
HIGH = lax.Precision.HIGHEST
PCHUNK = ROWS // COLS
P1 = PCHUNK + 1
MESSAGE = 17
PEERS = 32
VMEM = pl.BlockSpec(memory_space=pltpu.VMEM)
SMEM = pl.BlockSpec(memory_space=pltpu.SMEM)
HBM = pl.BlockSpec(memory_space=pltpu.HBM)


def halves(x):
    high = x.astype(BF16)
    return high, (x - high.astype(F32)).astype(BF16)


def two_pass(high, low, matrix):
    return jnp.dot(high, matrix, preferred_element_type=F32) + jnp.dot(
        low, matrix, preferred_element_type=F32
    )


def masks_of(labels_ref):
    rotated_bits = jnp.int32(0)
    y_bits = jnp.int32(0)
    scale = jnp.float32(1.0)
    for q in range(QUBITS):
        label = labels_ref[0, q]
        bit = jnp.int32(1 << (QUBITS - 1 - q))
        rotated_bits = rotated_bits + jnp.where(label == 2, 0, bit)
        y_bits = y_bits + jnp.where(label == 1, bit, 0)
        scale = scale * jnp.where(label == 2, jnp.float32(1.0), jnp.float32(0.5))
    return rotated_bits, y_bits, scale


def tall(tile, rows):
    return jnp.concatenate([tile] * (rows // 8), axis=0)


def store_hadamard(ref, size, bits):
    row = lax.broadcasted_iota(jnp.int32, (LANES, LANES), 0)
    col = lax.broadcasted_iota(jnp.int32, (LANES, LANES), 1)
    lower = tall(bits & (LANES - 1), LANES)
    odd = lax.population_count(row & col & lower) & 1
    same = ((row ^ col) & (LANES - 1 - lower)) == 0
    block = jnp.where(same, (1 - 2 * odd).astype(F32), 0.0)
    count = size // LANES
    signs = {}
    for t in range(2):
        here = ((bits >> (7 + t)) & 1).astype(F32)
        signs[t] = {(0, 0): 1.0, (0, 1): here, (1, 0): here, (1, 1): 1.0 - 2.0 * here}
    for i in range(count):
        for j in range(count):
            sign = signs[0][i & 1, j & 1] * signs[1][i >> 1, j >> 1] * jnp.ones((8, LANES), F32)
            ref[pl.ds(LANES * i, LANES), pl.ds(LANES * j, LANES)] = (
                block * tall(sign, LANES)
            ).astype(BF16)


def crossed(left, right, bit):
    return left + bit * right, bit * left + (1.0 - 2.0 * bit) * right


def store_tables(y_bits, scale, turned_ha_ref, cosine_ref, sine_ref, ha):
    core = lax.axis_index("core")
    own = lax.axis_index("zm") * 2 + lax.axis_index("zl")
    lane = lax.broadcasted_iota(jnp.int32, (8, LANES), 1)
    row = lax.broadcasted_iota(jnp.int32, (16, LANES), 0)
    right_turns = [
        tall(lax.population_count((lane + high * LANES) & y_bits), 16) for high in range(HIGHS)
    ]
    for half in range(2):
        for q, place in enumerate((own, 3 - own, own ^ 1, (3 - own) ^ 1)):
            for zt in range(TOPS):
                start = pl.multiple_of((zt * 4 + place) * 32 + (core ^ half) * 16, 16)
                at = 128 * half + 32 * q + 16 * zt
                turned_ha_ref[pl.ds(at, 16), :] = ha[pl.ds(start, 16), :]
                left_turns = lax.population_count(((row + start) * RIGHT) & y_bits)
                for high in range(HIGHS):
                    turns = (left_turns + right_turns[high]) & 3
                    to = pl.ds(high * LANES, LANES)
                    signed = jnp.where(turns >= 2, -scale, scale)
                    odd = (turns & 1) == 1
                    cosine_ref[pl.ds(at, 16), to] = jnp.where(odd, 0.0, signed)
                    sine_ref[pl.ds(at, 16), to] = jnp.where(odd, signed, 0.0)


STEP = 32
HALF = RIGHT // 2


def forward_kernel(labels_hbm, factor_hbm, rotated_ref, send_ref, top_ref, turned_ha_ref, hb, cosine_ref, sine_ref, labels_ref, factor_ref, xh, xl, th, tl, prob, ha, sems):
    def fetch(step):
        rows = pl.ds(pl.multiple_of(step * (STEP * 8), STEP * 8), STEP * 8)
        return pltpu.make_async_copy(factor_hbm.at[:, rows], factor_ref.at[:, rows], sems.at[step])

    fetched = pltpu.make_async_copy(labels_hbm, labels_ref, sems.at[LEFT // STEP])
    fetched.start()
    for step in range(LEFT // STEP):
        fetch(step).start()
    set_index = lax.axis_index(SET)
    fetched.wait()
    bits, y_bits, scale = masks_of(labels_ref)
    tile = jnp.full((8, LANES), bits, jnp.int32)
    store_hadamard(hb, HALF, tile & (HALF - 1))
    store_hadamard(ha, LEFT, tile >> QB)
    top = ((bits >> (QB - 1)) & 1).astype(F32)
    top_ref[...] = jnp.full((8, LANES), top, F32)
    store_tables(y_bits, scale, turned_ha_ref, cosine_ref, sine_ref, ha)
    prob[...] = jnp.zeros_like(prob)
    lane = lax.broadcasted_iota(jnp.int32, (8, LANES), 1)

    def turned(step, carry):
        fetch(step).wait()
        row = lax.broadcasted_iota(jnp.int32, (STEP, LANES), 0) + step * STEP
        left_turns = lax.population_count((row * RIGHT) & y_bits)
        to = pl.ds(pl.multiple_of(step * STEP, STEP), STEP)
        values = {}
        for high in (0, 2, 1, 3):
            right_turns = lax.population_count((lane + high * LANES) & y_bits)
            turns = (left_turns + tall(right_turns, STEP)) & 3
            swap = (turns & 1) == 1
            sign_real = jnp.where(turns >= 2, -1.0, 1.0)
            sign_imag = jnp.where(((turns + 1) & 2) == 2, -1.0, 1.0)
            for r in range(2):
                real, imag = (
                    factor_ref[r, pl.ds(step * (STEP * 8) + 2 * high + c, STEP, stride=8), :]
                    for c in range(2)
                )
                values[high, 2 * r] = sign_real * jnp.where(swap, imag, real)
                values[high, 2 * r + 1] = sign_imag * jnp.where(swap, real, imag)
            if high >= 2:
                for i in range(4):
                    pair = crossed(values[high - 2, i], values[high, i], top)
                    for at, value in zip((high - 2, high), pair):
                        block = pl.ds(at * LANES, LANES)
                        xh[i, to, block], xl[i, to, block] = halves(value)
        return carry

    lax.fori_loop(0, LEFT // STEP, turned, 0)

    def one(i, carry):
        for n in range(2):
            part = pl.ds(n * 256, 256)
            first = jnp.dot(ha[...], xh[i, :, part], preferred_element_type=F32) + jnp.dot(
                ha[...], xl[i, :, part], preferred_element_type=F32
            )
            th[:, part], tl[:, part] = halves(first)
        for n in range(2):
            part = pl.ds(n * 256, 256)
            second = two_pass(th[:, part], tl[:, part], hb[...])
            rotated_ref[i, :, part] = second
            prob[:, part] += second * second
        return carry

    lax.fori_loop(0, 4, one, 0, unroll=4)
    for c in range(COLS):
        for high in range(HIGHS):
            send_ref[c, pl.ds(16 * high, 16), :] = (
                prob[pl.ds(16 * c, 16), pl.ds(high * LANES, LANES)] * scale
            )
        start = pl.multiple_of(set_index * (ROWS * 2 // SETS) + 8 * c, 8)
        for r in range(2):
            send_ref[c, pl.ds(PCHUNK + 8 * r, 8), :] = factor_ref[r, pl.ds(start, 8), :]


def parts_of(rows):
    return tuple(
        jnp.concatenate(
            [rows[pl.ds(2 * high + c, 32, stride=2 * HIGHS), :] for high in range(HIGHS)], axis=1
        )
        for c in range(2)
    )


def summed_kernel(got_ref, send_ref, rows):
    total = got_ref[0, pl.ds(0, PCHUNK), :]
    for c in range(1, COLS):
        total = total + got_ref[c, pl.ds(0, PCHUNK), :]
    for c in range(COLS):
        rows[pl.ds(16 * c, 16), :] = got_ref[c, pl.ds(PCHUNK, 16), :]
    real, imag = parts_of(rows)
    left_high, left_low = halves(jnp.concatenate([real, imag], axis=1))
    both = jnp.concatenate(
        [jnp.concatenate([real, imag], axis=1), jnp.concatenate([imag, -real], axis=1)], axis=0
    )
    both_high, both_low = halves(both)
    gram = sum(
        lax.dot_general(x, y, (((1,), (1,)), ((), ())), preferred_element_type=F32)
        for x, y in ((left_high, both_low), (left_low, both_high), (left_high, both_high))
    )
    rows[pl.ds(0, 32), :] = jnp.zeros((32, LANES), F32)
    rows[pl.ds(0, 32), pl.ds(0, 64)] = gram
    pairs = rows[pl.ds(0, 16, stride=2), :] + pltpu.roll(rows[pl.ds(1, 16, stride=2), :], 64, 1)
    for c in range(COLS):
        send_ref[pl.ds(P1 * c, PCHUNK), :] = total
    send_ref[pl.ds(PCHUNK, 16, stride=P1), :] = pairs


ORDERS = ((0, 1, 2, 3), (0, 2, 1, 3))


def unrotated(r, weight_ref, rotated_ref, top_ref, ha_ref, hb_ref, cosine_ref, sine_ref, keep_ref, send_ref, wh, wl, th, tl):
    top = top_ref[:1, :1]
    for c in range(2):
        for n in range(2):
            parts = [pl.ds(n * LANES, LANES), pl.ds(HALF + n * LANES, LANES)]
            pair = crossed(
                *(weight_ref[:, part] * rotated_ref[2 * r + c, :, part] for part in parts), top
            )
            for part, value in zip(parts, pair):
                wh[:, part], wl[:, part] = halves(value)
        for n in range(2):
            part = pl.ds(n * HALF, HALF)
            th[c, :, part], tl[c, :, part] = halves(two_pass(wh[:, part], wl[:, part], hb_ref[...]))
    for n in range(2):
        part = pl.ds(n * HALF, HALF)
        real, imag = (
            jnp.dot(ha_ref[...], th[c, :, part], preferred_element_type=F32)
            + jnp.dot(ha_ref[...], tl[c, :, part], preferred_element_type=F32)
            for c in range(2)
        )
        cosine, sine = cosine_ref[:, part], sine_ref[:, part]
        for c, value in ((0, cosine * real - sine * imag), (1, cosine * imag + sine * real)):
            for half, out in ((0, keep_ref), (1, send_ref)):
                for at, q in enumerate(ORDERS[r]):
                    rows = slice(128 * half + PEERS * q, 128 * half + PEERS * (q + 1))
                    for k in range(2):
                        out[at, 4 * n + 2 * k + c] = value[rows, k * LANES : (k + 1) * LANES]


def back_first_kernel(got_ref, counts_ref, rotated_ref, top_ref, ha_ref, hb_ref, cosine_ref, sine_ref, keep_ref, send_ref, weight_ref, wh, wl, th, tl):
    total = jnp.zeros((PCHUNK, LANES), F32)
    gram = jnp.zeros((1, LANES), F32)
    for c in range(COLS):
        total = total + got_ref[pl.ds(P1 * c, PCHUNK), :]
        gram = gram + got_ref[pl.ds(P1 * c + PCHUNK, 1), :]
    trace = jnp.sum(total)
    slope = (1.0 - mixing) / trace
    ratio_sum = jnp.zeros((16, LANES), F32)
    for c in range(COLS):
        for high in range(HIGHS):
            count = counts_ref[pl.ds(64 * c + high, 16, stride=HIGHS), :].astype(F32)
            p = got_ref[pl.ds(P1 * c + 16 * high, 16), :]
            w = count / ((slope * p + mixing / ORDER) * (count_norm * ORDER))
            weight_ref[pl.ds(16 * c, 16), pl.ds(high * LANES, LANES)] = w
            ratio_sum = ratio_sum + w * p
    weight_ref[...] = weight_ref[...] - jnp.sum(ratio_sum) / trace
    unrotated(0, weight_ref, rotated_ref, top_ref, ha_ref, hb_ref, cosine_ref, sine_ref, keep_ref, send_ref, wh, wl, th, tl)
    for out in (keep_ref, send_ref):
        for at in range(4):
            out[at, 8] = jnp.broadcast_to(gram, (PEERS, LANES))


def back_second_kernel(weight_ref, *refs):
    unrotated(1, weight_ref, *refs)


def merged_kernel(mine_a, got_a, mine_b, got_b, send_ref):
    for j in range(8):
        send_ref[pl.ds(j, PEERS, stride=MESSAGE), :] = mine_a[j] + got_a[j]
        send_ref[pl.ds(8 + j, PEERS, stride=MESSAGE), :] = mine_b[j] + got_b[j]
    send_ref[pl.ds(16, PEERS, stride=MESSAGE), :] = mine_a[8] + got_a[8]


def update_kernel(got_ref, first_ref, velocity_ref, new_factor_ref, new_velocity_ref, rows, sums, gram_ref, mixed_ref):
    block = COLS * MESSAGE
    total = got_ref[pl.ds(0, block), :]
    for zt in range(1, TOPS):
        total = total + got_ref[pl.ds(block * zt, block), :]
    sums[...] = total
    for c in range(COLS):
        rows[pl.ds(16 * c, 16), :] = first_ref[c, pl.ds(PCHUNK, 16), :]
    pairs = sums[pl.ds(16, 16, stride=MESSAGE), :]
    gram_ref[pl.ds(0, 16, stride=2), :] = pairs
    gram_ref[pl.ds(1, 16, stride=2), :] = pltpu.roll(pairs, 64, 1)
    gram = gram_ref[:, pl.ds(0, 64)]
    i = lax.broadcasted_iota(jnp.int32, (32, 64), 0)
    j = lax.broadcasted_iota(jnp.int32, (32, 64), 1)
    trace = jnp.sum(jnp.where(i == j, gram, 0.0))
    purity = jnp.sum(gram * gram) / (trace * trace)
    real, imag = parts_of(rows)
    for c, parts in ((0, (real, imag)), (1, (imag, -real))):
        mixed = jnp.dot(
            gram, jnp.concatenate(parts, axis=0), precision=HIGH, preferred_element_type=F32
        )
        for high in range(HIGHS):
            mixed_ref[pl.ds(2 * high + c, 32, stride=2 * HIGHS), :] = mixed[
                :, high * LANES : (high + 1) * LANES
            ]
    for c in range(COLS):
        at = pl.ds(16 * c, 16)
        own = rows[at, :]
        gradient = -((1.0 - mixing) / SETS) * sums[pl.ds(MESSAGE * c, 16), :] + penalty * (
            2.0 * mixed_ref[at, :] / trace - 2.0 * purity * own
        )
        velocity = momentum * velocity_ref[at, :] + gradient
        new_velocity_ref[at, :] = velocity
        new_factor_ref[at, :] = own - step_size * velocity


def shape(*dims, dtype=F32):
    return jax.ShapeDtypeStruct(dims, dtype)


def call(kernel, name, out, specs, scratch=(), flops=0, moved=0, vmem=16 * 2**20):
    return pl.pallas_call(
        kernel,
        name=name,
        out_shape=out,
        in_specs=specs,
        out_specs=jax.tree.map(lambda _: VMEM, out),
        scratch_shapes=list(scratch),
        compiler_params=pltpu.CompilerParams(vmem_limit_bytes=vmem),
        cost_estimate=pl.CostEstimate(flops=flops, bytes_accessed=moved, transcendentals=0),
    )


def exchange(array, axis):
    return lax.all_to_all(array, axis, split_axis=0, concat_axis=0, tiled=True)


def exchange_flat(array, axis, peers):
    return exchange(array.reshape(peers, 1, -1), axis).reshape(array.shape)


def shards(factor, velocity, labels, counts):
    own = factor.reshape(2, 2, ROWS, LANES).transpose(0, 2, 1, 3).reshape(2, 2 * ROWS, LANES)
    moved = velocity.reshape(32, 2, HIGHS, LANES).transpose(0, 2, 1, 3).reshape(256, LANES)
    matrix = (LEFT, RIGHT)
    rotated, sent, *forms = call(
        forward_kernel,
        "forward",
        (
            shape(4, *matrix),
            shape(COLS, PCHUNK + 16, LANES),
            shape(8, LANES),
            shape(LEFT, LEFT, dtype=BF16),
            shape(HALF, HALF, dtype=BF16),
            shape(*matrix),
            shape(*matrix),
        ),
        [HBM, HBM],
        [
            pltpu.SMEM((1, QUBITS), jnp.int32),
            pltpu.VMEM((2, 2 * ROWS, LANES), F32),
            pltpu.VMEM((4, *matrix), BF16),
            pltpu.VMEM((4, *matrix), BF16),
            pltpu.VMEM(matrix, BF16),
            pltpu.VMEM(matrix, BF16),
            pltpu.VMEM(matrix, F32),
            pltpu.VMEM((LEFT, LEFT), BF16),
            pltpu.SemaphoreType.DMA((LEFT // STEP + 1,)),
        ],
        flops=2 * 10**9,
        moved=7 * 10**6,
    )(*(pltpu.with_memory_space_constraint(x, pltpu.HBM) for x in (labels, own)))
    first = exchange(sent, COL)
    sent = call(
        summed_kernel,
        "summed",
        shape(COLS * P1, LANES),
        [VMEM],
        [pltpu.VMEM((256, LANES), F32)],
        flops=10**7,
        moved=10**6,
    )(first)
    second = exchange_flat(sent, COL, COLS)
    back_scratch = [
        pltpu.VMEM(matrix, BF16),
        pltpu.VMEM(matrix, BF16),
        pltpu.VMEM((2, *matrix), BF16),
        pltpu.VMEM((2, *matrix), BF16),
    ]
    keep_a, send_a, weight = call(
        back_first_kernel,
        "back_first",
        (shape(4, 9, PEERS, LANES), shape(4, 9, PEERS, LANES), shape(*matrix)),
        [VMEM] * 8,
        back_scratch,
        flops=10**9,
        moved=4 * 10**6,
    )(second, counts.reshape(ROWS, LANES), rotated, *forms)
    swap = [(0, 1), (1, 0)]
    got_a = lax.ppermute(send_a, "core", swap)
    keep_b, send_b = call(
        back_second_kernel,
        "back_second",
        (shape(4, 8, PEERS, LANES), shape(4, 8, PEERS, LANES)),
        [VMEM] * 7,
        back_scratch,
        flops=10**9,
        moved=4 * 10**6,
    )(weight, rotated, *forms)
    got_b = lax.ppermute(send_b, "core", swap)
    sides = (
        ("zl", swap),
        (("zt", "zm", "zl"), [(z, (z + (1 if z % 2 else -1)) % 8) for z in range(8)]),
    )
    pair_a = lax.ppermute(keep_a[2:] + got_a[2:], *sides[0])
    pair_b = lax.ppermute(keep_b[2:] + got_b[2:], *sides[1])
    four_a = lax.ppermute(keep_a[1] + got_a[1] + pair_a[1], *sides[1])
    four_b = lax.ppermute(keep_b[1] + got_b[1] + pair_b[1], *sides[0])
    sent = call(
        merged_kernel,
        "merged",
        shape(PEERS * MESSAGE, LANES),
        [VMEM] * 4,
        flops=10**6,
        moved=2 * 10**6,
    )(
        keep_a[0] + got_a[0] + pair_a[0], four_a, keep_b[0] + got_b[0] + pair_b[0], four_b
    )
    third = exchange_flat(sent, ("zt", *COL), PEERS)
    new_factor, new_velocity = call(
        update_kernel,
        "update",
        (shape(256, LANES), shape(256, LANES)),
        [VMEM] * 3,
        [
            pltpu.VMEM((256, LANES), F32),
            pltpu.VMEM((COLS * MESSAGE, LANES), F32),
            pltpu.VMEM((32, LANES), F32),
            pltpu.VMEM((256, LANES), F32),
        ],
        flops=10**7,
        moved=10**6,
    )(third, first, moved)

    def back_to_rows(array):
        return array.reshape(32, HIGHS, 2, LANES).transpose(0, 2, 1, 3).reshape(32, 2, RIGHT)

    return back_to_rows(new_factor), back_to_rows(new_velocity)


def solution(mesh):
    split = Mesh(mesh.devices.reshape(2, 2, 2, 2, 4, 4), ("zt", "zm", "zl", "core", "y", "x"))
    every = ("zt", "zm", "zl", "core", "y", "x")
    return jax.shard_map(
        shards,
        mesh=split,
        in_specs=(P(COL, None, None), P(None, None, every), P(SET, None), P(SET, None)),
        out_specs=(P(None, None, every), P(None, None, every)),
        check_vma=False,
    )
```

```python
import functools

import jax
import jax.numpy as jnp
from jax import lax
from jax.experimental import pallas as pl
from jax.experimental.pallas import tpu as pltpu
from jax.sharding import Mesh
from jax.sharding import PartitionSpec as P

QA, QB, QUBITS = 8, 9, 17
ORDER = 2**QUBITS
LEFT, RIGHT = 2**QA, 2**QB
LANES = 128
HIGHS = RIGHT // LANES
ROWS = ORDER // LANES
COLS = 16
SETS = 16
TOPS = 2

COL = ("y", "x")
SET = ("zt", "zm", "zl", "core")

mixing = 0.1
penalty = 8.0
momentum = 0.9
step_size = 0.5
count_norm = 8.0

F32 = jnp.float32
BF16 = jnp.bfloat16
HIGH = lax.Precision.HIGHEST
PCHUNK = ROWS // COLS
P1 = PCHUNK + 1
MESSAGE = 17
PEERS = 32
VMEM = pl.BlockSpec(memory_space=pltpu.VMEM)
SMEM = pl.BlockSpec(memory_space=pltpu.SMEM)
HBM = pl.BlockSpec(memory_space=pltpu.HBM)


def halves(x):
    high = x.astype(BF16)
    return high, (x - high.astype(F32)).astype(BF16)


def two_pass(high, low, matrix):
    return jnp.dot(high, matrix, preferred_element_type=F32) + jnp.dot(
        low, matrix, preferred_element_type=F32
    )


def masks_of(labels_ref):
    rotated_bits = jnp.int32(0)
    y_bits = jnp.int32(0)
    scale = jnp.float32(1.0)
    for q in range(QUBITS):
        label = labels_ref[0, q]
        bit = jnp.int32(1 << (QUBITS - 1 - q))
        rotated_bits = rotated_bits + jnp.where(label == 2, 0, bit)
        y_bits = y_bits + jnp.where(label == 1, bit, 0)
        scale = scale * jnp.where(label == 2, jnp.float32(1.0), jnp.float32(0.5))
    return rotated_bits, y_bits, scale


def tall(tile, rows):
    return jnp.concatenate([tile] * (rows // 8), axis=0)


def store_hadamard(ref, size, bits):
    row = lax.broadcasted_iota(jnp.int32, (LANES, LANES), 0)
    col = lax.broadcasted_iota(jnp.int32, (LANES, LANES), 1)
    lower = tall(bits & (LANES - 1), LANES)
    odd = lax.population_count(row & col & lower) & 1
    same = ((row ^ col) & (LANES - 1 - lower)) == 0
    block = jnp.where(same, (1 - 2 * odd).astype(F32), 0.0)
    count = size // LANES
    signs = {}
    for t in range(2):
        here = ((bits >> (7 + t)) & 1).astype(F32)
        signs[t] = {(0, 0): 1.0, (0, 1): here, (1, 0): here, (1, 1): 1.0 - 2.0 * here}
    for i in range(count):
        for j in range(count):
            sign = signs[0][i & 1, j & 1] * signs[1][i >> 1, j >> 1] * jnp.ones((8, LANES), F32)
            ref[pl.ds(LANES * i, LANES), pl.ds(LANES * j, LANES)] = (
                block * tall(sign, LANES)
            ).astype(BF16)


def crossed(left, right, bit):
    return left + bit * right, bit * left + (1.0 - 2.0 * bit) * right


def store_tables(y_bits, scale, turned_ha_ref, cosine_ref, sine_ref, ha):
    core = lax.axis_index("core")
    own = lax.axis_index("zm") * 2 + lax.axis_index("zl")
    lane = lax.broadcasted_iota(jnp.int32, (8, LANES), 1)
    row = lax.broadcasted_iota(jnp.int32, (16, LANES), 0)
    right_turns = [
        tall(lax.population_count((lane + high * LANES) & y_bits), 16) for high in range(HIGHS)
    ]
    for half in range(2):
        for q, place in enumerate((own, 3 - own, own ^ 1, (3 - own) ^ 1)):
            for zt in range(TOPS):
                start = pl.multiple_of((zt * 4 + place) * 32 + (core ^ half) * 16, 16)
                at = 128 * half + 32 * q + 16 * zt
                turned_ha_ref[pl.ds(at, 16), :] = ha[pl.ds(start, 16), :]
                left_turns = lax.population_count(((row + start) * RIGHT) & y_bits)
                for high in range(HIGHS):
                    turns = (left_turns + right_turns[high]) & 3
                    to = pl.ds(high * LANES, LANES)
                    signed = jnp.where(turns >= 2, -scale, scale)
                    odd = (turns & 1) == 1
                    cosine_ref[pl.ds(at, 16), to] = jnp.where(odd, 0.0, signed)
                    sine_ref[pl.ds(at, 16), to] = jnp.where(odd, signed, 0.0)


STEP = 32
HALF = RIGHT // 2


def forward_kernel(labels_hbm, factor_hbm, rotated_ref, send_ref, top_ref, turned_ha_ref, hb, cosine_ref, sine_ref, labels_ref, factor_ref, xh, xl, th, tl, prob, ha, sems):
    def fetch(step):
        rows = pl.ds(pl.multiple_of(step * (STEP * 8), STEP * 8), STEP * 8)
        return pltpu.make_async_copy(factor_hbm.at[:, rows], factor_ref.at[:, rows], sems.at[step])

    fetched = pltpu.make_async_copy(labels_hbm, labels_ref, sems.at[LEFT // STEP])
    fetched.start()
    for step in range(LEFT // STEP):
        fetch(step).start()
    set_index = lax.axis_index(SET)
    fetched.wait()
    bits, y_bits, scale = masks_of(labels_ref)
    tile = jnp.full((8, LANES), bits, jnp.int32)
    store_hadamard(hb, HALF, tile & (HALF - 1))
    store_hadamard(ha, LEFT, tile >> QB)
    top = ((bits >> (QB - 1)) & 1).astype(F32)
    top_ref[...] = jnp.full((8, LANES), top, F32)
    store_tables(y_bits, scale, turned_ha_ref, cosine_ref, sine_ref, ha)
    prob[...] = jnp.zeros_like(prob)
    lane = lax.broadcasted_iota(jnp.int32, (8, LANES), 1)

    def turned(step, carry):
        fetch(step).wait()
        row = lax.broadcasted_iota(jnp.int32, (STEP, LANES), 0) + step * STEP
        left_turns = lax.population_count((row * RIGHT) & y_bits)
        to = pl.ds(pl.multiple_of(step * STEP, STEP), STEP)
        values = {}
        for high in (0, 2, 1, 3):
            right_turns = lax.population_count((lane + high * LANES) & y_bits)
            turns = (left_turns + tall(right_turns, STEP)) & 3
            swap = (turns & 1) == 1
            sign_real = jnp.where(turns >= 2, -1.0, 1.0)
            sign_imag = jnp.where(((turns + 1) & 2) == 2, -1.0, 1.0)
            for r in range(2):
                real, imag = (
                    factor_ref[r, pl.ds(step * (STEP * 8) + 2 * high + c, STEP, stride=8), :]
                    for c in range(2)
                )
                values[high, 2 * r] = sign_real * jnp.where(swap, imag, real)
                values[high, 2 * r + 1] = sign_imag * jnp.where(swap, real, imag)
            if high >= 2:
                for i in range(4):
                    pair = crossed(values[high - 2, i], values[high, i], top)
                    for at, value in zip((high - 2, high), pair):
                        block = pl.ds(at * LANES, LANES)
                        xh[i, to, block], xl[i, to, block] = halves(value)
        return carry

    lax.fori_loop(0, LEFT // STEP, turned, 0)

    def one(i, carry):
        for n in range(2):
            part = pl.ds(n * 256, 256)
            first = jnp.dot(ha[...], xh[i, :, part], preferred_element_type=F32) + jnp.dot(
                ha[...], xl[i, :, part], preferred_element_type=F32
            )
            th[:, part], tl[:, part] = halves(first)
        for n in range(2):
            part = pl.ds(n * 256, 256)
            second = two_pass(th[:, part], tl[:, part], hb[...])
            rotated_ref[i, :, part] = second
            prob[:, part] += second * second
        return carry

    lax.fori_loop(0, 4, one, 0, unroll=4)
    for c in range(COLS):
        for high in range(HIGHS):
            send_ref[c, pl.ds(16 * high, 16), :] = (
                prob[pl.ds(16 * c, 16), pl.ds(high * LANES, LANES)] * scale
            )
        start = pl.multiple_of(set_index * (ROWS * 2 // SETS) + 8 * c, 8)
        for r in range(2):
            send_ref[c, pl.ds(PCHUNK + 8 * r, 8), :] = factor_ref[r, pl.ds(start, 8), :]


def parts_of(rows):
    return tuple(
        jnp.concatenate(
            [rows[pl.ds(2 * high + c, 32, stride=2 * HIGHS), :] for high in range(HIGHS)], axis=1
        )
        for c in range(2)
    )


def summed_kernel(got_ref, send_ref, rows):
    total = got_ref[0, pl.ds(0, PCHUNK), :]
    for c in range(1, COLS):
        total = total + got_ref[c, pl.ds(0, PCHUNK), :]
    for c in range(COLS):
        rows[pl.ds(16 * c, 16), :] = got_ref[c, pl.ds(PCHUNK, 16), :]
    real, imag = parts_of(rows)
    left_high, left_low = halves(jnp.concatenate([real, imag], axis=1))
    both = jnp.concatenate(
        [jnp.concatenate([real, imag], axis=1), jnp.concatenate([imag, -real], axis=1)], axis=0
    )
    both_high, both_low = halves(both)
    gram = sum(
        lax.dot_general(x, y, (((1,), (1,)), ((), ())), preferred_element_type=F32)
        for x, y in ((left_high, both_low), (left_low, both_high), (left_high, both_high))
    )
    rows[pl.ds(0, 32), :] = jnp.zeros((32, LANES), F32)
    rows[pl.ds(0, 32), pl.ds(0, 64)] = gram
    pairs = rows[pl.ds(0, 16, stride=2), :] + pltpu.roll(rows[pl.ds(1, 16, stride=2), :], 64, 1)
    for c in range(COLS):
        send_ref[pl.ds(P1 * c, PCHUNK), :] = total
    send_ref[pl.ds(PCHUNK, 16, stride=P1), :] = pairs


ORDERS = ((0, 1, 2, 3), (0, 2, 1, 3))


def unrotated(r, weight_ref, rotated_ref, top_ref, ha_ref, hb_ref, cosine_ref, sine_ref, keep_ref, send_ref, wh, wl, th, tl):
    top = top_ref[:1, :1]
    for c in range(2):
        for n in range(2):
            parts = [pl.ds(n * LANES, LANES), pl.ds(HALF + n * LANES, LANES)]
            pair = crossed(
                *(weight_ref[:, part] * rotated_ref[2 * r + c, :, part] for part in parts), top
            )
            for part, value in zip(parts, pair):
                wh[:, part], wl[:, part] = halves(value)
        for n in range(2):
            part = pl.ds(n * HALF, HALF)
            th[c, :, part], tl[c, :, part] = halves(two_pass(wh[:, part], wl[:, part], hb_ref[...]))
    for n in range(2):
        part = pl.ds(n * HALF, HALF)
        real, imag = (
            jnp.dot(ha_ref[...], th[c, :, part], preferred_element_type=F32)
            + jnp.dot(ha_ref[...], tl[c, :, part], preferred_element_type=F32)
            for c in range(2)
        )
        cosine, sine = cosine_ref[:, part], sine_ref[:, part]
        for c, value in ((0, cosine * real - sine * imag), (1, cosine * imag + sine * real)):
            for half, out in ((0, keep_ref), (1, send_ref)):
                for at, q in enumerate(ORDERS[r]):
                    rows = slice(128 * half + PEERS * q, 128 * half + PEERS * (q + 1))
                    for k in range(2):
                        out[at, 4 * n + 2 * k + c] = value[rows, k * LANES : (k + 1) * LANES]


def back_first_kernel(got_ref, counts_ref, rotated_ref, top_ref, ha_ref, hb_ref, cosine_ref, sine_ref, keep_ref, send_ref, weight_ref, wh, wl, th, tl):
    total = jnp.zeros((PCHUNK, LANES), F32)
    gram = jnp.zeros((1, LANES), F32)
    for c in range(COLS):
        total = total + got_ref[pl.ds(P1 * c, PCHUNK), :]
        gram = gram + got_ref[pl.ds(P1 * c + PCHUNK, 1), :]
    trace = jnp.sum(total)
    slope = (1.0 - mixing) / trace
    ratio_sum = jnp.zeros((16, LANES), F32)
    for c in range(COLS):
        for high in range(HIGHS):
            count = counts_ref[pl.ds(64 * c + high, 16, stride=HIGHS), :].astype(F32)
            p = got_ref[pl.ds(P1 * c + 16 * high, 16), :]
            w = count / ((slope * p + mixing / ORDER) * (count_norm * ORDER))
            weight_ref[pl.ds(16 * c, 16), pl.ds(high * LANES, LANES)] = w
            ratio_sum = ratio_sum + w * p
    weight_ref[...] = weight_ref[...] - jnp.sum(ratio_sum) / trace
    unrotated(0, weight_ref, rotated_ref, top_ref, ha_ref, hb_ref, cosine_ref, sine_ref, keep_ref, send_ref, wh, wl, th, tl)
    for out in (keep_ref, send_ref):
        for at in range(4):
            out[at, 8] = jnp.broadcast_to(gram, (PEERS, LANES))


def back_second_kernel(weight_ref, *refs):
    unrotated(1, weight_ref, *refs)


def split_kernel(mine, got, keep_ref, send_ref):
    own = lax.axis_index("zt")
    here, there = (pl.ds(pl.multiple_of(16 * half, 16), 16) for half in (own, 1 - own))
    for j in range(mine.shape[0]):
        keep_ref[j] = mine[j, here, :] + got[j, here, :]
        send_ref[j] = mine[j, there, :] + got[j, there, :]


def merged_kernel(mine_a, got_a, mine_b, got_b, send_ref):
    for j in range(8):
        send_ref[pl.ds(j, COLS, stride=MESSAGE), :] = mine_a[j] + got_a[j]
        send_ref[pl.ds(8 + j, COLS, stride=MESSAGE), :] = mine_b[j] + got_b[j]
    send_ref[pl.ds(16, COLS, stride=MESSAGE), :] = mine_a[8] + got_a[8]


def update_kernel(got_ref, first_ref, velocity_ref, new_factor_ref, new_velocity_ref, rows, gram_ref, mixed_ref):
    for c in range(COLS):
        rows[pl.ds(16 * c, 16), :] = first_ref[c, pl.ds(PCHUNK, 16), :]
    pairs = got_ref[pl.ds(16, 16, stride=MESSAGE), :]
    gram_ref[pl.ds(0, 16, stride=2), :] = pairs
    gram_ref[pl.ds(1, 16, stride=2), :] = pltpu.roll(pairs, 64, 1)
    gram = gram_ref[:, pl.ds(0, 64)]
    i = lax.broadcasted_iota(jnp.int32, (32, 64), 0)
    j = lax.broadcasted_iota(jnp.int32, (32, 64), 1)
    trace = jnp.sum(jnp.where(i == j, gram, 0.0))
    purity = jnp.sum(gram * gram) / (trace * trace)
    real, imag = parts_of(rows)
    for c, parts in ((0, (real, imag)), (1, (imag, -real))):
        mixed = jnp.dot(
            gram, jnp.concatenate(parts, axis=0), precision=HIGH, preferred_element_type=F32
        )
        for high in range(HIGHS):
            mixed_ref[pl.ds(2 * high + c, 32, stride=2 * HIGHS), :] = mixed[
                :, high * LANES : (high + 1) * LANES
            ]
    for c in range(COLS):
        at = pl.ds(16 * c, 16)
        own = rows[at, :]
        gradient = -((1.0 - mixing) / SETS) * got_ref[pl.ds(MESSAGE * c, 16), :] + penalty * (
            2.0 * mixed_ref[at, :] / trace - 2.0 * purity * own
        )
        velocity = momentum * velocity_ref[at, :] + gradient
        new_velocity_ref[at, :] = velocity
        new_factor_ref[at, :] = own - step_size * velocity


def shape(*dims, dtype=F32):
    return jax.ShapeDtypeStruct(dims, dtype)


def call(kernel, name, out, specs, scratch=(), flops=0, moved=0, vmem=16 * 2**20):
    return pl.pallas_call(
        kernel,
        name=name,
        out_shape=out,
        in_specs=specs,
        out_specs=jax.tree.map(lambda _: VMEM, out),
        scratch_shapes=list(scratch),
        compiler_params=pltpu.CompilerParams(vmem_limit_bytes=vmem),
        cost_estimate=pl.CostEstimate(flops=flops, bytes_accessed=moved, transcendentals=0),
    )


def exchange(array, axis):
    return lax.all_to_all(array, axis, split_axis=0, concat_axis=0, tiled=True)


def exchange_flat(array, axis, peers):
    return exchange(array.reshape(peers, 1, -1), axis).reshape(array.shape)


def shards(factor, velocity, labels, counts):
    own = factor.reshape(2, 2, ROWS, LANES).transpose(0, 2, 1, 3).reshape(2, 2 * ROWS, LANES)
    moved = velocity.reshape(32, 2, HIGHS, LANES).transpose(0, 2, 1, 3).reshape(256, LANES)
    matrix = (LEFT, RIGHT)
    rotated, sent, *forms = call(
        forward_kernel,
        "forward",
        (
            shape(4, *matrix),
            shape(COLS, PCHUNK + 16, LANES),
            shape(8, LANES),
            shape(LEFT, LEFT, dtype=BF16),
            shape(HALF, HALF, dtype=BF16),
            shape(*matrix),
            shape(*matrix),
        ),
        [HBM, HBM],
        [
            pltpu.SMEM((1, QUBITS), jnp.int32),
            pltpu.VMEM((2, 2 * ROWS, LANES), F32),
            pltpu.VMEM((4, *matrix), BF16),
            pltpu.VMEM((4, *matrix), BF16),
            pltpu.VMEM(matrix, BF16),
            pltpu.VMEM(matrix, BF16),
            pltpu.VMEM(matrix, F32),
            pltpu.VMEM((LEFT, LEFT), BF16),
            pltpu.SemaphoreType.DMA((LEFT // STEP + 1,)),
        ],
        flops=2 * 10**9,
        moved=7 * 10**6,
    )(*(pltpu.with_memory_space_constraint(x, pltpu.HBM) for x in (labels, own)))
    first = exchange(sent, COL)
    sent = call(
        summed_kernel,
        "summed",
        shape(COLS * P1, LANES),
        [VMEM],
        [pltpu.VMEM((256, LANES), F32)],
        flops=10**7,
        moved=10**6,
    )(first)
    second = exchange_flat(sent, COL, COLS)
    back_scratch = [
        pltpu.VMEM(matrix, BF16),
        pltpu.VMEM(matrix, BF16),
        pltpu.VMEM((2, *matrix), BF16),
        pltpu.VMEM((2, *matrix), BF16),
    ]
    keep_a, send_a, weight = call(
        back_first_kernel,
        "back_first",
        (shape(4, 9, PEERS, LANES), shape(4, 9, PEERS, LANES), shape(*matrix)),
        [VMEM] * 8,
        back_scratch,
        flops=10**9,
        moved=4 * 10**6,
    )(second, counts.reshape(ROWS, LANES), rotated, *forms)
    swap = [(0, 1), (1, 0)]
    got_a = lax.ppermute(send_a, "core", swap)
    keep_b, send_b = call(
        back_second_kernel,
        "back_second",
        (shape(4, 8, PEERS, LANES), shape(4, 8, PEERS, LANES)),
        [VMEM] * 7,
        back_scratch,
        flops=10**9,
        moved=4 * 10**6,
    )(weight, rotated, *forms)
    got_b = lax.ppermute(send_b, "core", swap)
    sides = (
        ("zl", swap),
        (("zt", "zm", "zl"), [(z, (z + (1 if z % 2 else -1)) % 8) for z in range(8)]),
    )
    pair_a = lax.ppermute(keep_a[2:] + got_a[2:], *sides[0])
    pair_b = lax.ppermute(keep_b[2:] + got_b[2:], *sides[1])
    four_a = lax.ppermute(keep_a[1] + got_a[1] + pair_a[1], *sides[1])
    four_b = lax.ppermute(keep_b[1] + got_b[1] + pair_b[1], *sides[0])
    merged = []
    for mine, got in (
        (keep_a[0] + got_a[0] + pair_a[0], four_a),
        (keep_b[0] + got_b[0] + pair_b[0], four_b),
    ):
        half = shape(mine.shape[0], COLS, LANES)
        kept, sent = call(
            split_kernel, "split", (half, half), [VMEM] * 2, flops=10**5, moved=10**6
        )(mine, got)
        merged += [kept, lax.ppermute(sent, "zt", swap)]
    sent = call(
        merged_kernel,
        "merged",
        shape(COLS * MESSAGE, LANES),
        [VMEM] * 4,
        flops=10**5,
        moved=10**6,
    )(*merged)
    third = exchange_flat(sent, COL, COLS)
    new_factor, new_velocity = call(
        update_kernel,
        "update",
        (shape(256, LANES), shape(256, LANES)),
        [VMEM] * 3,
        [
            pltpu.VMEM((256, LANES), F32),
            pltpu.VMEM((32, LANES), F32),
            pltpu.VMEM((256, LANES), F32),
        ],
        flops=10**7,
        moved=10**6,
    )(third, first, moved)

    def back_to_rows(array):
        return array.reshape(32, HIGHS, 2, LANES).transpose(0, 2, 1, 3).reshape(32, 2, RIGHT)

    return back_to_rows(new_factor), back_to_rows(new_velocity)


def solution(mesh):
    split = Mesh(mesh.devices.reshape(2, 2, 2, 2, 4, 4), ("zt", "zm", "zl", "core", "y", "x"))
    every = ("zt", "zm", "zl", "core", "y", "x")
    return jax.shard_map(
        shards,
        mesh=split,
        in_specs=(P(COL, None, None), P(None, None, every), P(SET, None), P(SET, None)),
        out_specs=(P(None, None, every), P(None, None, every)),
        check_vma=False,
    )
```

```python
import functools

import jax
import jax.numpy as jnp
from jax import lax
from jax.experimental import pallas as pl
from jax.experimental.pallas import tpu as pltpu
from jax.sharding import Mesh
from jax.sharding import PartitionSpec as P

QA, QB, QUBITS = 8, 9, 17
ORDER = 2**QUBITS
LEFT, RIGHT = 2**QA, 2**QB
LANES = 128
HIGHS = RIGHT // LANES
ROWS = ORDER // LANES
COLS = 16
SETS = 16
TOPS = 2

COL = ("y", "x")
SET = ("zt", "zm", "zl", "core")

mixing = 0.1
penalty = 8.0
momentum = 0.9
step_size = 0.5
count_norm = 8.0

F32 = jnp.float32
BF16 = jnp.bfloat16
HIGH = lax.Precision.HIGHEST
PCHUNK = ROWS // COLS
P1 = PCHUNK + 1
MESSAGE = 17
PEERS = 32
VMEM = pl.BlockSpec(memory_space=pltpu.VMEM)
SMEM = pl.BlockSpec(memory_space=pltpu.SMEM)
HBM = pl.BlockSpec(memory_space=pltpu.HBM)


def halves(x):
    high = x.astype(BF16)
    return high, (x - high.astype(F32)).astype(BF16)


def two_pass(high, low, matrix):
    return jnp.dot(high, matrix, preferred_element_type=F32) + jnp.dot(
        low, matrix, preferred_element_type=F32
    )


def masks_of(labels_ref):
    rotated_bits = jnp.int32(0)
    y_bits = jnp.int32(0)
    scale = jnp.float32(1.0)
    for q in range(QUBITS):
        label = labels_ref[0, q]
        bit = jnp.int32(1 << (QUBITS - 1 - q))
        rotated_bits = rotated_bits + jnp.where(label == 2, 0, bit)
        y_bits = y_bits + jnp.where(label == 1, bit, 0)
        scale = scale * jnp.where(label == 2, jnp.float32(1.0), jnp.float32(0.5))
    return rotated_bits, y_bits, scale


def tall(tile, rows):
    return jnp.concatenate([tile] * (rows // 8), axis=0)


def store_hadamard(ref, size, bits):
    row = lax.broadcasted_iota(jnp.int32, (LANES, LANES), 0)
    col = lax.broadcasted_iota(jnp.int32, (LANES, LANES), 1)
    lower = tall(bits & (LANES - 1), LANES)
    odd = lax.population_count(row & col & lower) & 1
    same = ((row ^ col) & (LANES - 1 - lower)) == 0
    block = jnp.where(same, (1 - 2 * odd).astype(F32), 0.0)
    count = size // LANES
    signs = {}
    for t in range(2):
        here = ((bits >> (7 + t)) & 1).astype(F32)
        signs[t] = {(0, 0): 1.0, (0, 1): here, (1, 0): here, (1, 1): 1.0 - 2.0 * here}
    for i in range(count):
        for j in range(count):
            sign = signs[0][i & 1, j & 1] * signs[1][i >> 1, j >> 1] * jnp.ones((8, LANES), F32)
            ref[pl.ds(LANES * i, LANES), pl.ds(LANES * j, LANES)] = (
                block * tall(sign, LANES)
            ).astype(BF16)


def crossed(left, right, bit):
    return left + bit * right, bit * left + (1.0 - 2.0 * bit) * right


def store_tables(y_bits, scale, turned_ha_ref, cosine_ref, sine_ref, ha):
    core = lax.axis_index("core")
    own = lax.axis_index("zm") * 2 + lax.axis_index("zl")
    lane = lax.broadcasted_iota(jnp.int32, (8, LANES), 1)
    row = lax.broadcasted_iota(jnp.int32, (16, LANES), 0)
    right_turns = [
        tall(lax.population_count((lane + high * LANES) & y_bits), 16) for high in range(HIGHS)
    ]
    for half in range(2):
        for q, place in enumerate((own, 3 - own, own ^ 1, (3 - own) ^ 1)):
            for zt in range(TOPS):
                start = pl.multiple_of((zt * 4 + place) * 32 + (core ^ half) * 16, 16)
                at = 128 * half + 32 * q + 16 * zt
                turned_ha_ref[pl.ds(at, 16), :] = ha[pl.ds(start, 16), :]
                left_turns = lax.population_count(((row + start) * RIGHT) & y_bits)
                for high in range(HIGHS):
                    turns = (left_turns + right_turns[high]) & 3
                    to = pl.ds(high * LANES, LANES)
                    signed = jnp.where(turns >= 2, -scale, scale)
                    odd = (turns & 1) == 1
                    cosine_ref[pl.ds(at, 16), to] = jnp.where(odd, 0.0, signed)
                    sine_ref[pl.ds(at, 16), to] = jnp.where(odd, signed, 0.0)


STEP = 32
HALF = RIGHT // 2


def forward_kernel(labels_hbm, factor_hbm, rotated_ref, send_ref, top_ref, turned_ha_ref, hb, cosine_ref, sine_ref, labels_ref, factor_ref, xh, xl, th, tl, prob, ha, sems):
    def fetch(step):
        rows = pl.ds(pl.multiple_of(step * (STEP * 8), STEP * 8), STEP * 8)
        return pltpu.make_async_copy(factor_hbm.at[:, rows], factor_ref.at[:, rows], sems.at[step])

    fetched = pltpu.make_async_copy(labels_hbm, labels_ref, sems.at[LEFT // STEP])
    fetched.start()
    for step in range(LEFT // STEP):
        fetch(step).start()
    set_index = lax.axis_index(SET)
    fetched.wait()
    bits, y_bits, scale = masks_of(labels_ref)
    tile = jnp.full((8, LANES), bits, jnp.int32)
    store_hadamard(hb, HALF, tile & (HALF - 1))
    store_hadamard(ha, LEFT, tile >> QB)
    top = ((bits >> (QB - 1)) & 1).astype(F32)
    top_ref[...] = jnp.full((8, LANES), top, F32)
    store_tables(y_bits, scale, turned_ha_ref, cosine_ref, sine_ref, ha)
    prob[...] = jnp.zeros_like(prob)
    lane = lax.broadcasted_iota(jnp.int32, (8, LANES), 1)

    def turned(step, carry):
        fetch(step).wait()
        row = lax.broadcasted_iota(jnp.int32, (STEP, LANES), 0) + step * STEP
        left_turns = lax.population_count((row * RIGHT) & y_bits)
        to = pl.ds(pl.multiple_of(step * STEP, STEP), STEP)
        values = {}
        for high in (0, 2, 1, 3):
            right_turns = lax.population_count((lane + high * LANES) & y_bits)
            turns = (left_turns + tall(right_turns, STEP)) & 3
            swap = (turns & 1) == 1
            sign_real = jnp.where(turns >= 2, -1.0, 1.0)
            sign_imag = jnp.where(((turns + 1) & 2) == 2, -1.0, 1.0)
            for r in range(2):
                real, imag = (
                    factor_ref[r, pl.ds(step * (STEP * 8) + 2 * high + c, STEP, stride=8), :]
                    for c in range(2)
                )
                values[high, 2 * r] = sign_real * jnp.where(swap, imag, real)
                values[high, 2 * r + 1] = sign_imag * jnp.where(swap, real, imag)
            if high >= 2:
                for i in range(4):
                    pair = crossed(values[high - 2, i], values[high, i], top)
                    for at, value in zip((high - 2, high), pair):
                        block = pl.ds(at * LANES, LANES)
                        xh[i, to, block], xl[i, to, block] = halves(value)
        return carry

    lax.fori_loop(0, LEFT // STEP, turned, 0)

    def one(i, carry):
        for n in range(2):
            part = pl.ds(n * 256, 256)
            first = jnp.dot(ha[...], xh[i, :, part], preferred_element_type=F32) + jnp.dot(
                ha[...], xl[i, :, part], preferred_element_type=F32
            )
            th[:, part], tl[:, part] = halves(first)
        for n in range(2):
            part = pl.ds(n * 256, 256)
            second = two_pass(th[:, part], tl[:, part], hb[...])
            rotated_ref[i, :, part] = second
            prob[:, part] += second * second
        return carry

    lax.fori_loop(0, 4, one, 0, unroll=4)
    for c in range(COLS):
        for high in range(HIGHS):
            send_ref[c, pl.ds(16 * high, 16), :] = (
                prob[pl.ds(16 * c, 16), pl.ds(high * LANES, LANES)] * scale
            )
        start = pl.multiple_of(set_index * (ROWS * 2 // SETS) + 8 * c, 8)
        for r in range(2):
            send_ref[c, pl.ds(PCHUNK + 8 * r, 8), :] = factor_ref[r, pl.ds(start, 8), :]


def parts_of(rows):
    return tuple(
        jnp.concatenate(
            [rows[pl.ds(2 * high + c, 32, stride=2 * HIGHS), :] for high in range(HIGHS)], axis=1
        )
        for c in range(2)
    )


def summed_kernel(got_ref, send_ref, rows):
    total = got_ref[0, pl.ds(0, PCHUNK), :]
    for c in range(1, COLS):
        total = total + got_ref[c, pl.ds(0, PCHUNK), :]
    for c in range(COLS):
        rows[pl.ds(16 * c, 16), :] = got_ref[c, pl.ds(PCHUNK, 16), :]
    real, imag = parts_of(rows)
    left_high, left_low = halves(jnp.concatenate([real, imag], axis=1))
    both = jnp.concatenate(
        [jnp.concatenate([real, imag], axis=1), jnp.concatenate([imag, -real], axis=1)], axis=0
    )
    both_high, both_low = halves(both)
    gram = sum(
        lax.dot_general(x, y, (((1,), (1,)), ((), ())), preferred_element_type=F32)
        for x, y in ((left_high, both_low), (left_low, both_high), (left_high, both_high))
    )
    rows[pl.ds(0, 32), :] = jnp.zeros((32, LANES), F32)
    rows[pl.ds(0, 32), pl.ds(0, 64)] = gram
    pairs = rows[pl.ds(0, 16, stride=2), :] + pltpu.roll(rows[pl.ds(1, 16, stride=2), :], 64, 1)
    for c in range(COLS):
        send_ref[pl.ds(P1 * c, PCHUNK), :] = total
    send_ref[pl.ds(PCHUNK, 16, stride=P1), :] = pairs


ORDERS = ((0, 1, 2, 3), (0, 2, 1, 3))


def unrotated(r, weight_ref, rotated_ref, top_ref, ha_ref, hb_ref, cosine_ref, sine_ref, keep_ref, send_ref, wh, wl, th, tl):
    top = top_ref[:1, :1]
    for c in range(2):
        for n in range(2):
            parts = [pl.ds(n * LANES, LANES), pl.ds(HALF + n * LANES, LANES)]
            pair = crossed(
                *(weight_ref[:, part] * rotated_ref[2 * r + c, :, part] for part in parts), top
            )
            for part, value in zip(parts, pair):
                wh[c, :, part], wl[c, :, part] = halves(value)
        for n in range(2):
            part = pl.ds(n * HALF, HALF)
            th[c, :, part], tl[c, :, part] = halves(two_pass(wh[c, :, part], wl[c, :, part], hb_ref[...]))
    for n in range(2):
        part = pl.ds(n * HALF, HALF)
        real, imag = (
            jnp.dot(ha_ref[...], th[c, :, part], preferred_element_type=F32)
            + jnp.dot(ha_ref[...], tl[c, :, part], preferred_element_type=F32)
            for c in range(2)
        )
        cosine, sine = cosine_ref[:, part], sine_ref[:, part]
        for c, value in ((0, cosine * real - sine * imag), (1, cosine * imag + sine * real)):
            for half, out in ((0, keep_ref), (1, send_ref)):
                for at, q in enumerate(ORDERS[r]):
                    rows = slice(128 * half + PEERS * q, 128 * half + PEERS * (q + 1))
                    for k in range(2):
                        out[at, 4 * n + 2 * k + c] = value[rows, k * LANES : (k + 1) * LANES]


def back_first_kernel(got_ref, counts_ref, rotated_ref, top_ref, ha_ref, hb_ref, cosine_ref, sine_ref, keep_ref, send_ref, weight_ref, wh, wl, th, tl):
    total = jnp.zeros((PCHUNK, LANES), F32)
    gram = jnp.zeros((1, LANES), F32)
    for c in range(COLS):
        total = total + got_ref[pl.ds(P1 * c, PCHUNK), :]
        gram = gram + got_ref[pl.ds(P1 * c + PCHUNK, 1), :]
    trace = jnp.sum(total)
    slope = (1.0 - mixing) / trace
    ratio_sum = jnp.zeros((16, LANES), F32)
    for c in range(COLS):
        for high in range(HIGHS):
            count = counts_ref[pl.ds(64 * c + high, 16, stride=HIGHS), :].astype(F32)
            p = got_ref[pl.ds(P1 * c + 16 * high, 16), :]
            w = count / ((slope * p + mixing / ORDER) * (count_norm * ORDER))
            weight_ref[pl.ds(16 * c, 16), pl.ds(high * LANES, LANES)] = w
            ratio_sum = ratio_sum + w * p
    weight_ref[...] = weight_ref[...] - jnp.sum(ratio_sum) / trace
    unrotated(0, weight_ref, rotated_ref, top_ref, ha_ref, hb_ref, cosine_ref, sine_ref, keep_ref, send_ref, wh, wl, th, tl)
    for out in (keep_ref, send_ref):
        for at in range(4):
            out[at, 8] = jnp.broadcast_to(gram, (PEERS, LANES))


def back_second_kernel(weight_ref, *refs):
    unrotated(1, weight_ref, *refs)


def merged_kernel(mine_a, got_a, mine_b, got_b, send_ref):
    for j in range(8):
        send_ref[pl.ds(j, PEERS, stride=MESSAGE), :] = mine_a[j] + got_a[j]
        send_ref[pl.ds(8 + j, PEERS, stride=MESSAGE), :] = mine_b[j] + got_b[j]
    send_ref[pl.ds(16, PEERS, stride=MESSAGE), :] = mine_a[8] + got_a[8]


def update_kernel(got_ref, first_ref, velocity_ref, new_factor_ref, new_velocity_ref, rows, sums, gram_ref, mixed_ref):
    block = COLS * MESSAGE
    total = got_ref[pl.ds(0, block), :]
    for zt in range(1, TOPS):
        total = total + got_ref[pl.ds(block * zt, block), :]
    sums[...] = total
    for c in range(COLS):
        rows[pl.ds(16 * c, 16), :] = first_ref[c, pl.ds(PCHUNK, 16), :]
    pairs = sums[pl.ds(16, 16, stride=MESSAGE), :]
    gram_ref[pl.ds(0, 16, stride=2), :] = pairs
    gram_ref[pl.ds(1, 16, stride=2), :] = pltpu.roll(pairs, 64, 1)
    gram = gram_ref[:, pl.ds(0, 64)]
    i = lax.broadcasted_iota(jnp.int32, (32, 64), 0)
    j = lax.broadcasted_iota(jnp.int32, (32, 64), 1)
    trace = jnp.sum(jnp.where(i == j, gram, 0.0))
    purity = jnp.sum(gram * gram) / (trace * trace)
    real, imag = parts_of(rows)
    for c, parts in ((0, (real, imag)), (1, (imag, -real))):
        mixed = jnp.dot(
            gram, jnp.concatenate(parts, axis=0), precision=HIGH, preferred_element_type=F32
        )
        for high in range(HIGHS):
            mixed_ref[pl.ds(2 * high + c, 32, stride=2 * HIGHS), :] = mixed[
                :, high * LANES : (high + 1) * LANES
            ]
    for c in range(COLS):
        at = pl.ds(16 * c, 16)
        own = rows[at, :]
        gradient = -((1.0 - mixing) / SETS) * sums[pl.ds(MESSAGE * c, 16), :] + penalty * (
            2.0 * mixed_ref[at, :] / trace - 2.0 * purity * own
        )
        velocity = momentum * velocity_ref[at, :] + gradient
        new_velocity_ref[at, :] = velocity
        new_factor_ref[at, :] = own - step_size * velocity


def shape(*dims, dtype=F32):
    return jax.ShapeDtypeStruct(dims, dtype)


def call(kernel, name, out, specs, scratch=(), flops=0, moved=0, vmem=16 * 2**20):
    return pl.pallas_call(
        kernel,
        name=name,
        out_shape=out,
        in_specs=specs,
        out_specs=jax.tree.map(lambda _: VMEM, out),
        scratch_shapes=list(scratch),
        compiler_params=pltpu.CompilerParams(vmem_limit_bytes=vmem),
        cost_estimate=pl.CostEstimate(flops=flops, bytes_accessed=moved, transcendentals=0),
    )


def exchange(array, axis):
    return lax.all_to_all(array, axis, split_axis=0, concat_axis=0, tiled=True)


def exchange_flat(array, axis, peers):
    return exchange(array.reshape(peers, 1, -1), axis).reshape(array.shape)


def shards(factor, velocity, labels, counts):
    own = factor.reshape(2, 2, ROWS, LANES).transpose(0, 2, 1, 3).reshape(2, 2 * ROWS, LANES)
    moved = velocity.reshape(32, 2, HIGHS, LANES).transpose(0, 2, 1, 3).reshape(256, LANES)
    matrix = (LEFT, RIGHT)
    rotated, sent, *forms = call(
        forward_kernel,
        "forward",
        (
            shape(4, *matrix),
            shape(COLS, PCHUNK + 16, LANES),
            shape(8, LANES),
            shape(LEFT, LEFT, dtype=BF16),
            shape(HALF, HALF, dtype=BF16),
            shape(*matrix),
            shape(*matrix),
        ),
        [HBM, HBM],
        [
            pltpu.SMEM((1, QUBITS), jnp.int32),
            pltpu.VMEM((2, 2 * ROWS, LANES), F32),
            pltpu.VMEM((4, *matrix), BF16),
            pltpu.VMEM((4, *matrix), BF16),
            pltpu.VMEM(matrix, BF16),
            pltpu.VMEM(matrix, BF16),
            pltpu.VMEM(matrix, F32),
            pltpu.VMEM((LEFT, LEFT), BF16),
            pltpu.SemaphoreType.DMA((LEFT // STEP + 1,)),
        ],
        flops=2 * 10**9,
        moved=7 * 10**6,
    )(*(pltpu.with_memory_space_constraint(x, pltpu.HBM) for x in (labels, own)))
    first = exchange(sent, COL)
    sent = call(
        summed_kernel,
        "summed",
        shape(COLS * P1, LANES),
        [VMEM],
        [pltpu.VMEM((256, LANES), F32)],
        flops=10**7,
        moved=10**6,
    )(first)
    second = exchange_flat(sent, COL, COLS)
    back_scratch = [
        pltpu.VMEM((2, *matrix), BF16),
        pltpu.VMEM((2, *matrix), BF16),
        pltpu.VMEM((2, *matrix), BF16),
        pltpu.VMEM((2, *matrix), BF16),
    ]
    keep_a, send_a, weight = call(
        back_first_kernel,
        "back_first",
        (shape(4, 9, PEERS, LANES), shape(4, 9, PEERS, LANES), shape(*matrix)),
        [VMEM] * 8,
        back_scratch,
        flops=10**9,
        moved=4 * 10**6,
    )(second, counts.reshape(ROWS, LANES), rotated, *forms)
    swap = [(0, 1), (1, 0)]
    got_a = lax.ppermute(send_a, "core", swap)
    keep_b, send_b = call(
        back_second_kernel,
        "back_second",
        (shape(4, 8, PEERS, LANES), shape(4, 8, PEERS, LANES)),
        [VMEM] * 7,
        back_scratch,
        flops=10**9,
        moved=4 * 10**6,
    )(weight, rotated, *forms)
    got_b = lax.ppermute(send_b, "core", swap)
    sides = (
        ("zl", swap),
        (("zt", "zm", "zl"), [(z, (z + (1 if z % 2 else -1)) % 8) for z in range(8)]),
    )
    pair_a = lax.ppermute(keep_a[2:] + got_a[2:], *sides[0])
    pair_b = lax.ppermute(keep_b[2:] + got_b[2:], *sides[1])
    four_a = lax.ppermute(keep_a[1] + got_a[1] + pair_a[1], *sides[1])
    four_b = lax.ppermute(keep_b[1] + got_b[1] + pair_b[1], *sides[0])
    sent = call(
        merged_kernel,
        "merged",
        shape(PEERS * MESSAGE, LANES),
        [VMEM] * 4,
        flops=10**6,
        moved=2 * 10**6,
    )(
        keep_a[0] + got_a[0] + pair_a[0], four_a, keep_b[0] + got_b[0] + pair_b[0], four_b
    )
    third = exchange_flat(sent, ("zt", *COL), PEERS)
    new_factor, new_velocity = call(
        update_kernel,
        "update",
        (shape(256, LANES), shape(256, LANES)),
        [VMEM] * 3,
        [
            pltpu.VMEM((256, LANES), F32),
            pltpu.VMEM((COLS * MESSAGE, LANES), F32),
            pltpu.VMEM((32, LANES), F32),
            pltpu.VMEM((256, LANES), F32),
        ],
        flops=10**7,
        moved=10**6,
    )(third, first, moved)

    def back_to_rows(array):
        return array.reshape(32, HIGHS, 2, LANES).transpose(0, 2, 1, 3).reshape(32, 2, RIGHT)

    return back_to_rows(new_factor), back_to_rows(new_velocity)


def solution(mesh):
    split = Mesh(mesh.devices.reshape(2, 2, 2, 2, 4, 4), ("zt", "zm", "zl", "core", "y", "x"))
    every = ("zt", "zm", "zl", "core", "y", "x")
    return jax.shard_map(
        shards,
        mesh=split,
        in_specs=(P(COL, None, None), P(None, None, every), P(SET, None), P(SET, None)),
        out_specs=(P(None, None, every), P(None, None, every)),
        check_vma=False,
    )
```
